32 devices in a mesh: tensor: 4 (over y, x), dp: 8 (over z, core).
Axes of the slice: x: 2, y: 2, z: 4, core: 2. Of those that a mesh axis runs over, the one named last changes fastest.
Arguments:
- images: bfloat16 [32, 729, 1152], P('dp'), may hold values from -16 to 16
- counts: int32 [8], P('dp'), may hold values from 3 to 4, as said below
- ln1_gain: bfloat16 [1152], replicated, may hold values from 0.099609375 to 1.8984375
- ln1_bias: bfloat16 [1152], replicated, may hold values from -3 to 3
- qkv_weight: bfloat16 [3, 1152, 1152], P(None, None, 'tensor'), may hold values from -1 to 1
- qv_bias: bfloat16 [2, 1152], P(None, 'tensor'), may hold values from -3 to 3
- out_weight: bfloat16 [1152, 1152], P('tensor'), may hold values from -1.5 to 1.5
- out_bias: bfloat16 [1152], replicated, may hold values from -3 to 3
- ln2_gain: bfloat16 [1152], replicated, may hold values from 0.099609375 to 1.8984375
- ln2_bias: bfloat16 [1152], replicated, may hold values from -3 to 3
- fc1_weight: bfloat16 [1152, 4304], P(None, 'tensor'), may hold values from -0.1875 to 0.1875
- fc1_bias: bfloat16 [4304], P('tensor'), may hold values from -3 to 3
- fc2_weight: bfloat16 [4304, 1152], P('tensor'), may hold values from -0.25 to 0.25
- fc2_bias: bfloat16 [1152], replicated, may hold values from -3 to 3
- grad_out: bfloat16 [32, 729, 1152], P('dp'), may hold values from -6 to 6
Outputs:
- block_out: float32 [32, 729, 1152], P('dp', None, 'tensor')
- grad_in: float32 [32, 729, 1152], P('dp', None, 'tensor')
- grad_ln1_gain: float32 [1152], P('tensor')
- grad_ln1_bias: float32 [1152], P('tensor')
- grad_qkv_weight: float32 [3, 1152, 1152], P(None, None, 'tensor')
- grad_qv_bias: float32 [2, 1152], P(None, 'tensor')
- grad_out_weight: float32 [1152, 1152], P('tensor')
- grad_out_bias: float32 [1152], P('tensor')
- grad_ln2_gain: float32 [1152], P('tensor')
- grad_ln2_bias: float32 [1152], P('tensor')
- grad_fc1_weight: float32 [1152, 4304], P(None, 'tensor')
- grad_fc1_bias: float32 [4304], P('tensor')
- grad_fc2_weight: float32 [4304, 1152], P('tensor')
- grad_fc2_bias: float32 [1152], P('tensor')
The draws below stay inside these ranges and needn't reach their ends.
Inputs may be any that keep to these rules, and one draw needn't show every extreme that they name: `counts`: exactly 6 of the 8 replicas hold 4 live images, the others 4 - 1; a replica's live images fill its first slots.
All inputs are finite; a program needn't handle non-finite values.
Results may differ from the reference program's by a relative error of at most 0.02.
Values may be sent and summed in bfloat16 or wider, within the bound.
A program may use at most 192 MiB of HBM per device.

```python
import math
import jax
import jax.numpy as jnp
from jax import lax

D = 1152
HEADS = 16
HD = 72
FF = 4304
L = 729
SLOTS = 4
FULL = 6
BUFFER = 32
N_TENSOR = 4
N_DP = 8


def draw_images(key, part):
    first, second = jax.random.split(jax.random.fold_in(key, 11), 2)
    scales = jnp.exp(jax.random.uniform(second, (BUFFER, L, 1), jnp.float32, math.log(0.5), math.log(5.0)))
    values = jax.random.normal(first, (BUFFER, L, D), jnp.float32) * scales
    return jnp.clip(values, -16.0, 16.0).astype(jnp.bfloat16)


def draw_counts(key, part):
    order = jax.random.permutation(jax.random.fold_in(key, 5), N_DP)
    return (SLOTS - 1 + (order < FULL).astype(jnp.int32)).astype(jnp.int32)


def draw_qkv_weight(key, part):
    base = jax.random.truncated_normal(jax.random.fold_in(key, 23), -6.0, 6.0, (3, D, D), jnp.float32) / math.sqrt(D)
    return base.astype(jnp.bfloat16)


def block_levels(stream_key, dims, shards, low, high):
    level = 1.0
    for axis_at, blocks in shards:
        steps = jax.random.uniform(jax.random.fold_in(jax.random.fold_in(stream_key, 6), axis_at), (blocks,), jnp.float32, low / len(shards), high / len(shards))
        level = level * jnp.repeat(jnp.exp(steps), dims[axis_at] // blocks).reshape((-1,) + (1,) * (len(dims) - 1 - axis_at))
    return level


def centred(stream_key, shape, scale, reach, shards=(), kind=jnp.bfloat16):
    entries = jax.random.normal(stream_key, shape, jnp.float32) * scale
    if len(shards) > 0:
        entries = block_levels(stream_key, shape, shards, -0.22, 0.18) * entries
    return jnp.clip(entries, min=-reach, max=reach).astype(kind)


def setup_inputs(seed: int = 0) -> dict:
    splits = jax.random.split(jax.random.key(seed), 16)
    return {
        "images": draw_images(jax.random.fold_in(splits[15], 71), 0),
        "counts": draw_counts(jax.random.fold_in(splits[15], 71), 0),
        "ln1_gain": jnp.clip(1.0 + 0.18 * jax.random.normal(splits[2], (D,), jnp.float32), 0.099609375, 1.8984375).astype(jnp.bfloat16),
        "ln1_bias": centred(splits[3], (D,), 0.3, 3.0),
        "qkv_weight": draw_qkv_weight(jax.random.fold_in(splits[15], 71), 0),
        "qv_bias": centred(splits[5], (2, D), 0.5, 3.0, ((1, 4),)),
        "out_weight": centred(splits[6], (D, D), (max(1, D // 64)) ** -0.5, 1.5, ((0, 4),)),
        "out_bias": centred(splits[7], (D,), 0.5, 3.0),
        "ln2_gain": jnp.clip(1.0 + 0.18 * jax.random.normal(splits[8], (D,), jnp.float32), 0.099609375, 1.8984375).astype(jnp.bfloat16),
        "ln2_bias": centred(splits[9], (D,), 0.3, 3.0),
        "fc1_weight": centred(splits[10], (D, FF), D ** -0.5, 0.1875, ((1, 4),)),
        "fc1_bias": centred(splits[11], (FF,), 0.5, 3.0, ((0, 4),)),
        "fc2_weight": centred(splits[12], (FF, D), (max(1, FF // 8)) ** -0.5, 0.25, ((0, 4),)),
        "fc2_bias": centred(splits[13], (D,), 0.5, 3.0),
        "grad_out": centred(splits[14], (BUFFER, L, D), 1.0, 6.0, ((0, 8),)),
    }


EPS = 1e-06

@jax.custom_vjp
def low(v):
    return lax.optimization_barrier(v.astype(jnp.bfloat16)).astype(jnp.float32)

@jax.custom_vjp
def low_back(v):
    return v

def low_keep(v):
    return (low(v), None)

def low_pass(kept, grad):
    return (grad,)

def back_keep(v):
    return (v, None)

def back_low(kept, grad):
    return (low(grad),)
low.defvjp(low_keep, low_pass)
low_back.defvjp(back_keep, back_low)

def both_ways(values):
    return low(low_back(values))

def matmul(left, right):
    return jnp.dot(left, right, precision=lax.Precision.HIGHEST)

def norm_rows(values, gain, shift):
    average = lax.optimization_barrier(jnp.mean(values, axis=-1, keepdims=True))
    centered = values - average
    variance = lax.optimization_barrier(jnp.mean(centered * centered, axis=-1, keepdims=True))
    return centered * lax.rsqrt(variance + EPS) * gain + shift

def to_heads(values):
    return values.reshape(values.shape[0], HEADS, HD)

def group_sum(left, weight):
    row_count = left.shape[0]
    split_left = left.reshape(row_count, N_TENSOR, -1)
    split_weight = weight.reshape(N_TENSOR, -1, weight.shape[1])
    partial_value = jnp.einsum('rgk,gkd->grd', split_left, split_weight, precision=lax.Precision.HIGHEST)
    return lax.optimization_barrier(jnp.sum(low(partial_value), axis=0))

def one_image(picture, params):
    ln1_gain, ln1_bias, qkv_weight, qv_bias, out_weight, out_bias, ln2_gain, ln2_bias, fc1_weight, fc1_bias, fc2_weight, fc2_bias = params
    normed_one = low(norm_rows(picture, ln1_gain, ln1_bias))
    query_rows = both_ways(matmul(normed_one, qkv_weight[0]) + qv_bias[0])
    key_rows = both_ways(matmul(normed_one, qkv_weight[1]))
    value_rows = both_ways(matmul(normed_one, qkv_weight[2]) + qv_bias[1])
    scores = jnp.einsum('qhd,khd->hqk', to_heads(query_rows), to_heads(key_rows), precision=lax.Precision.HIGHEST)
    scores = low_back(scores * (1.0 / math.sqrt(HD)))
    attention = low(jax.nn.softmax(scores, axis=-1))
    mixed = jnp.einsum('hqk,khd->qhd', attention, to_heads(value_rows), precision=lax.Precision.HIGHEST)
    mixed = both_ways(mixed.reshape(picture.shape[0], D))
    residual = picture + low_back(group_sum(mixed, out_weight)) + out_bias
    normed_two = low(norm_rows(residual, ln2_gain, ln2_bias))
    preact = low_back(matmul(normed_two, fc1_weight) + fc1_bias)
    activated = low(jax.nn.gelu(preact, approximate=True))
    return residual + low_back(group_sum(activated, fc2_weight)) + fc2_bias

def reference(images, counts, ln1_gain, ln1_bias, qkv_weight, qv_bias, out_weight, out_bias, ln2_gain, ln2_bias, fc1_weight, fc1_bias, fc2_weight, fc2_bias, grad_out):
    params = tuple((item.astype(jnp.float32) for item in (ln1_gain, ln1_bias, qkv_weight, qv_bias, out_weight, out_bias, ln2_gain, ln2_bias, fc1_weight, fc1_bias, fc2_weight, fc2_bias)))
    slot_ids = jnp.arange(N_DP * SLOTS, dtype=jnp.int32)
    live = (slot_ids % SLOTS < jnp.take(counts, slot_ids // SLOTS)).astype(jnp.float32)

    def forward(pictures, weights):

        def per_image(picture):
            return one_image(picture, weights)
        outputs = lax.map(jax.checkpoint(per_image), pictures)
        return outputs * live[:, None, None]
    block_out, pullback = jax.vjp(forward, images.astype(jnp.float32), params)
    grad_in, grads = pullback(grad_out.astype(jnp.float32))
    return (block_out, grad_in, grads[0], grads[1], grads[2], grads[3], grads[4], grads[5], grads[6], grads[7], grads[8], grads[9], grads[10], grads[11])
```

```python
import math

import jax
import jax.numpy as jnp
from jax import lax
from jax.experimental import pallas as pl
from jax.experimental.pallas import tpu as pltpu
from jax.sharding import PartitionSpec as P

HD = 72


EPS = 1e-06


def own_columns(values, share_width):
    start = lax.axis_index("tensor") * share_width
    return lax.dynamic_slice_in_dim(values, start, share_width, values.ndim - 1)


def row_mean(values):
    return jnp.mean(values, axis=-1, keepdims=True)


def group_stats(first, second):
    return lax.psum((first, second), "tensor")


def contract_rows(left, right):
    return lax.dot_general(
        left, right, (((0,), (0,)), ((), ())), preferred_element_type=jnp.float32
    )


def contract_cols(left, right):
    return lax.dot_general(
        left, right, (((1,), (1,)), ((), ())), preferred_element_type=jnp.float32
    )


def gelu_tanh(values):
    return jax.nn.gelu(values, approximate=True)


def local(
    images,
    counts,
    ln1_gain,
    ln1_bias,
    qkv_weight,
    qv_bias,
    out_weight,
    out_bias,
    ln2_gain,
    ln2_bias,
    fc1_weight,
    fc1_bias,
    fc2_weight,
    fc2_bias,
    grad_out,
):
    slot_count, length, full_width = images.shape
    share_width = full_width // lax.axis_size("tensor")
    local_width = qkv_weight.shape[2]
    local_heads = local_width // HD
    hidden_width = fc1_weight.shape[1]
    score_scale = 1.0 / math.sqrt(HD)
    gain_one = ln1_gain.astype(jnp.float32)
    shift_one = ln1_bias.astype(jnp.float32)
    gain_two = ln2_gain.astype(jnp.float32)
    shift_two = ln2_bias.astype(jnp.float32)
    bias_out = out_bias.astype(jnp.float32)
    bias_fc1 = fc1_bias.astype(jnp.float32)
    bias_fc2 = fc2_bias.astype(jnp.float32)
    bias_query = qv_bias[0].astype(jnp.float32)
    bias_value = qv_bias[1].astype(jnp.float32)
    live_count = counts[0]

    def to_heads(values):
        return values.reshape(length, local_heads, HD)

    def head_scores(query_heads, key_heads):
        return (
            jnp.einsum("qhd,khd->hqk", query_heads, key_heads, preferred_element_type=jnp.float32)
            * score_scale
        )

    def layer_step(slot_index, loop_state):
        block_acc, input_acc, grads = loop_state
        (
            grad_gain_one,
            grad_shift_one,
            grad_qkv,
            grad_qv,
            grad_out_w,
            grad_out_b,
            grad_gain_two,
            grad_shift_two,
            grad_fc1_w,
            grad_fc1_b,
            grad_fc2_w,
            grad_fc2_b,
        ) = grads
        live_flag = (slot_index < live_count).astype(jnp.float32)
        picture = lax.dynamic_index_in_dim(images, slot_index, 0, keepdims=False).astype(
            jnp.float32
        )
        upstream = (
            lax.dynamic_index_in_dim(grad_out, slot_index, 0, keepdims=False).astype(jnp.float32)
            * live_flag
        )
        upstream_low = upstream.astype(jnp.bfloat16)
        centered = picture - row_mean(picture)
        inv_one = lax.rsqrt(row_mean(centered * centered) + EPS)
        unit_one = centered * inv_one
        normed_one = (unit_one * gain_one + shift_one).astype(jnp.bfloat16)
        query_rows = (
            jnp.dot(normed_one, qkv_weight[0], preferred_element_type=jnp.float32) + bias_query
        ).astype(jnp.bfloat16)
        key_rows = jnp.dot(normed_one, qkv_weight[1], preferred_element_type=jnp.float32).astype(
            jnp.bfloat16
        )
        value_rows = (
            jnp.dot(normed_one, qkv_weight[2], preferred_element_type=jnp.float32) + bias_value
        ).astype(jnp.bfloat16)
        query_heads = to_heads(query_rows)
        key_heads = to_heads(key_rows)
        value_heads = to_heads(value_rows)
        scores = head_scores(query_heads, key_heads)
        row_top = jnp.max(scores, axis=-1, keepdims=True)
        logsum = row_top + jnp.log(jnp.sum(jnp.exp(scores - row_top), axis=-1, keepdims=True))
        probs_low = jnp.exp(scores - logsum).astype(jnp.bfloat16)
        mixed = jnp.einsum(
            "hqk,khd->qhd", probs_low, value_heads, preferred_element_type=jnp.float32
        )
        mixed = mixed.reshape(length, local_width).astype(jnp.bfloat16)
        partial_out = jnp.dot(mixed, out_weight, preferred_element_type=jnp.float32).astype(
            jnp.bfloat16
        )
        residual = (
            own_columns(picture, share_width)
            + lax.psum_scatter(partial_out, "tensor", scatter_dimension=1, tiled=True).astype(
                jnp.float32
            )
            + own_columns(bias_out, share_width)
        )
        row_sum, row_square = group_stats(
            jnp.sum(residual, axis=-1), jnp.sum(residual * residual, axis=-1)
        )
        average = row_sum[:, None] / full_width
        inv_two = lax.rsqrt(row_square[:, None] / full_width - average * average + EPS)
        unit_two = (residual - average) * inv_two
        own_normed = (
            unit_two * own_columns(gain_two, share_width) + own_columns(shift_two, share_width)
        ).astype(jnp.bfloat16)
        normed_two = lax.all_gather(own_normed, "tensor", axis=1, tiled=True)
        preact = jnp.dot(normed_two, fc1_weight, preferred_element_type=jnp.float32) + bias_fc1
        activated = gelu_tanh(preact).astype(jnp.bfloat16)
        partial_mlp = jnp.dot(activated, fc2_weight, preferred_element_type=jnp.float32).astype(
            jnp.bfloat16
        )
        block_rows = (
            residual
            + lax.psum_scatter(partial_mlp, "tensor", scatter_dimension=1, tiled=True).astype(
                jnp.float32
            )
            + own_columns(bias_fc2, share_width)
        )
        block_rows = block_rows * live_flag
        grad_fc2_b = grad_fc2_b + own_columns(jnp.sum(upstream, axis=0), share_width)
        grad_fc2_w = grad_fc2_w + contract_rows(activated, upstream_low)
        d_act = contract_cols(upstream_low, fc2_weight)
        gelu_pull = jax.vjp(gelu_tanh, preact)[1]
        d_pre = gelu_pull(d_act)[0].astype(jnp.bfloat16)
        grad_fc1_b = grad_fc1_b + jnp.sum(d_pre.astype(jnp.float32), axis=0)
        grad_fc1_w = grad_fc1_w + contract_rows(normed_two, d_pre)
        back_mlp = contract_cols(d_pre, fc1_weight)
        d_norm_two = lax.psum_scatter(
            back_mlp.astype(jnp.bfloat16), "tensor", scatter_dimension=1, tiled=True
        ).astype(jnp.float32)
        scaled_two = d_norm_two * own_columns(gain_two, share_width)
        sum_plain, sum_cross = group_stats(
            jnp.sum(scaled_two, axis=-1), jnp.sum(scaled_two * unit_two, axis=-1)
        )
        d_residual = own_columns(upstream, share_width) + inv_two * (
            scaled_two
            - sum_plain[:, None] / full_width
            - unit_two * (sum_cross[:, None] / full_width)
        )
        grad_gain_two = grad_gain_two + jnp.sum(d_norm_two * unit_two, axis=0)
        grad_shift_two = grad_shift_two + jnp.sum(d_norm_two, axis=0)
        grad_out_b = grad_out_b + jnp.sum(d_residual, axis=0)
        d_residual_low = lax.all_gather(
            d_residual.astype(jnp.bfloat16), "tensor", axis=1, tiled=True
        )
        grad_out_w = grad_out_w + contract_rows(mixed, d_residual_low)
        d_mixed_heads = to_heads(contract_cols(d_residual_low, out_weight).astype(jnp.bfloat16))
        probs = jnp.exp(head_scores(query_heads, key_heads) - logsum)
        probs_again = probs.astype(jnp.bfloat16)
        d_value = jnp.einsum(
            "hqk,qhd->khd", probs_again, d_mixed_heads, preferred_element_type=jnp.float32
        )
        d_probs = jnp.einsum(
            "qhd,khd->hqk", d_mixed_heads, value_heads, preferred_element_type=jnp.float32
        )
        inner = jnp.sum(probs * d_probs, axis=-1, keepdims=True)
        d_scores = (probs * (d_probs - inner)).astype(jnp.bfloat16)
        d_query = (
            jnp.einsum("hqk,khd->qhd", d_scores, key_heads, preferred_element_type=jnp.float32)
            * score_scale
        )
        d_key = (
            jnp.einsum("hqk,qhd->khd", d_scores, query_heads, preferred_element_type=jnp.float32)
            * score_scale
        )
        d_stack = (
            jnp.stack([d_query, d_key, d_value], axis=1)
            .reshape(length, 3, local_width)
            .astype(jnp.bfloat16)
        )
        grad_qkv = grad_qkv + jnp.einsum(
            "ld,lje->jde", normed_one, d_stack, preferred_element_type=jnp.float32
        )
        bias_sums = jnp.sum(d_stack.astype(jnp.float32), axis=0)
        grad_qv = grad_qv + jnp.stack([bias_sums[0], bias_sums[2]])
        back_attn = jnp.einsum(
            "lje,jde->ld", d_stack, qkv_weight, preferred_element_type=jnp.float32
        )
        d_norm_one = lax.psum_scatter(
            back_attn.astype(jnp.bfloat16), "tensor", scatter_dimension=1, tiled=True
        ).astype(jnp.float32)
        own_unit = own_columns(unit_one, share_width)
        scaled_one = d_norm_one * own_columns(gain_one, share_width)
        plain_one, cross_one = group_stats(
            jnp.sum(scaled_one, axis=-1), jnp.sum(scaled_one * own_unit, axis=-1)
        )
        d_input = d_residual + inv_one * (
            scaled_one
            - plain_one[:, None] / full_width
            - own_unit * (cross_one[:, None] / full_width)
        )
        grad_gain_one = grad_gain_one + jnp.sum(d_norm_one * own_unit, axis=0)
        grad_shift_one = grad_shift_one + jnp.sum(d_norm_one, axis=0)
        block_acc = lax.dynamic_update_index_in_dim(block_acc, block_rows, slot_index, 0)
        input_acc = lax.dynamic_update_index_in_dim(input_acc, d_input, slot_index, 0)
        new_grads = (
            grad_gain_one,
            grad_shift_one,
            grad_qkv,
            grad_qv,
            grad_out_w,
            grad_out_b,
            grad_gain_two,
            grad_shift_two,
            grad_fc1_w,
            grad_fc1_b,
            grad_fc2_w,
            grad_fc2_b,
        )
        return (block_acc, input_acc, new_grads)

    share_zeros = jnp.zeros((share_width,), jnp.float32)
    start_grads = (
        share_zeros,
        share_zeros,
        jnp.zeros((3, full_width, local_width), jnp.float32),
        jnp.zeros((2, local_width), jnp.float32),
        jnp.zeros((local_width, full_width), jnp.float32),
        share_zeros,
        share_zeros,
        share_zeros,
        jnp.zeros((full_width, hidden_width), jnp.float32),
        jnp.zeros((hidden_width,), jnp.float32),
        jnp.zeros((hidden_width, full_width), jnp.float32),
        share_zeros,
    )
    start_rows = jnp.zeros((slot_count, length, share_width), jnp.float32)
    block_acc, input_acc, grads = lax.fori_loop(
        0, slot_count, layer_step, (start_rows, start_rows, start_grads)
    )
    (
        grad_gain_one,
        grad_shift_one,
        grad_qkv,
        grad_qv,
        grad_out_w,
        grad_out_b,
        grad_gain_two,
        grad_shift_two,
        grad_fc1_w,
        grad_fc1_b,
        grad_fc2_w,
        grad_fc2_b,
    ) = grads
    summed = (
        lax.psum(grad_gain_one.astype(jnp.bfloat16), "dp").astype(jnp.float32),
        lax.psum(grad_shift_one.astype(jnp.bfloat16), "dp").astype(jnp.float32),
        lax.psum(grad_qkv.astype(jnp.bfloat16), "dp").astype(jnp.float32),
        lax.psum(grad_qv.astype(jnp.bfloat16), "dp").astype(jnp.float32),
        lax.psum(grad_out_w.astype(jnp.bfloat16), "dp").astype(jnp.float32),
        lax.psum(grad_out_b.astype(jnp.bfloat16), "dp").astype(jnp.float32),
        lax.psum(grad_gain_two.astype(jnp.bfloat16), "dp").astype(jnp.float32),
        lax.psum(grad_shift_two.astype(jnp.bfloat16), "dp").astype(jnp.float32),
        lax.psum(grad_fc1_w.astype(jnp.bfloat16), "dp").astype(jnp.float32),
        lax.psum(grad_fc1_b.astype(jnp.bfloat16), "dp").astype(jnp.float32),
        lax.psum(grad_fc2_w.astype(jnp.bfloat16), "dp").astype(jnp.float32),
        lax.psum(grad_fc2_b.astype(jnp.bfloat16), "dp").astype(jnp.float32),
    )
    return (
        block_acc,
        input_acc,
        summed[0],
        summed[1],
        summed[2],
        summed[3],
        summed[4],
        summed[5],
        summed[6],
        summed[7],
        summed[8],
        summed[9],
        summed[10],
        summed[11],
    )


LOG2E = math.log2(math.e)
LN2 = math.log(2.0)
GELU_A = math.sqrt(2.0 / math.pi)
GELU_B = 0.044715
BF = jnp.bfloat16
F32 = jnp.float32
QUERY_BLOCK = 256
MESH = pl.DeviceIdType.MESH
TURN = {"x": 1, "y": 2}
OTHER = {"x": "y", "y": "x"}
SIDE = {"x": 0, "y": 1}
LANES = ("x", "y")
ANYWHERE = pl.BlockSpec(memory_space=pl.ANY)


def dot_nn(left, right):
    return lax.dot_general(left, right, (((1,), (0,)), ((), ())), preferred_element_type=F32)


def place(bit):
    if bit == "core":
        return {"dp": lax.axis_index("dp") ^ 1}
    return {"tensor": lax.axis_index("tensor") ^ TURN[bit]}


def hop(source, target, sems, index, to):
    return pltpu.make_async_remote_copy(
        src_ref=source,
        dst_ref=target,
        send_sem=sems.at[0, index],
        recv_sem=sems.at[1, index],
        device_id=place(to) if isinstance(to, str) else to,
        device_id_type=MESH,
    )


def line_place():
    dp = lax.axis_index("dp")
    return dp // 2, {"dp": lax.rem(dp + 2, 8)}, {"dp": lax.rem(dp + 6, 8)}


class GatherRide:
    partners = ("x", "y", "core")

    def __init__(self, own, steps):
        _, count, rows, width = own.shape
        self.inputs = [own]
        shape = lambda *lead: jax.ShapeDtypeStruct((*lead, count, rows, width), own.dtype)
        self.outputs = [shape(2), shape(2), shape(), shape()]
        self.scratch = [pltpu.SemaphoreType.DMA((2, 6 * count))]
        self.steps = steps

    def events(self, refs):
        own, near, near_part, far, far_part, sems = refs
        count = len(LANES)
        near_hop, far_hop, swap_near, swap_far = {}, [], {}, []
        for lane, first in enumerate(LANES):
            for bit in LANES:
                k = SIDE[bit]
                near_hop[bit, lane] = hop(
                    own.at[0, lane], near.at[k, lane], sems, 2 * lane + k, bit
                )
                swap_near[bit, lane] = hop(
                    near.at[k, lane], near_part.at[k, lane], sems, 3 * count + 2 * lane + k, "core"
                )
            far_hop.append(
                hop(near.at[SIDE[first], lane], far.at[lane], sems, 2 * count + lane, OTHER[first])
            )
            swap_far.append(hop(far.at[lane], far_part.at[lane], sems, 5 * count + lane, "core"))

        def start():
            for bit in LANES:
                for lane in sorted(range(count), key=lambda lane: LANES[lane] != bit):
                    near_hop[bit, lane].start()

        def forward():
            for lane, first in enumerate(LANES):
                near_hop[first, lane].wait_recv()
                far_hop[lane].start()
                swap_near[first, lane].start()

        def finish():
            for lane, first in enumerate(LANES):
                near_hop[OTHER[first], lane].wait_recv()
                swap_near[OTHER[first], lane].start()
            for lane in range(count):
                far_hop[lane].wait_recv()
                swap_far[lane].start()
            for each in near_hop.values():
                each.wait_send()
            for each in far_hop:
                each.wait_send()
            for each in [*swap_near.values(), *swap_far]:
                each.wait()

        return [(self.steps[0], start), (self.steps[1], forward), ("end", finish)]


class SwapRide:
    partners = ("core",)

    def __init__(self, *arrays):
        self.inputs = list(arrays)
        self.outputs = [jax.ShapeDtypeStruct(a.shape, a.dtype) for a in arrays]
        self.scratch = [pltpu.SemaphoreType.DMA((2, len(arrays)))]

    def events(self, refs):
        count = len(self.inputs)
        hops = [hop(refs[k], refs[count + k], refs[-1], k, "core") for k in range(count)]

        def start():
            for each in hops:
                each.start()

        def finish():
            for each in hops:
                each.wait()

        return [(0, start), ("end", finish)]


class PlaneRide:
    partners = LANES

    def __init__(self, rows, step):
        _, count, unit, width = rows.shape
        self.inputs = [rows]
        self.outputs = [jax.ShapeDtypeStruct((count, unit, width), rows.dtype)]
        tile = lambda *lead: pltpu.VMEM((*lead, unit, width), rows.dtype)
        self.scratch = [
            tile(count, 2),
            tile(count, 2),
            tile(count),
            pltpu.SemaphoreType.DMA((2, 3 * count)),
            pltpu.SemaphoreType.DMA((3 * count,)),
        ]
        self.step = step

    def events(self, refs):
        rows, total, base, got, last, sems, local = refs
        kept = {"x": (0, 2), "y": (0, 1)}
        gone = {"x": (1, 3), "y": (2, 3)}
        first_hop, loads, next_hop, stores = {}, {}, [], []
        for lane, first in enumerate(LANES):
            for k in range(2):
                index = 2 * lane + k
                first_hop[lane, k] = hop(
                    rows.at[gone[first][k], lane], got.at[lane, k], sems, index, first
                )
                loads[lane, k] = pltpu.make_async_copy(
                    rows.at[kept[first][k], lane], base.at[lane, k], local.at[index]
                )
            next_hop.append(hop(base.at[lane, 1], last.at[lane], sems, 4 + lane, OTHER[first]))
            stores.append(
                pltpu.make_async_copy(base.at[lane, 0], total.at[lane], local.at[4 + lane])
            )

        def start():
            for k in (1, 0):
                for lane in range(2):
                    first_hop[lane, k].start()
                    loads[lane, k].start()

        def forward():
            for k in (1, 0):
                for lane in range(2):
                    loads[lane, k].wait()
                    first_hop[lane, k].wait_recv()
                    base[lane, k] += got[lane, k]
                    if k == 1:
                        next_hop[lane].start()

        def finish():
            for lane in range(2):
                next_hop[lane].wait_recv()
                base[lane, 0] += last[lane]
                stores[lane].start()
            for lane in range(2):
                next_hop[lane].wait_send()
                stores[lane].wait()
            for each in first_hop.values():
                each.wait_send()

        return [(0, start), (self.step, forward), ("end", finish)]


class LineRide:
    partners = ("line", "core")

    def __init__(self, rows, steps):
        count, unit, width = rows.shape
        self.inputs = [rows]
        self.outputs = [jax.ShapeDtypeStruct(rows.shape, rows.dtype)] * 2
        tile = pltpu.VMEM((count, unit, width), rows.dtype)
        self.scratch = [
            tile,
            tile,
            tile,
            pltpu.SemaphoreType.DMA((2, 4 * count)),
            pltpu.SemaphoreType.DMA((2 * count,)),
        ]
        self.steps = steps

    def events(self, refs):
        rows, total, other, held, outer, middle, sems, local = refs
        count = self.inputs[0].shape[0]
        z, up, down = line_place()
        is_outer = jnp.logical_or(z == 0, z == 3)
        is_inner = jnp.logical_not(is_outer)
        low = z < 2
        to = {True: (up, up, down), False: (down, down, up)}

        def both(action):
            pl.when(low)(lambda: action(*to[True]))
            pl.when(jnp.logical_not(low))(lambda: action(*to[False]))

        load = [pltpu.make_async_copy(rows.at[k], held.at[k], local.at[k]) for k in range(count)]
        store = [
            pltpu.make_async_copy(held.at[k], total.at[k], local.at[count + k])
            for k in range(count)
        ]
        inward = lambda k, at: hop(held.at[k], outer.at[k], sems, k, at)
        across = lambda k, at: hop(held.at[k], middle.at[k], sems, count + k, at)
        back = lambda k, at: hop(held.at[k], outer.at[k], sems, 2 * count + k, at)
        swap = [hop(held.at[k], other.at[k], sems, 3 * count + k, "core") for k in range(count)]
        every = range(count)

        def start():
            for k in every:
                load[k].start()
            for k in every:
                load[k].wait()

            @pl.when(is_outer)
            def _():
                for k in every:
                    both(lambda a, b, c, k=k: inward(k, a).start())

        def meet():
            @pl.when(is_inner)
            def _():
                for k in every:
                    inward(k, up).wait_recv()
                    held[k] += outer[k]
                    both(lambda a, b, c, k=k: across(k, b).start())

        def leave():
            @pl.when(is_inner)
            def _():
                for k in every:
                    across(k, up).wait_recv()
                    across(k, up).wait_send()
                    held[k] += middle[k]
                    both(lambda a, b, c, k=k: back(k, c).start())
                    swap[k].start()
                    store[k].start()

        def finish():
            @pl.when(is_outer)
            def _():
                for k in every:
                    inward(k, up).wait_send()
                    back(k, up).wait_recv()
                    held[k] = outer[k]
                    swap[k].start()
                    store[k].start()

            @pl.when(is_inner)
            def _():
                for k in every:
                    back(k, up).wait_send()

            for k in every:
                store[k].wait()
                swap[k].wait()

        return [(0, start), (self.steps[0], meet), (self.steps[1], leave), ("end", finish)]


class SpreadRide:
    partners = ("x", "y", "xy")

    def __init__(self, rows):
        self.inputs = [rows]
        self.outputs = [jax.ShapeDtypeStruct((3, *rows.shape[1:]), rows.dtype)]
        self.scratch = [pltpu.SemaphoreType.DMA((2, 3))]

    def events(self, refs):
        rows, landed, sems = refs
        t = lax.axis_index("tensor")
        hops = [
            hop(rows.at[t ^ r], landed.at[r - 1], sems, r - 1, {"tensor": t ^ r}) for r in (3, 1, 2)
        ]

        def start():
            for each in hops:
                each.start()

        def finish():
            for each in hops:
                each.wait()

        return [(0, start), ("end", finish)]


class VectorRide:
    partners = ("x", "y", "core", "line")

    def __init__(self, rows):
        self.inputs = [rows]
        self.outputs = [jax.ShapeDtypeStruct(rows.shape, rows.dtype)]
        self.scratch = [
            pltpu.VMEM(rows.shape, rows.dtype),
            pltpu.VMEM((6, *rows.shape), rows.dtype),
            pltpu.SemaphoreType.DMA((2, 6)),
            pltpu.SemaphoreType.DMA((2,)),
        ]

    def events(self, refs):
        rows, total, held, got, sems, local = refs
        z, up, down = line_place()
        is_outer = jnp.logical_or(z == 0, z == 3)
        low = z < 2
        step = lambda k, at: hop(held, got.at[k], sems, k, at)

        def towards(k, first, second):
            pl.when(low)(lambda: step(k, first).start())
            pl.when(jnp.logical_not(low))(lambda: step(k, second).start())

        def finish():
            load = pltpu.make_async_copy(rows, held, local.at[0])
            load.start()
            load.wait()
            for k, bit in enumerate(("core", "x", "y")):
                step(k, bit).start()
                step(k, bit).wait()
                held[...] += got[k]

            @pl.when(is_outer)
            def _():
                towards(3, up, down)
                step(3, up).wait_send()
                step(5, up).wait_recv()
                held[...] = got[5]

            @pl.when(jnp.logical_not(is_outer))
            def _():
                step(3, up).wait_recv()
                held[...] += got[3]
                towards(4, up, down)
                step(4, up).wait()
                held[...] += got[4]
                towards(5, down, up)
                step(5, up).wait_send()

            store = pltpu.make_async_copy(held, total, local.at[1])
            store.start()
            store.wait()

        return [("end", finish)]


def carry(body, inputs, in_specs, out_shape, out_specs, steps, name, rides=(), scratch=(), cost=0):
    ride_in = [array for ride in rides for array in ride.inputs]
    ride_out = [shape for ride in rides for shape in ride.outputs]
    ride_scratch = [each for ride in rides for each in ride.scratch]
    partners = sorted({bit for ride in rides for bit in ride.partners})

    def kernel(*refs):
        refs = list(refs)
        take = lambda count: [refs.pop(0) for _ in range(count)]
        ins, r_ins = take(len(inputs)), take(len(ride_in))
        outs, r_outs = take(len(out_shape)), take(len(ride_out))
        own, r_scratch = take(len(scratch)), take(len(ride_scratch))
        step = pl.program_id(0)
        events = []
        for ride in rides:
            mine = []
            for pool, kind in ((r_ins, ride.inputs), (r_outs, ride.outputs), (r_scratch, ride.scratch)):
                mine += [pool.pop(0) for _ in range(len(kind))]
            events += ride.events(mine)

        if rides:

            @pl.when(step == 0)
            def _():
                barrier = pltpu.get_barrier_semaphore()
                signal = lambda at: pl.semaphore_signal(
                    barrier, inc=1, device_id=at, device_id_type=MESH
                )
                for bit in partners:
                    if bit == "xy":
                        signal({"tensor": lax.axis_index("tensor") ^ 3})
                    elif bit != "line":
                        signal(place(bit))
                singles = len([bit for bit in partners if bit != "line"])
                if "line" in partners:
                    z, up, down = line_place()
                    pl.when(z < 3)(lambda: signal(up))
                    pl.when(z > 0)(lambda: signal(down))
                    inner = jnp.logical_and(z > 0, z < 3)
                    pl.when(inner)(lambda: pl.semaphore_wait(barrier, singles + 2))
                    pl.when(jnp.logical_not(inner))(
                        lambda: pl.semaphore_wait(barrier, singles + 1)
                    )
                else:
                    pl.semaphore_wait(barrier, singles)

        for when, event in events:
            if when != "end":
                pl.when(step == min(when, steps - 1))(event)
        body(*ins, *outs, *own)
        for when, event in events:
            if when == "end":
                pl.when(step == steps - 1)(event)

    params = {"vmem_limit_bytes": 60 << 20}
    if rides:
        carry.count += 1
        params.update(collective_id=carry.count, has_side_effects=True)
    results = pl.pallas_call(
        kernel,
        grid=(steps,),
        in_specs=list(in_specs) + [ANYWHERE] * len(ride_in),
        out_specs=list(out_specs) + [ANYWHERE] * len(ride_out),
        out_shape=list(out_shape) + ride_out,
        scratch_shapes=list(scratch) + ride_scratch,
        compiler_params=pltpu.CompilerParams(**params),
        cost_estimate=pl.CostEstimate(flops=int(cost), bytes_accessed=1 << 24, transcendentals=0),
        name=name,
    )(*inputs, *ride_in)
    results = list(results)
    groups = [results[: len(out_shape)]]
    results = results[len(out_shape) :]
    for ride in rides:
        groups.append(results[: len(ride.outputs)])
        results = results[len(ride.outputs) :]
    return groups


carry.count = 0


def whole(array):
    zeros = (0,) * array.ndim
    return pl.BlockSpec(array.shape, lambda i: zeros)


def shaped(shape, dtype=BF):
    return jax.ShapeDtypeStruct(shape, dtype)


def prepare_body(slot_ref, live_ref, im_ref, go_ref, gain_ref, bias_ref, x_ref, g_ref, n_ref, s_ref):
    slot = slot_ref[0]

    def pick(ref):
        values = ref[...].astype(F32)
        chosen = values[:, 0]
        for index in range(1, values.shape[1]):
            chosen = jnp.where(slot == index, values[:, index], chosen)
        return chosen

    picture = pick(im_ref)
    centered = picture - row_mean(picture)
    inverse = lax.rsqrt(row_mean(centered * centered) + EPS)
    normed = centered * inverse * gain_ref[...] + bias_ref[...]
    x_ref[...] = picture.T.astype(BF)
    g_ref[...] = (pick(go_ref) * live_ref[0].astype(F32)).T.astype(BF)
    n_ref[...] = normed.T.astype(BF)
    s_ref[0:1, :] = row_mean(picture).T
    s_ref[1:2, :] = inverse.T


def prepare(images, grad_out, slot, live, gain, bias, rides):
    slots, length, width = images.shape
    rows = 128
    scalar = pl.BlockSpec(memory_space=pltpu.SMEM)
    tokens = pl.BlockSpec((rows, slots, width), lambda i: (i, 0, 0))
    vector = pl.BlockSpec((1, width), lambda i: (0, 0))
    return carry(
        prepare_body,
        [slot, live, images.transpose(1, 0, 2), grad_out.transpose(1, 0, 2), gain, bias],
        [scalar, scalar, tokens, tokens, vector, vector],
        [shaped((width, length))] * 3 + [shaped((2, length), F32)],
        [pl.BlockSpec((width, rows), lambda i: (0, i))] * 3
        + [pl.BlockSpec((2, rows), lambda i: (0, i))],
        pl.cdiv(length, rows),
        "prepare",
        rides,
    )


def attend_head(weight, normed, bias, scale, qkv_ref, o_ref, lse_ref):
    length = normed.shape[1]
    rows = (dot_nn(weight, normed) + bias) * scale
    rows = rows.reshape(3, HD, length).astype(BF)
    qkv_ref[0] = rows
    queries, keys, values = rows[0], rows[1].T, rows[2]
    for start in range(0, length, QUERY_BLOCK):
        block = slice(start, min(start + QUERY_BLOCK, length))
        scores = dot_nn(keys, queries[:, block])
        top = jnp.max(scores, axis=0, keepdims=True)
        weights = jnp.exp2(scores - top)
        total = jnp.sum(weights, axis=0, keepdims=True)
        mixed = dot_nn(values, weights.astype(BF))
        o_ref[0, :, block] = (mixed * (1.0 / total)).astype(BF)
        lse_ref[0, :, block] = top + jnp.log2(total)


def attend(pieces, normed, bias, scale, rides):
    own, near, near_part, far, far_part = pieces
    width, length = normed.shape
    chunk = own.shape[2]
    rows = 3 * HD
    heads = 16
    lane = lambda i: lax.rem(i, 2)
    half = lambda i: lax.rem(i // 2, 2)
    clip = lambda i, low, high: jnp.minimum(jnp.maximum(i, low), high)

    def body(own_ref, near_ref, near_part_ref, far_ref, far_part_ref, n_ref, b_ref, s_ref, *outs):
        step = pl.program_id(0)
        shard, which = step // 4, half(step)
        weight = jnp.where(which == 0, near_ref[0, 0, :rows], near_part_ref[0, 0, :rows])
        last = jnp.where(which == 0, far_ref[0, :rows], far_part_ref[0, :rows])
        weight = jnp.where(shard == 0, own_ref[0, 0, :rows], jnp.where(shard == 3, last, weight))
        attend_head(weight, n_ref[...], b_ref[0], s_ref[...], *outs)

    near_spec = pl.BlockSpec(
        (1, 1, chunk, width), lambda i: (clip(i // 4 - 1, 0, 1), lane(i), 0, 0)
    )
    far_spec = pl.BlockSpec((1, chunk, width), lambda i: (lane(i), 0, 0))
    return carry(
        body,
        [own, near, near_part, far, far_part, normed, bias, scale],
        [
            pl.BlockSpec((1, 1, chunk, width), lambda i: (half(i), lane(i), 0, 0)),
            near_spec,
            near_spec,
            far_spec,
            far_spec,
            whole(normed),
            pl.BlockSpec((1, rows, 1), lambda i: (i, 0, 0)),
            whole(scale),
        ],
        [
            shaped((heads, 3, HD, length)),
            shaped((heads, HD, length)),
            shaped((heads, 1, length), F32),
        ],
        [
            pl.BlockSpec((1, 3, HD, length), lambda i: (i, 0, 0, 0)),
            pl.BlockSpec((1, HD, length), lambda i: (i, 0, 0)),
            pl.BlockSpec((1, 1, length), lambda i: (i, 0, 0)),
        ],
        heads,
        "attend",
        rides,
        cost=3e10,
    )


def piece_refs(own, near, near_part, far, far_part):
    return [
        own.at[0],
        own.at[1],
        near.at[0],
        near_part.at[0],
        near.at[1],
        near_part.at[1],
        far,
        far_part,
    ]


def project_out(pieces, mixed, picture, vectors, rides=()):
    width, length = picture.shape
    skip = 3 * HD

    def body(own, near, near_part, far, far_part, o_ref, x_ref, v_ref, h_ref, n_ref, s_ref, w_ref, held, sems):
        refs = piece_refs(own, near, near_part, far, far_part)
        copies = [
            pltpu.make_async_copy(
                ref.at[j, pl.ds(skip, HD)], held.at[2 * p + j], sems.at[2 * p + j]
            )
            for p, ref in enumerate(refs)
            for j in range(2)
        ]
        for each in copies:
            each.start()
        for each in copies:
            each.wait()
        weight = held[...].reshape(width, width)
        w_ref[...] = weight
        residual = x_ref[...].astype(F32) + contract_rows(weight, o_ref[...].reshape(width, length))
        residual = residual + v_ref[:, 2:3]
        average = jnp.mean(residual, axis=0, keepdims=True)
        centered = residual - average
        inverse = lax.rsqrt(jnp.mean(centered * centered, axis=0, keepdims=True) + EPS)
        h_ref[...] = residual
        n_ref[...] = (centered * inverse * v_ref[:, 3:4] + v_ref[:, 4:5]).astype(BF)
        s_ref[0:1, :] = average
        s_ref[1:2, :] = inverse

    outs = [
        shaped((width, length), F32),
        shaped((width, length)),
        shaped((2, length), F32),
        shaped((width, width)),
    ]
    return carry(
        body,
        [*pieces, mixed, picture, vectors],
        [ANYWHERE] * 5 + [whole(mixed), whole(picture), whole(vectors)],
        outs,
        [whole(each) for each in outs],
        1,
        "project_out",
        rides,
        scratch=[pltpu.VMEM((16, HD, width), BF), pltpu.SemaphoreType.DMA((16,))],
        cost=2e9,
    )


class Stream:
    def __init__(self, pieces, pair, rows=None):
        _, count, unit, width = pieces[0].shape
        self.pieces = list(pieces)
        self.group = 2 if pair else 1
        self.count = count
        self.rows = unit if rows is None else rows
        self.steps = 8 // self.group
        self.scratch = [
            pltpu.VMEM((2, self.group, count, self.rows, width), BF),
            pltpu.SemaphoreType.DMA((2, self.group * count)),
        ]

    def bring(self, refs, held, sems):
        step = pl.program_id(0)
        refs = piece_refs(*refs)

        def copies(piece, slot):
            return [
                pltpu.make_async_copy(
                    refs[piece * self.group + g].at[c, pl.ds(0, self.rows)],
                    held.at[slot, g, c],
                    sems.at[slot, g * self.count + c],
                )
                for g in range(self.group)
                for c in range(self.count)
            ]

        def start(piece):
            for each in copies(piece, piece % 2):
                each.start()

        pl.when(step == 0)(lambda: start(0))
        for piece in range(1, self.steps):
            pl.when(step == piece - 1)(lambda piece=piece: start(piece))
        slot = lax.rem(step, 2)
        for each in copies(0, slot):
            each.wait()
        return held[slot].reshape(-1, held.shape[-1])


def hidden_act(pieces, normed, bias, rides=()):
    width, length = normed.shape
    stream = Stream(pieces, False)
    rows = stream.count * stream.rows

    def body(p0, p1, p2, p3, p4, n_ref, b_ref, act_ref, slope_ref, held, sems):
        weight = stream.bring((p0, p1, p2, p3, p4), held, sems)
        preact = dot_nn(weight, n_ref[...]) + b_ref[0]
        square = preact * preact
        curve = jnp.tanh(preact * (GELU_A + (GELU_A * GELU_B) * square))
        rise = 0.5 * (1.0 + curve)
        act_ref[0] = (preact * rise).astype(BF)
        inner = GELU_A + (3.0 * GELU_A * GELU_B) * square
        slope_ref[0] = (rise + (0.5 * preact) * (1.0 - curve * curve) * inner).astype(BF)

    out = shaped((8, rows, length))
    spec = pl.BlockSpec((1, rows, length), lambda i: (i, 0, 0))
    return carry(
        body,
        [*pieces, normed, bias],
        [ANYWHERE] * 5 + [whole(normed), pl.BlockSpec((1, rows, 1), lambda i: (i, 0, 0))],
        [out, out],
        [spec, spec],
        8,
        "hidden_act",
        rides,
        scratch=stream.scratch,
        cost=8e9,
    )


def hidden_back(pieces, upstream, slope, rides=()):
    width, length = upstream.shape
    stream = Stream(pieces, False)
    rows = stream.count * stream.rows

    def body(p0, p1, p2, p3, p4, g_ref, slope_ref, d_ref, sum_ref, held, sems):
        weight = stream.bring((p0, p1, p2, p3, p4), held, sems)
        d_pre = (dot_nn(weight, g_ref[...]) * slope_ref[0].astype(F32)).astype(BF)
        d_ref[0] = d_pre
        sum_ref[0] = jnp.sum(d_pre.astype(F32), axis=1, keepdims=True)

    spec = pl.BlockSpec((1, rows, length), lambda i: (i, 0, 0))
    return carry(
        body,
        [*pieces, upstream, slope],
        [ANYWHERE] * 5 + [whole(upstream), spec],
        [shaped((8, rows, length)), shaped((8, rows, 1), F32)],
        [spec, pl.BlockSpec((1, rows, 1), lambda i: (i, 0, 0))],
        8,
        "hidden_back",
        rides,
        scratch=stream.scratch,
        cost=8e9,
    )


def weight_rows(rows, other, half, lanes, plus=None, rides=(), name="weight_rows"):
    _, count, length = rows.shape
    width = other.shape[0]
    unit = count // lanes

    def body(a_ref, b_ref, *refs):
        sums = contract_cols(a_ref[0], b_ref[...])
        if plus is not None:
            sums = sums + refs[0][0].reshape(count, width).astype(F32)
        refs[-1][0] = sums.astype(BF).reshape(lanes, unit, width)

    spec = pl.BlockSpec((1, lanes, unit, width), lambda i: (i, 0, 0, 0))
    extra = [] if plus is None else [plus]
    return carry(
        body,
        [rows, other] + extra,
        [pl.BlockSpec((1, count, length), lambda i: (2 * i + half, 0, 0)), whole(other)]
        + [spec] * len(extra),
        [shaped((4, lanes, unit, width))],
        [spec],
        4,
        name,
        rides,
        cost=2 * 4 * count * length * width,
    )


def norm_back(grad, unit_values, inverse, gain):
    scaled = grad * gain
    mean = lambda values: jnp.mean(values, axis=0, keepdims=True)
    return inverse * (scaled - mean(scaled) - unit_values * mean(scaled * unit_values))


def stream_back(pieces, values, rows, name, more, more_specs, outs, finish, rides):
    width = pieces[0].shape[-1]
    length = values.shape[-1]
    stream = Stream(pieces, True, rows)
    depth = 2 * stream.count * stream.rows
    count_more = len(more)

    def body(p0, p1, p2, p3, p4, d_ref, *refs):
        step = pl.program_id(0)
        more_refs, refs = refs[:count_more], refs[count_more:]
        out_refs, (acc, held, sems) = refs[: len(outs)], refs[len(outs) :]
        weight = stream.bring((p0, p1, p2, p3, p4), held, sems)
        part = contract_rows(weight, d_ref[...].reshape(depth, length))

        @pl.when(step == 0)
        def _():
            acc[...] = part

        @pl.when(step > 0)
        def _():
            acc[...] += part

        @pl.when(step == stream.steps - 1)
        def _():
            finish(acc[...], more_refs, out_refs)

    lead = values.shape[0] // stream.steps
    tail = (0,) * (values.ndim - 1)
    return carry(
        body,
        [*pieces, values, *more],
        [ANYWHERE] * 5
        + [pl.BlockSpec((lead, *values.shape[1:]), lambda i: (i, *tail))]
        + list(more_specs),
        outs,
        [whole(each) for each in outs],
        stream.steps,
        name,
        rides,
        scratch=[pltpu.VMEM((width, length), F32)] + stream.scratch,
        cost=2 * 4 * depth * width * length,
    )


def attend_back_body(qkv_ref, do_ref, o_ref, lse_ref, d_ref, sum_ref, dk_acc, dv_acc):
    queries_all, keys_t, values_t = qkv_ref[0, 0], qkv_ref[0, 1], qkv_ref[0, 2]
    keys = keys_t.T
    values = values_t.T
    length = queries_all.shape[1]
    scale = 1.0 / math.sqrt(HD)
    for start in range(0, length, QUERY_BLOCK):
        block = slice(start, min(start + QUERY_BLOCK, length))
        queries_t = qkv_ref[0, 0, :, block]
        pull_t = do_ref[0, :, block]
        delta = jnp.sum(
            pull_t.astype(F32) * o_ref[0, :, block].astype(F32), axis=0, keepdims=True
        )
        probs = jnp.exp2(dot_nn(keys, queries_t) - lse_ref[0, :, block])
        probs_low = probs.astype(BF)
        d_probs = dot_nn(values, pull_t)
        d_scores = (probs * (d_probs - delta)).astype(BF)
        d_ref[0, 0, :, block] = (dot_nn(keys_t, d_scores) * scale).astype(BF)
        d_keys = dot_nn(d_scores, queries_t.T)
        d_values = dot_nn(probs_low, pull_t.T)
        if start == 0:
            dk_acc[...] = d_keys
            dv_acc[...] = d_values
        else:
            dk_acc[...] += d_keys
            dv_acc[...] += d_values
    d_ref[0, 1] = (dk_acc[...].T * LN2).astype(BF)
    d_ref[0, 2] = dv_acc[...].T.astype(BF)
    for k in (0, 2):
        sum_ref[0, k // 2] = jnp.sum(d_ref[0, k].astype(F32), axis=1, keepdims=True)


def attend_back(qkv, pull, mixed, lse, first, heads, rides=()):
    _, _, _, length = qkv.shape
    flat = pl.BlockSpec((1, HD, length), lambda n: (n + first, 0, 0))
    return carry(
        attend_back_body,
        [qkv, pull, mixed, lse],
        [
            pl.BlockSpec((1, 3, HD, length), lambda n: (n + first, 0, 0, 0)),
            flat,
            flat,
            pl.BlockSpec((1, 1, length), lambda n: (n + first, 0, 0)),
        ],
        [shaped((heads, 3, HD, length)), shaped((heads, 2, HD, 1), F32)],
        [
            pl.BlockSpec((1, 3, HD, length), lambda n: (n, 0, 0, 0)),
            pl.BlockSpec((1, 2, HD, 1), lambda n: (n, 0, 0, 0)),
        ],
        heads,
        "attend_back",
        rides,
        scratch=[pltpu.VMEM((length, HD), F32), pltpu.VMEM((length, HD), F32)],
        cost=heads * 2.5e9,
    )


def head_pull(weight, values, rides=()):
    width, length = values.shape
    rows = width // 4

    def body(w_ref, d_ref, o_ref):
        o_ref[...] = dot_nn(w_ref[...], d_ref[...]).reshape(4, HD, length).astype(BF)

    return carry(
        body,
        [weight, values],
        [pl.BlockSpec((rows, width), lambda i: (i, 0)), whole(values)],
        [shaped((16, HD, length))],
        [pl.BlockSpec((4, HD, length), lambda i: (i, 0, 0))],
        4,
        "head_pull",
        rides,
        cost=2e9,
    )


def turned(values, axis, bit):
    return jnp.where(bit == 1, lax.rev(values, (axis,)), values)


def whole_image(
    images,
    counts,
    ln1_gain,
    ln1_bias,
    qkv_weight,
    qv_bias,
    out_weight,
    out_bias,
    ln2_gain,
    ln2_bias,
    fc1_weight,
    fc1_bias,
    fc2_weight,
    fc2_bias,
    grad_out,
):
    carry.count = 0
    slot_count, length, width = images.shape
    share = width // 4
    hidden = fc1_weight.shape[1]
    unit = -(-hidden // 64) * 16
    half_hidden = 2 * unit
    place_t = lax.axis_index("tensor")
    place_d = lax.axis_index("dp")
    core = lax.rem(place_d, 2)
    bit_x = lax.rem(place_t, 2)
    bit_y = place_t // 2
    block = 3 * HD

    def own_halves(rows):
        return turned(rows, 0, core)

    qkv_rows = qkv_weight.reshape(3, width, 2, 2, HD).transpose(2, 3, 0, 4, 1)
    attn_own = own_halves(
        jnp.concatenate(
            [qkv_rows.reshape(2, 2, block, width), out_weight.reshape(2, 2, HD, width)], axis=2
        )
    )
    pad = 4 * unit - hidden
    fc1_own, fc2_own = (
        own_halves(jnp.pad(rows, ((0, pad), (0, 0))).reshape(2, 2, unit, width))
        for rows in (fc1_weight.T, fc2_weight)
    )

    bias_row = jnp.concatenate(
        [
            qv_bias.reshape(2, 2, 2, HD).transpose(1, 2, 0, 3).reshape(1, -1),
            jnp.zeros((1, 2 * half_hidden - 2 * share), BF),
            fc1_bias[None],
            jnp.zeros((1, pad), BF),
        ],
        axis=1,
    ).reshape(2, 2 * half_hidden)
    bias_all = jnp.stack(
        [bias_row]
        + [
            lax.ppermute(bias_row, "tensor", [(i, i ^ turn) for i in range(4)])
            for turn in (1, 2, 3)
        ]
    ).astype(F32)
    qv_all = turned(bias_all[:, 0, : 2 * share].reshape(4, 2, 2, 2, HD), 1, core)
    qv_all = qv_all.reshape(16, 2, HD)
    qkv_bias = jnp.stack([qv_all[:, 0], jnp.zeros_like(qv_all[:, 0]), qv_all[:, 1]], axis=1)
    qkv_bias = qkv_bias.reshape(16, block, 1)
    qkv_scale = jnp.repeat(
        jnp.array([LOG2E / math.sqrt(HD), 1.0, 1.0], F32), HD, total_repeat_length=block
    )[:, None]
    hidden_bias = turned(bias_all[:, 1].reshape(4, 2, half_hidden), 1, core)
    hidden_bias = hidden_bias.reshape(8, half_hidden, 1)
    vectors = jnp.stack(
        [ln1_gain, ln1_bias, out_bias, ln2_gain, ln2_bias, fc2_bias, fc2_bias, fc2_bias], axis=1
    ).astype(F32)

    live = (place_t < counts[0]).astype(jnp.int32)
    live_scale = live.astype(F32).reshape(1, 1)

    (picture, upstream, normed_one, stats_one), attn_far = prepare(
        images,
        grad_out,
        place_t[None].astype(jnp.int32),
        live[None],
        ln1_gain.astype(F32)[None],
        ln1_bias.astype(F32)[None],
        [GatherRide(attn_own, (0, 5))],
    )
    attn = [attn_own, *attn_far]
    (qkv, mixed, lse), fc1_far = attend(
        attn, normed_one, qkv_bias, qkv_scale, [GatherRide(fc1_own, (0, 6))]
    )
    fc1 = [fc1_own, *fc1_far]
    ((residual, normed_two, stats_two, out_all),) = project_out(attn, mixed, picture, vectors)
    (activated, slope), fc2_far = hidden_act(
        fc1, normed_two, hidden_bias, [GatherRide(fc2_own, (0, 6))]
    )
    fc2 = [fc2_own, *fc2_far]

    ((fc2_part,),) = weight_rows(activated, upstream, 1, 2)
    (d_pre, hidden_sums), (fc2_got,) = hidden_back(fc2, upstream, slope, [SwapRide(fc2_part)])
    ((fc2_mine,),) = weight_rows(activated, upstream, 0, 2, fc2_got)
    (fc1_part,), (fc2_plane,) = weight_rows(d_pre, normed_two, 1, 2, rides=[PlaneRide(fc2_mine, 3)])

    def finish_two(grad, more, outs):
        h_ref, s_ref, g_ref, v_ref = more
        d_ref, low_ref, sum_ref = outs
        units = (h_ref[...] - s_ref[0:1, :]) * s_ref[1:2, :]
        d_residual = g_ref[...].astype(F32) + norm_back(grad, units, s_ref[1:2, :], v_ref[:, 3:4])
        d_ref[...] = d_residual
        low_ref[...] = d_residual.astype(BF)
        total = lambda values: jnp.sum(values, axis=1, keepdims=True)
        sum_ref[:, 0:1] = total(d_residual)
        sum_ref[:, 1:2] = total(grad * units)
        sum_ref[:, 2:3] = total(grad)
        sum_ref[:, 3:4] = total(g_ref[...].astype(F32))

    more = [residual, stats_two, upstream, vectors]
    (d_residual, d_low, sums_two), (fc1_got,), (fc2_mine_sum, fc2_other_sum) = stream_back(
        fc1,
        d_pre,
        None,
        "back_fc1",
        more,
        [whole(each) for each in more],
        [shaped((width, length), F32), shaped((width, length)), shaped((width, 4), F32)],
        finish_two,
        [SwapRide(fc1_part), LineRide(fc2_plane, (2, 3))],
    )
    ((fc1_mine,),) = weight_rows(d_pre, normed_two, 0, 2, fc1_got)
    ((pull,),) = head_pull(out_all, d_low)
    mixed_rows = mixed.reshape(8, 2 * HD, length)
    ((out_part,),) = weight_rows(mixed_rows, d_low, 1, 2)
    (d_qkv_a, qv_sums_a), (fc1_plane,), (out_got,) = attend_back(
        qkv, pull, mixed, lse, 0, 8, [PlaneRide(fc1_mine, 4), SwapRide(out_part)]
    )
    ((out_mine,),) = weight_rows(mixed_rows, d_low, 0, 2, out_got)
    (d_qkv_b, qv_sums_b), (fc1_mine_sum, fc1_other_sum), (out_plane,) = attend_back(
        qkv, pull, mixed, lse, 8, 8, [LineRide(fc1_plane, (3, 6)), PlaneRide(out_mine, 4)]
    )
    d_qkv = jnp.concatenate([d_qkv_a, d_qkv_b])
    d_rows = d_qkv.reshape(8, 2 * block, length)
    ((qkv_part,),) = weight_rows(d_rows, normed_one, 1, 2)

    def finish_block(total, more, outs):
        h_ref, v_ref, live_ref = more
        rows = (h_ref[...] + total + v_ref[:, 5:6]) * live_ref[...]
        outs[0][...] = rows.astype(BF).reshape(4, share, length)

    more = [residual, vectors, live_scale]
    (block_rows,), (qkv_got,), (out_mine_sum, out_other_sum) = stream_back(
        fc2,
        activated,
        None,
        "block_out",
        more,
        [whole(each) for each in more],
        [shaped((4, share, length))],
        finish_block,
        [SwapRide(qkv_part), LineRide(out_plane, (2, 3))],
    )
    ((qkv_mine,),) = weight_rows(d_rows, normed_one, 0, 2, qkv_got)

    def finish_one(grad, more, outs):
        x_ref, s_ref, d_ref, v_ref = more
        units = (x_ref[...].astype(F32) - s_ref[0:1, :]) * s_ref[1:2, :]
        d_input = d_ref[...] + norm_back(grad, units, s_ref[1:2, :], v_ref[:, 0:1])
        outs[0][...] = d_input.astype(BF).reshape(4, share, length)
        outs[1][:, 0:1] = jnp.sum(grad * units, axis=1, keepdims=True)
        outs[1][:, 1:2] = jnp.sum(grad, axis=1, keepdims=True)

    more = [picture, stats_one, d_residual, vectors]
    (input_rows, sums_one), (qkv_plane,), (block_far,) = stream_back(
        attn,
        d_qkv,
        block,
        "back_one",
        more,
        [whole(each) for each in more],
        [shaped((4, share, length)), shaped((width, 2), F32)],
        finish_one,
        [PlaneRide(qkv_mine, 3), SpreadRide(block_rows)],
    )

    def absolute(values):
        values = values.reshape(2, 2, 2, *values.shape[2:])
        values = turned(turned(turned(values, 2, core), 0, bit_y), 1, bit_x)
        return values.reshape(4, -1)

    qv_sums = jnp.concatenate([qv_sums_a, qv_sums_b]).reshape(4, 2, -1)
    wide = jnp.concatenate([sums_one, sums_two], axis=1).reshape(4, share, 6)
    wide = wide.transpose(0, 2, 1).reshape(4, 6 * share)
    sums = jnp.concatenate(
        [wide, absolute(qv_sums), absolute(hidden_sums.reshape(4, 2, half_hidden))], axis=1
    )
    sums = jnp.pad(sums, ((0, 0), (0, -sums.shape[1] % 128)))

    def nothing(*refs):
        refs[-1][...] = jnp.zeros(refs[-1].shape, F32)

    _, (qkv_mine_sum, qkv_other_sum), (input_far,), (sums,) = carry(
        nothing,
        [live_scale],
        [whole(live_scale)],
        [shaped((8, 128), F32)],
        [whole(shaped((8, 128), F32))],
        1,
        "last",
        [LineRide(qkv_plane, (0, 0)), SpreadRide(input_rows), VectorRide(sums)],
    )
    own = lax.dynamic_index_in_dim(sums, place_t, 0, keepdims=False)
    own_wide = own[: 6 * share].reshape(6, share)
    own_qv = own[6 * share : 8 * share].reshape(4, 2, HD).transpose(1, 0, 2).reshape(2, share)
    own_hidden = own[8 * share : 8 * share + hidden]

    def columns(rows, far):
        result = jnp.zeros((slot_count, share, length), F32)
        pieces = [lax.dynamic_index_in_dim(rows, place_t, 0, keepdims=False)]
        pieces += [far[r] for r in range(3)]
        for r, piece in enumerate(pieces):
            result = lax.dynamic_update_index_in_dim(result, piece.astype(F32), place_t ^ r, 0)
        return result.transpose(0, 2, 1)

    def ordered(mine, other):
        return jnp.stack([jnp.where(core == 0, mine, other), jnp.where(core == 0, other, mine)])

    fc2_result = ordered(fc2_mine_sum, fc2_other_sum).reshape(-1, width)[:hidden].astype(F32)
    fc1_result = ordered(fc1_mine_sum, fc1_other_sum).reshape(-1, width)[:hidden].T.astype(F32)
    out_result = ordered(out_mine_sum, out_other_sum).reshape(share, width).astype(F32)
    qkv_result = ordered(qkv_mine_sum, qkv_other_sum).reshape(2, 2, 3, HD, width)
    qkv_result = qkv_result.transpose(2, 4, 0, 1, 3).reshape(3, width, share).astype(F32)
    return (
        columns(block_rows, block_far),
        columns(input_rows, input_far),
        own_wide[0],
        own_wide[1],
        qkv_result,
        own_qv,
        out_result,
        own_wide[2],
        own_wide[3],
        own_wide[4],
        fc1_result,
        own_hidden,
        fc2_result,
        own_wide[5],
    )


def solution(mesh):
    whole_fits = mesh.shape["tensor"] == 4 and mesh.shape["dp"] == 8
    return jax.shard_map(
        whole_image if whole_fits else local,
        mesh=mesh,
        in_specs=(
            P("dp", None, None),
            P("dp"),
            P(),
            P(),
            P(None, None, "tensor"),
            P(None, "tensor"),
            P("tensor", None),
            P(),
            P(),
            P(),
            P(None, "tensor"),
            P("tensor"),
            P("tensor", None),
            P(),
            P("dp", None, None),
        ),
        out_specs=(
            P("dp", None, "tensor"),
            P("dp", None, "tensor"),
            P("tensor"),
            P("tensor"),
            P(None, None, "tensor"),
            P(None, "tensor"),
            P("tensor", None),
            P("tensor"),
            P("tensor"),
            P("tensor"),
            P(None, "tensor"),
            P("tensor"),
            P("tensor", None),
            P("tensor"),
        ),
        check_vma=False,
    )
```

```python
import math

import jax
import jax.numpy as jnp
from jax import lax
from jax.experimental import pallas as pl
from jax.experimental.pallas import tpu as pltpu
from jax.sharding import PartitionSpec as P

HD = 72


EPS = 1e-06


def own_columns(values, share_width):
    start = lax.axis_index(TENSOR) * share_width
    return lax.dynamic_slice_in_dim(values, start, share_width, values.ndim - 1)


def row_mean(values):
    return jnp.mean(values, axis=-1, keepdims=True)


def group_stats(first, second):
    return lax.psum((first, second), TENSOR)


def contract_rows(left, right):
    return lax.dot_general(
        left, right, (((0,), (0,)), ((), ())), preferred_element_type=jnp.float32
    )


def contract_cols(left, right):
    return lax.dot_general(
        left, right, (((1,), (1,)), ((), ())), preferred_element_type=jnp.float32
    )


def gelu_tanh(values):
    return jax.nn.gelu(values, approximate=True)


def local(
    images,
    counts,
    ln1_gain,
    ln1_bias,
    qkv_weight,
    qv_bias,
    out_weight,
    out_bias,
    ln2_gain,
    ln2_bias,
    fc1_weight,
    fc1_bias,
    fc2_weight,
    fc2_bias,
    grad_out,
):
    slot_count, length, full_width = images.shape
    share_width = full_width // lax.axis_size(TENSOR)
    local_width = qkv_weight.shape[2]
    local_heads = local_width // HD
    hidden_width = fc1_weight.shape[1]
    score_scale = 1.0 / math.sqrt(HD)
    gain_one = ln1_gain.astype(jnp.float32)
    shift_one = ln1_bias.astype(jnp.float32)
    gain_two = ln2_gain.astype(jnp.float32)
    shift_two = ln2_bias.astype(jnp.float32)
    bias_out = out_bias.astype(jnp.float32)
    bias_fc1 = fc1_bias.astype(jnp.float32)
    bias_fc2 = fc2_bias.astype(jnp.float32)
    bias_query = qv_bias[0].astype(jnp.float32)
    bias_value = qv_bias[1].astype(jnp.float32)
    live_count = counts[0]

    def to_heads(values):
        return values.reshape(length, local_heads, HD)

    def head_scores(query_heads, key_heads):
        return (
            jnp.einsum("qhd,khd->hqk", query_heads, key_heads, preferred_element_type=jnp.float32)
            * score_scale
        )

    def layer_step(slot_index, loop_state):
        block_acc, input_acc, grads = loop_state
        (
            grad_gain_one,
            grad_shift_one,
            grad_qkv,
            grad_qv,
            grad_out_w,
            grad_out_b,
            grad_gain_two,
            grad_shift_two,
            grad_fc1_w,
            grad_fc1_b,
            grad_fc2_w,
            grad_fc2_b,
        ) = grads
        live_flag = (slot_index < live_count).astype(jnp.float32)
        picture = lax.dynamic_index_in_dim(images, slot_index, 0, keepdims=False).astype(
            jnp.float32
        )
        upstream = (
            lax.dynamic_index_in_dim(grad_out, slot_index, 0, keepdims=False).astype(jnp.float32)
            * live_flag
        )
        upstream_low = upstream.astype(jnp.bfloat16)
        centered = picture - row_mean(picture)
        inv_one = lax.rsqrt(row_mean(centered * centered) + EPS)
        unit_one = centered * inv_one
        normed_one = (unit_one * gain_one + shift_one).astype(jnp.bfloat16)
        query_rows = (
            jnp.dot(normed_one, qkv_weight[0], preferred_element_type=jnp.float32) + bias_query
        ).astype(jnp.bfloat16)
        key_rows = jnp.dot(normed_one, qkv_weight[1], preferred_element_type=jnp.float32).astype(
            jnp.bfloat16
        )
        value_rows = (
            jnp.dot(normed_one, qkv_weight[2], preferred_element_type=jnp.float32) + bias_value
        ).astype(jnp.bfloat16)
        query_heads = to_heads(query_rows)
        key_heads = to_heads(key_rows)
        value_heads = to_heads(value_rows)
        scores = head_scores(query_heads, key_heads)
        row_top = jnp.max(scores, axis=-1, keepdims=True)
        logsum = row_top + jnp.log(jnp.sum(jnp.exp(scores - row_top), axis=-1, keepdims=True))
        probs_low = jnp.exp(scores - logsum).astype(jnp.bfloat16)
        mixed = jnp.einsum(
            "hqk,khd->qhd", probs_low, value_heads, preferred_element_type=jnp.float32
        )
        mixed = mixed.reshape(length, local_width).astype(jnp.bfloat16)
        partial_out = jnp.dot(mixed, out_weight, preferred_element_type=jnp.float32).astype(
            jnp.bfloat16
        )
        residual = (
            own_columns(picture, share_width)
            + lax.psum_scatter(partial_out, TENSOR, scatter_dimension=1, tiled=True).astype(
                jnp.float32
            )
            + own_columns(bias_out, share_width)
        )
        row_sum, row_square = group_stats(
            jnp.sum(residual, axis=-1), jnp.sum(residual * residual, axis=-1)
        )
        average = row_sum[:, None] / full_width
        inv_two = lax.rsqrt(row_square[:, None] / full_width - average * average + EPS)
        unit_two = (residual - average) * inv_two
        own_normed = (
            unit_two * own_columns(gain_two, share_width) + own_columns(shift_two, share_width)
        ).astype(jnp.bfloat16)
        normed_two = lax.all_gather(own_normed, TENSOR, axis=1, tiled=True)
        preact = jnp.dot(normed_two, fc1_weight, preferred_element_type=jnp.float32) + bias_fc1
        activated = gelu_tanh(preact).astype(jnp.bfloat16)
        partial_mlp = jnp.dot(activated, fc2_weight, preferred_element_type=jnp.float32).astype(
            jnp.bfloat16
        )
        block_rows = (
            residual
            + lax.psum_scatter(partial_mlp, TENSOR, scatter_dimension=1, tiled=True).astype(
                jnp.float32
            )
            + own_columns(bias_fc2, share_width)
        )
        block_rows = block_rows * live_flag
        grad_fc2_b = grad_fc2_b + own_columns(jnp.sum(upstream, axis=0), share_width)
        grad_fc2_w = grad_fc2_w + contract_rows(activated, upstream_low)
        d_act = contract_cols(upstream_low, fc2_weight)
        gelu_pull = jax.vjp(gelu_tanh, preact)[1]
        d_pre = gelu_pull(d_act)[0].astype(jnp.bfloat16)
        grad_fc1_b = grad_fc1_b + jnp.sum(d_pre.astype(jnp.float32), axis=0)
        grad_fc1_w = grad_fc1_w + contract_rows(normed_two, d_pre)
        back_mlp = contract_cols(d_pre, fc1_weight)
        d_norm_two = lax.psum_scatter(
            back_mlp.astype(jnp.bfloat16), TENSOR, scatter_dimension=1, tiled=True
        ).astype(jnp.float32)
        scaled_two = d_norm_two * own_columns(gain_two, share_width)
        sum_plain, sum_cross = group_stats(
            jnp.sum(scaled_two, axis=-1), jnp.sum(scaled_two * unit_two, axis=-1)
        )
        d_residual = own_columns(upstream, share_width) + inv_two * (
            scaled_two
            - sum_plain[:, None] / full_width
            - unit_two * (sum_cross[:, None] / full_width)
        )
        grad_gain_two = grad_gain_two + jnp.sum(d_norm_two * unit_two, axis=0)
        grad_shift_two = grad_shift_two + jnp.sum(d_norm_two, axis=0)
        grad_out_b = grad_out_b + jnp.sum(d_residual, axis=0)
        d_residual_low = lax.all_gather(
            d_residual.astype(jnp.bfloat16), TENSOR, axis=1, tiled=True
        )
        grad_out_w = grad_out_w + contract_rows(mixed, d_residual_low)
        d_mixed_heads = to_heads(contract_cols(d_residual_low, out_weight).astype(jnp.bfloat16))
        probs = jnp.exp(head_scores(query_heads, key_heads) - logsum)
        probs_again = probs.astype(jnp.bfloat16)
        d_value = jnp.einsum(
            "hqk,qhd->khd", probs_again, d_mixed_heads, preferred_element_type=jnp.float32
        )
        d_probs = jnp.einsum(
            "qhd,khd->hqk", d_mixed_heads, value_heads, preferred_element_type=jnp.float32
        )
        inner = jnp.sum(probs * d_probs, axis=-1, keepdims=True)
        d_scores = (probs * (d_probs - inner)).astype(jnp.bfloat16)
        d_query = (
            jnp.einsum("hqk,khd->qhd", d_scores, key_heads, preferred_element_type=jnp.float32)
            * score_scale
        )
        d_key = (
            jnp.einsum("hqk,qhd->khd", d_scores, query_heads, preferred_element_type=jnp.float32)
            * score_scale
        )
        d_stack = (
            jnp.stack([d_query, d_key, d_value], axis=1)
            .reshape(length, 3, local_width)
            .astype(jnp.bfloat16)
        )
        grad_qkv = grad_qkv + jnp.einsum(
            "ld,lje->jde", normed_one, d_stack, preferred_element_type=jnp.float32
        )
        bias_sums = jnp.sum(d_stack.astype(jnp.float32), axis=0)
        grad_qv = grad_qv + jnp.stack([bias_sums[0], bias_sums[2]])
        back_attn = jnp.einsum(
            "lje,jde->ld", d_stack, qkv_weight, preferred_element_type=jnp.float32
        )
        d_norm_one = lax.psum_scatter(
            back_attn.astype(jnp.bfloat16), TENSOR, scatter_dimension=1, tiled=True
        ).astype(jnp.float32)
        own_unit = own_columns(unit_one, share_width)
        scaled_one = d_norm_one * own_columns(gain_one, share_width)
        plain_one, cross_one = group_stats(
            jnp.sum(scaled_one, axis=-1), jnp.sum(scaled_one * own_unit, axis=-1)
        )
        d_input = d_residual + inv_one * (
            scaled_one
            - plain_one[:, None] / full_width
            - own_unit * (cross_one[:, None] / full_width)
        )
        grad_gain_one = grad_gain_one + jnp.sum(d_norm_one * own_unit, axis=0)
        grad_shift_one = grad_shift_one + jnp.sum(d_norm_one, axis=0)
        block_acc = lax.dynamic_update_index_in_dim(block_acc, block_rows, slot_index, 0)
        input_acc = lax.dynamic_update_index_in_dim(input_acc, d_input, slot_index, 0)
        new_grads = (
            grad_gain_one,
            grad_shift_one,
            grad_qkv,
            grad_qv,
            grad_out_w,
            grad_out_b,
            grad_gain_two,
            grad_shift_two,
            grad_fc1_w,
            grad_fc1_b,
            grad_fc2_w,
            grad_fc2_b,
        )
        return (block_acc, input_acc, new_grads)

    share_zeros = jnp.zeros((share_width,), jnp.float32)
    start_grads = (
        share_zeros,
        share_zeros,
        jnp.zeros((3, full_width, local_width), jnp.float32),
        jnp.zeros((2, local_width), jnp.float32),
        jnp.zeros((local_width, full_width), jnp.float32),
        share_zeros,
        share_zeros,
        share_zeros,
        jnp.zeros((full_width, hidden_width), jnp.float32),
        jnp.zeros((hidden_width,), jnp.float32),
        jnp.zeros((hidden_width, full_width), jnp.float32),
        share_zeros,
    )
    start_rows = jnp.zeros((slot_count, length, share_width), jnp.float32)
    block_acc, input_acc, grads = lax.fori_loop(
        0, slot_count, layer_step, (start_rows, start_rows, start_grads)
    )
    (
        grad_gain_one,
        grad_shift_one,
        grad_qkv,
        grad_qv,
        grad_out_w,
        grad_out_b,
        grad_gain_two,
        grad_shift_two,
        grad_fc1_w,
        grad_fc1_b,
        grad_fc2_w,
        grad_fc2_b,
    ) = grads
    summed = (
        lax.psum(grad_gain_one.astype(jnp.bfloat16), DP).astype(jnp.float32),
        lax.psum(grad_shift_one.astype(jnp.bfloat16), DP).astype(jnp.float32),
        lax.psum(grad_qkv.astype(jnp.bfloat16), DP).astype(jnp.float32),
        lax.psum(grad_qv.astype(jnp.bfloat16), DP).astype(jnp.float32),
        lax.psum(grad_out_w.astype(jnp.bfloat16), DP).astype(jnp.float32),
        lax.psum(grad_out_b.astype(jnp.bfloat16), DP).astype(jnp.float32),
        lax.psum(grad_gain_two.astype(jnp.bfloat16), DP).astype(jnp.float32),
        lax.psum(grad_shift_two.astype(jnp.bfloat16), DP).astype(jnp.float32),
        lax.psum(grad_fc1_w.astype(jnp.bfloat16), DP).astype(jnp.float32),
        lax.psum(grad_fc1_b.astype(jnp.bfloat16), DP).astype(jnp.float32),
        lax.psum(grad_fc2_w.astype(jnp.bfloat16), DP).astype(jnp.float32),
        lax.psum(grad_fc2_b.astype(jnp.bfloat16), DP).astype(jnp.float32),
    )
    return (
        block_acc,
        input_acc,
        summed[0],
        summed[1],
        summed[2],
        summed[3],
        summed[4],
        summed[5],
        summed[6],
        summed[7],
        summed[8],
        summed[9],
        summed[10],
        summed[11],
    )


LOG2E = math.log2(math.e)
LN2 = math.log(2.0)
GELU_A = math.sqrt(2.0 / math.pi)
GELU_B = 0.044715
BF = jnp.bfloat16
F32 = jnp.float32
QUERY_BLOCK = 256
MESH = pl.DeviceIdType.MESH
TENSOR, DP = "tensor", "dp"
X, Y, XY, CORE, LINE = range(5)
TURN = {X: 1, Y: 2, XY: 3}
OTHER = {X: Y, Y: X}
SIDE = {X: 0, Y: 1}
LANES = (X, Y)
FC2, FC1, OUT, QKV = range(4)
INWARD, ACROSS, BACK, SWAP = range(4)


class Bag:
    def __init__(self, **things):
        self.__dict__.update(things)

    def each(self, action):
        return Bag(**{name: action(thing) for name, thing in self.__dict__.items()})
ANYWHERE = pl.BlockSpec(memory_space=pl.ANY)


def dot_nn(left, right):
    return lax.dot_general(left, right, (((1,), (0,)), ((), ())), preferred_element_type=F32)


def place(bit):
    if bit == CORE:
        return {DP: lax.axis_index(DP) ^ 1}
    return {TENSOR: lax.axis_index(TENSOR) ^ TURN[bit]}


def hop(source, target, sems, index, to):
    return pltpu.make_async_remote_copy(
        src_ref=source,
        dst_ref=target,
        send_sem=sems.at[0, index],
        recv_sem=sems.at[1, index],
        device_id=place(to) if isinstance(to, int) else to,
        device_id_type=MESH,
    )


def line_place():
    dp = lax.axis_index(DP)
    return dp // 2, {DP: lax.rem(dp + 2, 8)}, {DP: lax.rem(dp + 6, 8)}


class Program:
    def __init__(self, name, partners):
        self.name = name
        self.partners = partners
        self.arrays, self.specs, self.shapes, self.scratches = [], [], [], []

    def input(self, array, spec=ANYWHERE):
        self.arrays.append(array)
        self.specs.append(spec)
        return (0, len(self.arrays) - 1)

    def output(self, *shape, dtype=BF):
        self.shapes.append(jax.ShapeDtypeStruct(shape, dtype))
        return (1, len(self.shapes) - 1)

    def scratch(self, spec):
        self.scratches.append(spec)
        return (2, len(self.scratches) - 1)

    def tile(self, *shape, dtype=BF):
        return self.scratch(pltpu.VMEM(shape, dtype))

    def sems(self, *shape):
        return self.scratch(pltpu.SemaphoreType.DMA(shape))

    def call(self, script, collective_id, cost):
        count_in, count_out = len(self.arrays), len(self.shapes)

        def kernel(*refs):
            pools = (
                refs[:count_in],
                refs[count_in : count_in + count_out],
                refs[count_in + count_out :],
            )
            meet(self.partners)
            script(lambda handle: pools[handle[0]][handle[1]])

        results = pl.pallas_call(
            kernel,
            in_specs=self.specs,
            out_specs=[ANYWHERE] * count_out,
            out_shape=self.shapes,
            scratch_shapes=self.scratches,
            compiler_params=pltpu.CompilerParams(
                vmem_limit_bytes=63 << 20, collective_id=collective_id, has_side_effects=True
            ),
            cost_estimate=pl.CostEstimate(
                flops=int(cost), bytes_accessed=1 << 26, transcendentals=0
            ),
            name=self.name,
        )(*self.arrays)
        return lambda handle: results[handle[1]]


def meet(partners):
    barrier = pltpu.get_barrier_semaphore()
    signal = lambda at: pl.semaphore_signal(barrier, inc=1, device_id=at, device_id_type=MESH)
    for bit in partners:
        if bit == XY:
            signal({TENSOR: lax.axis_index(TENSOR) ^ 3})
        elif bit != LINE:
            signal(place(bit))
    singles = len([bit for bit in partners if bit != LINE])
    if LINE in partners:
        z, up, down = line_place()
        pl.when(z < 3)(lambda: signal(up))
        pl.when(z > 0)(lambda: signal(down))
        inner = jnp.logical_and(z > 0, z < 3)
        pl.when(inner)(lambda: pl.semaphore_wait(barrier, singles + 2))
        pl.when(jnp.logical_not(inner))(lambda: pl.semaphore_wait(barrier, singles + 1))
    else:
        pl.semaphore_wait(barrier, singles)


def phase(steps, body, ins, in_specs, outs, out_specs, events=()):
    def inner(at, *refs):
        step = at.index[0]
        for when, event in events:
            pl.when(step == when)(event)
        body(step, *refs)

    pltpu.emit_pipeline(
        inner, grid=(steps,), in_specs=in_specs, out_specs=out_specs, _explicit_indices=True
    )(*ins, *outs)


def fetch(source, target, sem):
    copy = pltpu.make_async_copy(source, target, sem)
    copy.start()
    return copy


def spec(shape, index):
    return pl.BlockSpec(shape, index)


class Gather:
    def __init__(self, program, own, shape, early=None):
        _, count, unit, width = shape
        self.own = own
        self.early = early
        self.near = program.output(2, count, unit, width)
        self.near_part = program.output(2, count, unit, width)
        self.far = program.output(count, unit, width)
        self.far_part = program.output(count, unit, width)
        self.sems = program.sems(2, 12)

    def bind(self, ref):
        self.refs = Bag(
            own=ref(self.own),
            near=ref(self.near),
            near_part=ref(self.near_part),
            far=ref(self.far),
            far_part=ref(self.far_part),
            sems=ref(self.sems),
            early=None if self.early is None else ref(self.early),
        )
        return self

    def piece(self, shard, part, lane):
        r = self.refs
        if shard == 0:
            return r.own.at[lax.rem(lax.axis_index(DP) + part, 2), lane]
        if shard == 3:
            return (r.far_part if part else r.far).at[lane]
        if self.early is not None and part == 0 and LANES[lane] == LANES[shard - 1]:
            return r.early.at[lane]
        return (r.near_part if part else r.near).at[shard - 1, lane]

    def _near(self, bit, lane):
        r = self.refs
        k = SIDE[bit]
        own = self.piece(0, 0, lane)
        return hop(own, r.near.at[k, lane], r.sems, 2 * lane + k, bit)

    def _far(self, lane):
        first = LANES[lane]
        source = self.piece(1 + SIDE[first], 0, lane)
        return hop(source, self.refs.far.at[lane], self.refs.sems, 4 + lane, OTHER[first])

    def _swap(self, shard, lane):
        target = self.piece(shard, 1, lane)
        index = 6 + 2 * (shard - 1) + lane
        return hop(self.piece(shard, 0, lane), target, self.refs.sems, index, CORE)

    def start(self):
        for first in (True, False):
            for lane, bit in enumerate(LANES):
                if first and self.early is None:
                    self._near(bit, lane).start()
                if not first:
                    self._near(OTHER[bit], lane).start()

    def forward(self):
        for lane, first in enumerate(LANES):
            if self.early is None:
                self._near(first, lane).wait_recv()
            self._far(lane).start()
            self._swap(1 + SIDE[first], lane).start()

    def near_here(self):
        for lane, first in enumerate(LANES):
            self._near(OTHER[first], lane).wait_recv()
            self._swap(1 + SIDE[OTHER[first]], lane).start()

    def near_whole(self):
        for lane in range(2):
            for shard in (1, 2):
                self._swap(shard, lane).wait_recv()

    def far_here(self):
        for lane in range(2):
            self._far(lane).wait_recv()
            self._swap(3, lane).start()

    def far_whole(self):
        for lane in range(2):
            self._swap(3, lane).wait_recv()

    def drain(self):
        for lane, first in enumerate(LANES):
            if self.early is None:
                self._near(first, lane).wait_send()
            self._near(OTHER[first], lane).wait_send()
            self._far(lane).wait_send()
            for shard in (1, 2, 3):
                self._swap(shard, lane).wait_send()


class Swap:
    def __init__(self, program, source, shape):
        self.source = source
        self.got = program.output(*shape)
        self.sems = program.sems(2, shape[0])

    def bind(self, ref):
        self.refs = ref(self.source), ref(self.got), ref(self.sems)
        return self

    def _hop(self, k):
        source, got, sems = self.refs
        return hop(source.at[k], got.at[k], sems, k, CORE)

    def start(self, *parts):
        for k in parts:
            self._hop(k).start()

    def wait(self, *parts):
        for k in parts:
            self._hop(k).wait()


class Plane:
    KEPT = {X: (0, 2), Y: (0, 1)}
    GONE = {X: (1, 3), Y: (2, 3)}

    def __init__(self, program, rows, shape):
        _, count, unit, width = shape
        self.rows = rows
        self.base = program.tile(count, 2, unit, width)
        self.got = program.tile(count, 2, unit, width)
        self.last = program.tile(count, unit, width)
        self.sems = program.sems(2, 6)
        self.local = program.sems(4)

    def bind(self, ref):
        self.refs = [ref(h) for h in (self.rows, self.base, self.got, self.last, self.sems)]
        self.loads = ref(self.local)
        return self

    def _first(self, lane, k):
        rows, base, got, last, sems = self.refs
        first = LANES[lane]
        return hop(
            rows.at[self.GONE[first][k], lane], got.at[lane, k], sems, 2 * lane + k, first
        )

    def _load(self, lane, k):
        rows, base = self.refs[:2]
        return pltpu.make_async_copy(
            rows.at[self.KEPT[LANES[lane]][k], lane], base.at[lane, k], self.loads.at[2 * lane + k]
        )

    def _next(self, lane):
        rows, base, got, last, sems = self.refs
        return hop(base.at[lane, 1], last.at[lane], sems, 4 + lane, OTHER[LANES[lane]])

    def send(self, shard):
        for lane, first in enumerate(LANES):
            if shard in self.GONE[first]:
                self._first(lane, self.GONE[first].index(shard)).start()
            else:
                self._load(lane, self.KEPT[first].index(shard)).start()

    def start(self):
        for shard in (3, 1, 2, 0):
            self.send(shard)

    def forward(self):
        rows, base, got, last, sems = self.refs
        for lane in range(2):
            self._load(lane, 1).wait()
            self._first(lane, 1).wait_recv()
            base[lane, 1] += got[lane, 1]
            self._next(lane).start()

    def settle(self):
        rows, base, got, last, sems = self.refs
        for lane in range(2):
            self._load(lane, 0).wait()
            self._first(lane, 0).wait_recv()
            base[lane, 0] += got[lane, 0]

    def finish(self, line):
        rows, base, got, last, sems = self.refs
        for lane in range(2):
            self._next(lane).wait_recv()
            line.take(lane, base[lane, 0] + last[lane])

    def drain(self):
        for lane in range(2):
            self._next(lane).wait_send()
            for k in range(2):
                self._first(lane, k).wait_send()


class Line:
    def __init__(self, program, shape):
        count, unit, width = shape
        self.total = program.output(*shape)
        self.other = program.output(*shape)
        self.held = program.tile(*shape)
        self.outer = program.tile(*shape)
        self.middle = program.tile(*shape)
        self.sems = program.sems(2, 4 * count)
        self.local = program.sems(count)
        self.count = count

    def bind(self, ref):
        self.refs = Bag(
            total=ref(self.total),
            other=ref(self.other),
            held=ref(self.held),
            outer=ref(self.outer),
            middle=ref(self.middle),
            sems=ref(self.sems),
            local=ref(self.local),
        )
        z, up, down = line_place()
        self.up, self.down = up, down
        self.is_outer = jnp.logical_or(z == 0, z == 3)
        self.is_inner = jnp.logical_not(self.is_outer)
        self.low = z < 2
        return self

    def _hop(self, kind, k, at):
        r = self.refs
        target = (r.outer, r.middle, r.outer, r.other)[kind]
        return hop(r.held.at[k], target.at[k], r.sems, kind * self.count + k, at)

    def _store(self, k):
        r = self.refs
        return pltpu.make_async_copy(r.held.at[k], r.total.at[k], r.local.at[k])

    def _send(self, kind, k):
        if kind == BACK:
            low, high = self.down, self.up
        else:
            low, high = self.up, self.down
        pl.when(self.low)(lambda: self._hop(kind, k, low).start())
        pl.when(jnp.logical_not(self.low))(lambda: self._hop(kind, k, high).start())

    def take(self, k, values):
        self.refs.held[k] = values
        pl.when(self.is_outer)(lambda: self._send(INWARD, k))

    def meet(self, k):
        r = self.refs

        @pl.when(self.is_inner)
        def _():
            self._hop(INWARD, k, self.up).wait_recv()
            r.held[k] += r.outer[k]
            self._send(ACROSS, k)

    def leave(self, k):
        r = self.refs

        @pl.when(self.is_inner)
        def _():
            self._hop(ACROSS, k, self.up).wait()
            r.held[k] += r.middle[k]
            self._send(BACK, k)
            self._hop(SWAP, k, CORE).start()
            self._store(k).start()

    def finish(self, k):
        r = self.refs

        @pl.when(self.is_outer)
        def _():
            self._hop(INWARD, k, self.up).wait_send()
            self._hop(BACK, k, self.up).wait_recv()
            r.held[k] = r.outer[k]
            self._hop(SWAP, k, CORE).start()
            self._store(k).start()

        pl.when(self.is_inner)(lambda: self._hop(BACK, k, self.up).wait_send())
        self._store(k).wait()
        self._hop(SWAP, k, CORE).wait()


class Spread:
    def __init__(self, program, rows, shape):
        self.rows = rows
        self.landed = program.output(3, *shape[1:])
        self.sems = program.sems(2, 3)

    def bind(self, ref):
        self.refs = ref(self.rows), ref(self.landed), ref(self.sems)
        return self

    def _hop(self, r):
        rows, landed, sems = self.refs
        to = lax.axis_index(TENSOR) ^ r
        return hop(rows.at[to], landed.at[r - 1], sems, r - 1, {TENSOR: to})

    def start(self):
        for r in (3, 1, 2):
            self._hop(r).start()

    def finish(self):
        for r in (1, 2, 3):
            self._hop(r).wait()


class Vectors:
    def __init__(self, program, shape):
        self.total = program.output(*shape, dtype=F32)
        self.held = program.tile(*shape, dtype=F32)
        self.got = program.tile(6, *shape, dtype=F32)
        self.sems = program.sems(2, 6)
        self.local = program.sems(1)

    def bind(self, ref):
        self.refs = Bag(
            total=ref(self.total),
            held=ref(self.held),
            got=ref(self.got),
            sems=ref(self.sems),
            local=ref(self.local),
        )
        return self

    def run(self):
        r = self.refs
        held, got = r.held, r.got
        z, up, down = line_place()
        is_outer = jnp.logical_or(z == 0, z == 3)
        low = z < 2
        step = lambda k, at: hop(held, got.at[k], r.sems, k, at)

        def towards(k, first, second):
            pl.when(low)(lambda: step(k, first).start())
            pl.when(jnp.logical_not(low))(lambda: step(k, second).start())

        for k, (bit, turn) in enumerate(((CORE, 1), (X, 2), (Y, 4))):
            step(k, bit).start()
            step(k, bit).wait()
            held[0:8] += got[k, 0:8]
            for p in range(8):
                held[8 + p] += got[k, 8 + (p ^ turn)]

        @pl.when(is_outer)
        def _():
            towards(3, up, down)
            step(3, up).wait_send()
            step(5, up).wait_recv()
            held[...] = got[5]

        @pl.when(jnp.logical_not(is_outer))
        def _():
            step(3, up).wait_recv()
            held[...] += got[3]
            towards(4, up, down)
            step(4, up).wait()
            held[...] += got[4]
            towards(5, down, up)
            step(5, up).wait_send()

        fetch(held, r.total, r.local.at[0]).wait()


class Stream:
    def __init__(self, program, group, unit, width):
        self.group, self.unit = group, unit
        self.held = program.tile(2, group, 2, unit, width)
        self.sems = program.sems(2, group * 2)

    def bind(self, ref):
        self.refs = ref(self.held), ref(self.sems)
        return self

    def _copies(self, gather, index, slot, size):
        held, sems = self.refs
        return [
            pltpu.make_async_copy(
                gather.piece((index * self.group + g) // 2, (index * self.group + g) % 2, c).at[
                    pl.ds(0, size)
                ],
                held.at[slot, g, c, pl.ds(0, size)],
                sems.at[slot, 2 * g + c],
            )
            for g in range(self.group)
            for c in range(2)
        ]

    def begin(self, gather, index, size=None):
        for each in self._copies(gather, index, index % 2, size or self.unit):
            each.start()

    def bring(self, gather, step, first, last, size=None):
        size = size or self.unit
        for index in range(first + 1, last):
            pl.when(step == index - 1 - first)(
                lambda index=index: self.begin(gather, index, size)
            )
        slot = lax.rem(step + first, 2)
        for each in self._copies(gather, 0, slot, size):
            each.wait()
        held = self.refs[0]
        return held[slot, :, :, 0:size].reshape(-1, held.shape[-1])


def prepare_body(
    slot_ref, live_ref, im_ref, go_ref, gain_ref, shift_ref, own_ref, row_ref,
    x_ref, g_ref, n_ref, s_ref, early_ref, bias_ref, sems,
):
    step = pl.program_id(0)
    slot = slot_ref[0]
    hops = [lambda lane=lane: hop(own_ref.at[lax.rem(lax.axis_index(DP), 2), lane], early_ref.at[lane], sems, lane, LANES[lane]) for lane in range(2)]
    for r in range(1, 4):
        to = {TENSOR: lax.axis_index(TENSOR) ^ r}
        hops.append(lambda r=r, to=to: hop(row_ref, bias_ref.at[r - 1], sems, 1 + r, to))

    @pl.when(step == 0)
    def _():
        meet((X, Y, XY))
        for each in hops[2:] + hops[:2]:
            each().start()

    def pick(ref):
        values = ref[...].astype(F32)
        chosen = values[:, 0]
        for index in range(1, values.shape[1]):
            chosen = jnp.where(slot == index, values[:, index], chosen)
        return chosen

    picture = pick(im_ref)
    centered = picture - row_mean(picture)
    inverse = lax.rsqrt(row_mean(centered * centered) + EPS)
    normed = centered * inverse * gain_ref[...] + shift_ref[...]
    x_ref[...] = picture.T.astype(BF)
    g_ref[...] = (pick(go_ref) * live_ref[0].astype(F32)).T.astype(BF)
    n_ref[...] = normed.T.astype(BF)
    s_ref[0:1, :] = row_mean(picture).T
    s_ref[1:2, :] = inverse.T

    @pl.when(step == pl.num_programs(0) - 1)
    def _():
        for each in hops:
            each().wait()


def prepare(images, grad_out, slot, live, gain, shift, own, bias):
    slots, length, width = images.shape
    rows = 128
    scalar = pl.BlockSpec(memory_space=pltpu.SMEM)
    tokens = pl.BlockSpec((rows, slots, width), lambda i: (i, 0, 0))
    vector = pl.BlockSpec((1, width), lambda i: (0, 0))
    return pl.pallas_call(
        prepare_body,
        grid=(pl.cdiv(length, rows),),
        in_specs=[scalar, scalar, tokens, tokens, vector, vector, ANYWHERE, ANYWHERE],
        out_specs=[pl.BlockSpec((width, rows), lambda i: (0, i))] * 3
        + [pl.BlockSpec((2, rows), lambda i: (0, i)), ANYWHERE, ANYWHERE],
        out_shape=[jax.ShapeDtypeStruct((width, length), BF)] * 3
        + [
            jax.ShapeDtypeStruct((2, length), F32),
            jax.ShapeDtypeStruct(own.shape[1:], BF),
            jax.ShapeDtypeStruct((3, *bias.shape), F32),
        ],
        scratch_shapes=[pltpu.SemaphoreType.DMA((2, 5))],
        compiler_params=pltpu.CompilerParams(
            vmem_limit_bytes=50 << 20, collective_id=1, has_side_effects=True
        ),
        name="prepare",
    )(slot, live, images.transpose(1, 0, 2), grad_out.transpose(1, 0, 2), gain, shift, own, bias)


def as_column(row):
    return jnp.broadcast_to(row, (8, row.shape[1])).T[:, 0:1]


def as_row(column):
    return jnp.broadcast_to(column, (column.shape[0], 8)).T[0:1, :]


def attend_head(weight, normed, bias, qkv_ref, o_ref, lse_ref):
    length = normed.shape[1]
    rows = dot_nn(weight, normed)
    queries = ((rows[:HD] + bias[0]) * (LOG2E / math.sqrt(HD))).astype(BF)
    keys_t = rows[HD : 2 * HD].astype(BF)
    values = (rows[2 * HD :] + bias[1]).astype(BF)
    qkv_ref[0, 0] = queries
    qkv_ref[0, 1] = keys_t
    qkv_ref[0, 2] = values
    keys = keys_t.T
    for start in range(0, length, QUERY_BLOCK):
        block = slice(start, min(start + QUERY_BLOCK, length))
        scores = dot_nn(keys, queries[:, block])
        top = jnp.max(scores, axis=0, keepdims=True)
        weights = jnp.exp2(scores - top)
        total = jnp.sum(weights, axis=0, keepdims=True)
        mixed = dot_nn(values, weights.astype(BF))
        o_ref[0, :, block] = (mixed * (1.0 / total)).astype(BF)
        lse_ref[0, :, block] = top + jnp.log2(total)


def attend_back_head(qkv_ref, do_ref, o_ref, lse_ref, d_ref, dk_acc, dv_acc):
    keys_t = qkv_ref[0, 1]
    keys = keys_t.T
    values = qkv_ref[0, 2].T
    length = keys_t.shape[1]
    scale = 1.0 / math.sqrt(HD)
    for start in range(0, length, QUERY_BLOCK):
        block = slice(start, min(start + QUERY_BLOCK, length))
        queries_t = qkv_ref[0, 0, :, block]
        pull_t = do_ref[0, :, block]
        delta = jnp.sum(
            pull_t.astype(F32) * o_ref[0, :, block].astype(F32), axis=0, keepdims=True
        )
        probs = jnp.exp2(dot_nn(keys, queries_t) - lse_ref[0, :, block])
        probs_low = probs.astype(BF)
        d_probs = dot_nn(values, pull_t)
        d_scores = (probs * (d_probs - delta)).astype(BF)
        d_ref[0, 0, :, block] = (dot_nn(keys_t, d_scores) * scale).astype(BF)
        d_keys = dot_nn(d_scores, queries_t.T)
        d_values = dot_nn(probs_low, pull_t.T)
        if start == 0:
            dk_acc[...] = d_keys
            dv_acc[...] = d_values
        else:
            dk_acc[...] += d_keys
            dv_acc[...] += d_values
    d_ref[0, 1] = (dk_acc[...].T * LN2).astype(BF)
    d_ref[0, 2] = dv_acc[...].T.astype(BF)
    return [jnp.sum(d_ref[0, k].astype(F32), axis=1, keepdims=True) for k in (0, 2)]


def columns_of(length, block=128):
    return [slice(start, min(start + block, length)) for start in range(0, length, block)]


def norm_back(grad, unit_values, inverse, gain):
    scaled = grad * gain
    mean = lambda values: jnp.mean(values, axis=0, keepdims=True)
    return inverse * (scaled - mean(scaled) - unit_values * mean(scaled * unit_values))


def turned(values, axis, bit):
    return jnp.where(bit == 1, lax.rev(values, (axis,)), values)


def forward(attn_own, early, fc1_own, bias, bias_far, picture, normed_one, vectors):
    width, length = picture.shape
    chunk = attn_own.shape[2]
    unit = fc1_own.shape[2]
    rows = 2 * unit
    heads = 16
    p = Program("forward", (X, Y, CORE))
    own, soon, own_fc1 = p.input(attn_own), p.input(early), p.input(fc1_own)
    bias_in, x_in, n_in, v_in = p.input(bias), p.input(picture), p.input(normed_one), p.input(vectors)
    bias_far_in = p.input(bias_far)
    attn = Gather(p, own, attn_own.shape, soon)
    fc1 = Gather(p, own_fc1, fc1_own.shape)
    stream = Stream(p, 1, unit, width)
    qkv, mixed = p.output(heads, 3, HD, length), p.output(heads, HD, length)
    lse = p.output(heads, 1, length, dtype=F32)
    residual, normed = p.output(width, length, dtype=F32), p.output(width, length)
    stats, out_all = p.output(2, length, dtype=F32), p.output(heads, HD, width)
    act, slope = p.output(8, rows, length), p.output(8, rows, length)
    held = Bag(
        bias=p.tile(4, *bias.shape, dtype=F32),
        x=p.tile(width, length),
        n=p.tile(width, length),
        v=p.tile(*vectors.shape, dtype=F32),
        o=p.tile(heads, HD, length),
        w=p.tile(heads, HD, width),
        h=p.tile(width, length, dtype=F32),
        n2=p.tile(width, length),
        s=p.tile(2, length, dtype=F32),
    )
    sems, wsems = p.sems(8), p.sems(heads)

    def script(ref):
        hold = held.each(ref)
        sem, wsem = ref(sems), ref(wsems)
        attn.bind(ref)
        fc1.bind(ref)
        stream.bind(ref)
        attn.start()
        attn.forward()
        fc1.start()
        copies = [
            fetch(ref(n_in), hold.n, sem.at[0]),
            fetch(ref(bias_in), hold.bias.at[0], sem.at[1]),
            fetch(ref(bias_far_in), hold.bias.at[pl.ds(1, 3)], sem.at[2]),
            fetch(ref(x_in), hold.x, sem.at[5]),
            fetch(ref(v_in), hold.v, sem.at[6]),
        ]
        for each in copies[:3]:
            each.wait()

        def heads_of(first, count, part_of, sources, specs, events=()):
            def body(step, *refs):
                weights, (qkv_ref, o_ref, lse_ref) = refs[: len(sources)], refs[len(sources) :]
                shard, half, lane = part_of(step)
                rows_of = lambda w: w[...].reshape(chunk, width)[: 3 * HD]
                weight = rows_of(weights[0])
                if len(weights) > 2:
                    weight = jnp.where(lane == shard - 1, rows_of(weights[2]), weight)
                if len(weights) > 1:
                    weight = jnp.where(half == 0, weight, rows_of(weights[1]))
                at = 4 * half + 2 * lane
                shift = [
                    as_column(hold.bias[shard, at + k, :, 0:HD]) for k in range(2)
                ]
                attend_head(weight, hold.n[...], shift, qkv_ref, o_ref, lse_ref)
                hold.o[first + step] = o_ref[0]

            phase(
                count,
                body,
                sources,
                specs,
                [ref(qkv), ref(mixed), ref(lse)],
                [
                    spec((1, 3, HD, length), lambda i: (first + i, 0, 0, 0)),
                    spec((1, HD, length), lambda i: (first + i, 0, 0)),
                    spec((1, 1, length), lambda i: (first + i, 0, 0)),
                ],
                events,
            )

        def bring_out(shard):
            return [
                pltpu.make_async_copy(
                    attn.piece(shard, half, lane).at[pl.ds(3 * HD, HD)],
                    hold.w.at[4 * shard + 2 * half + lane],
                    wsem.at[4 * shard + 2 * half + lane],
                )
                for half in range(2)
                for lane in range(2)
            ]

        heads_of(
            0,
            4,
            lambda i: (0, i // 2, lax.rem(i, 2)),
            [ref(own).at[lax.rem(lax.axis_index(DP) + part, 2)] for part in range(2)],
            [spec((1, chunk, width), lambda i: (lax.rem(i, 2), 0, 0))] * 2,
        )
        attn.near_here()
        attn.near_whole()
        mine = lambda i: (i // 4, 1 - i // 4, 0, 0)
        heads_of(
            4,
            8,
            lambda i: (1 + i // 4, lax.rem(i // 2, 2), lax.rem(i, 2)),
            [ref(attn.near), ref(attn.near_part), ref(soon)],
            [
                spec((1, 1, chunk, width), mine),
                spec((1, 1, chunk, width), lambda i: (i // 4, lax.rem(i, 2), 0, 0)),
                spec((1, chunk, width), lambda i: (i // 4, 0, 0)),
            ],
        )
        attn.far_here()
        for shard in range(3):
            for each in bring_out(shard):
                each.start()
        attn.far_whole()
        for each in bring_out(3):
            each.start()
        heads_of(
            12,
            4,
            lambda i: (3, i // 2, lax.rem(i, 2)),
            [ref(attn.far), ref(attn.far_part)],
            [spec((1, chunk, width), lambda i: (lax.rem(i, 2), 0, 0))] * 2,
        )
        fc1.forward()
        for each in copies[3:]:
            each.wait()
        for shard in range(4):
            for each in bring_out(shard):
                each.wait()
        stream.begin(fc1, 0)
        store_w = fetch(hold.w, ref(out_all), sem.at[4])
        weight = hold.w[...].reshape(width, width)
        for block in columns_of(length, 256):
            mix = hold.o[:, :, block].reshape(width, -1)
            values = hold.x[:, block].astype(F32) + contract_rows(weight, mix)
            values = values + hold.v[:, 2:3]
            average = jnp.mean(values, axis=0, keepdims=True)
            centered = values - average
            inverse = lax.rsqrt(jnp.mean(centered * centered, axis=0, keepdims=True) + EPS)
            hold.h[:, block] = values
            hold.n2[:, block] = (
                centered * inverse * hold.v[:, 3:4] + hold.v[:, 4:5]
            ).astype(BF)
            hold.s[0:1, block] = average
            hold.s[1:2, block] = inverse
        stores = [store_w] + [
            fetch(source, ref(target), sem.at[k])
            for k, (source, target) in enumerate(((hold.h, residual), (hold.n2, normed), (hold.s, stats)))
        ]

        def hidden(step, act_ref, slope_ref):
            weight = stream.bring(fc1, step, 0, 8)
            shard, half = step // 2, lax.rem(step, 2)
            shift = as_column(hold.bias[shard, half, :, 128 : 128 + rows])
            preact = dot_nn(weight, hold.n2[...]) + shift
            square = preact * preact
            curve = jnp.tanh(preact * (GELU_A + (GELU_A * GELU_B) * square))
            rise = 0.5 * (1.0 + curve)
            act_ref[0] = (preact * rise).astype(BF)
            inner = GELU_A + (3.0 * GELU_A * GELU_B) * square
            slope_ref[0] = (rise + (0.5 * preact) * (1.0 - curve * curve) * inner).astype(BF)

        block = spec((1, rows, length), lambda i: (i, 0, 0))

        def near_all():
            fc1.near_here()
            fc1.near_whole()

        def far_all():
            fc1.far_here()
            fc1.far_whole()

        phase(
            8, hidden, [], [], [ref(act), ref(slope)], [block, block],
            [(1, near_all), (5, far_all)],
        )
        for each in stores:
            each.wait()
        attn.drain()
        fc1.drain()

    result = p.call(script, 2, 3e10)
    return (
        gathered(attn).each(result),
        gathered(fc1).each(result),
        Bag(
            qkv=qkv,
            mixed=mixed,
            lse=lse,
            residual=residual,
            normed_two=normed,
            stats_two=stats,
            out_all=out_all,
            act=act,
            slope=slope,
        ).each(result),
    )


def gathered(source):
    return Bag(
        near=source.near, near_part=source.near_part, far=source.far, far_part=source.far_part
    )


class Ready:
    def __init__(self, program, own, parts, early=None):
        self.handles = parts.each(program.input)
        self.handles.own = program.input(own)
        self.handles.early = None if early is None else program.input(early)
        self.early = early

    def bind(self, ref):
        self.refs = self.handles.each(lambda h: None if h is None else ref(h))
        return self

    piece = Gather.piece


def backward(arrays, fc1_parts, attn_parts, owns, early, live):
    width, length = arrays.picture.shape
    share = width // 4
    unit = owns.fc2.shape[2]
    rows = 2 * unit
    block = 3 * HD
    p = Program("backward", (X, Y, XY, CORE, LINE))
    into = arrays.each(p.input)
    live_in = p.input(live, pl.BlockSpec(memory_space=pltpu.SMEM))
    fc1 = Ready(p, owns.fc1, fc1_parts)
    attn = Ready(p, owns.attn, attn_parts, early)
    fc2 = Gather(p, p.input(owns.fc2), owns.fc2.shape)
    stream = Stream(p, 2, unit, width)

    fc_shape, out_shape, qkv_shape = ((4, 2, u, width) for u in (unit, HD, block))
    shapes = (fc_shape, fc_shape, out_shape, qkv_shape)
    part = [p.output(*shape) for shape in shapes]
    mine = [p.output(*shape) for shape in shapes]
    swap = [Swap(p, source, shape) for source, shape in zip(part, shapes)]
    plane = [Plane(p, source, shape) for source, shape in zip(mine, shapes)]
    line = [Line(p, shape[1:]) for shape in shapes]
    d_pre = p.output(8, rows, length)
    pull = p.output(16, HD, length)
    d_qkv = p.output(16, 3, HD, length)
    block_rows, input_rows = p.output(4, share, length), p.output(4, share, length)
    spread_block = Spread(p, block_rows, (4, share, length))
    spread_input = Spread(p, input_rows, (4, share, length))
    vectors = Vectors(p, (16, 1, width))
    held = Bag(
        upstream=p.tile(width, length),
        normed_two=p.tile(width, length),
        normed_one=p.tile(width, length),
        low=p.tile(width, length),
        residual=p.tile(width, length, dtype=F32),
        acc=p.tile(width, length, dtype=F32),
        vectors=p.tile(*arrays.vectors.shape, dtype=F32),
        cols=p.tile(width, 8, dtype=F32),
        stats_two=p.tile(2, length, dtype=F32),
        stats_one=p.tile(2, length, dtype=F32),
        dk=p.tile(length, HD, dtype=F32),
        dv=p.tile(length, HD, dtype=F32),
    )
    sems = p.sems(12)

    def script(ref):
        hold = held.each(ref)
        sem = ref(sems)
        for each in (fc1, attn, fc2, stream, spread_block, spread_input, vectors):
            each.bind(ref)
        for group in (swap, plane, line):
            for each in group:
                each.bind(ref)
        vec = vectors.refs.held
        array = into.each(ref)
        live_now = ref(live_in)[0].astype(F32)

        copies = Bag(
            upstream=fetch(array.upstream, hold.upstream, sem.at[0]),
            normed_two=fetch(array.normed_two, hold.normed_two, sem.at[1]),
            residual=fetch(array.residual, hold.residual, sem.at[2]),
            vectors=fetch(array.vectors, hold.vectors, sem.at[3]),
            stats_two=fetch(array.stats_two, hold.stats_two, sem.at[4]),
            normed_one=fetch(array.normed_one, hold.normed_one, sem.at[5]),
            stats_one=fetch(array.stats_one, hold.stats_one, sem.at[6]),
        )
        fc2.start()
        stream.begin(fc2, 0)
        vec[...] = jnp.zeros(vec.shape, F32)
        hold.cols[...] = jnp.zeros(hold.cols.shape, F32)
        copies.upstream.wait()
        copies.normed_two.wait()

        def gradient(source, other, name, half, shards, plus=False, events=()):
            _, lanes, size, _ = shapes[name]
            count = lanes * size
            pick = lambda i: jnp.where(i == 0, shards[0], shards[-1]) if len(shards) < 4 else i

            def body(step, *refs):
                sums = contract_cols(refs[0][...].reshape(count, length), other[...])
                if plus:
                    sums = sums + refs[1][0].reshape(count, width).astype(F32)
                refs[-1][0] = sums.astype(BF).reshape(lanes, size, width)

            lead = source.shape[0] // 8
            tail = source.shape[1:]
            out_spec = spec((1, lanes, size, width), lambda i: (pick(i), 0, 0, 0))
            zeros = (0,) * len(tail)
            phase(
                len(shards),
                body,
                [source] + ([swap[name].refs[1]] if plus else []),
                [spec((lead, *tail), lambda i: (2 * pick(i) + half, *zeros))]
                + ([out_spec] if plus else []),
                [ref((part, mine)[half == 0][name])],
                [out_spec],
                events,
            )

        every = (0, 1, 2, 3)
        gradient(array.act, hold.upstream, FC2, 1, every)
        swap[FC2].start(*every)

        def hidden(first, count, events=()):
            def body(step, slope_ref, d_ref):
                weight = stream.bring(fc2, step, first, first + count)
                values = dot_nn(weight, hold.upstream[...])
                values = (values * slope_ref[...].reshape(2 * rows, length).astype(F32)).astype(BF)
                d_ref[...] = values.reshape(2, rows, length)
                for half in range(2):
                    sums = jnp.sum(
                        values[half * rows : (half + 1) * rows].astype(F32), axis=1, keepdims=True
                    )
                    vec[8 + 2 * (first + step) + half, :, 0:rows] = as_row(sums)

            pair = spec((2, rows, length), lambda i: (first + i, 0, 0))
            phase(count, body, [array.slope], [pair], [ref(d_pre)], [pair], events)

        hidden(0, 1)
        fc2.forward()
        swap[FC2].wait(*every)
        gradient(array.act, hold.upstream, FC2, 0, every, True)
        plane[FC2].start()
        fc2.near_here()
        fc2.near_whole()
        stream.begin(fc2, 1)
        hidden(1, 2)
        fc2.far_here()
        fc2.far_whole()
        stream.begin(fc2, 3)
        hidden(3, 1)

        def back(weights, values, lead, size, events=()):
            def body(step, d_ref):
                weight = stream.bring(weights, step, 0, 4, size)
                sums = contract_rows(weight, d_ref[...].reshape(4 * size, length))

                @pl.when(step == 0)
                def _():
                    hold.acc[...] = sums

                @pl.when(step > 0)
                def _():
                    hold.acc[...] += sums

            tail = values.shape[1:]
            zeros = (0,) * len(tail)
            phase(4, body, [values], [spec((lead, *tail), lambda i: (i, *zeros))], [], [], events)

        stream.begin(fc1, 0)
        back(fc1, ref(d_pre), 2, unit)
        for each in (copies.residual, copies.vectors, copies.stats_two):
            each.wait()
        total = lambda values: jnp.sum(values, axis=1, keepdims=True)
        for cut in columns_of(length):
            inverse = hold.stats_two[1:2, cut]
            grad = hold.acc[:, cut]
            units = (hold.residual[:, cut] - hold.stats_two[0:1, cut]) * inverse
            up = hold.upstream[:, cut].astype(F32)
            d_residual = up + norm_back(grad, units, inverse, hold.vectors[:, 3:4])
            hold.low[:, cut] = d_residual.astype(BF)
            hold.cols[:, 2:3] += total(d_residual)
            hold.cols[:, 3:4] += total(grad * units)
            hold.cols[:, 4:5] += total(grad)
            hold.cols[:, 5:6] += total(up)

        gradient(ref(d_pre), hold.normed_two, FC1, 1, every)
        swap[FC1].start(*every)
        plane[FC2].forward()
        plane[FC2].settle()
        picture_copy = fetch(array.picture, hold.upstream, sem.at[7])

        def pull_body(step, w_ref, o_ref):
            weight = w_ref[...].reshape(4 * HD, width)
            o_ref[...] = dot_nn(weight, hold.low[...]).reshape(4, HD, length).astype(BF)

        quarter = lambda *tail: spec((4, *tail), lambda i: (i, *(0 for _ in tail)))
        phase(
            4, pull_body, [array.out_all], [quarter(HD, width)], [ref(pull)], [quarter(HD, length)]
        )
        gradient(array.mixed, hold.low, OUT, 1, every)
        swap[OUT].start(*every)
        swap[FC1].wait(*every)
        gradient(ref(d_pre), hold.normed_two, FC1, 0, every, True)
        plane[FC1].start()
        plane[FC2].finish(line[FC2])
        swap[OUT].wait(*every)
        gradient(array.mixed, hold.low, OUT, 0, every, True)
        plane[OUT].start()
        copies.normed_one.wait()

        def heads_back(shards, events):
            shard_of = lambda i: jnp.where(i < 4, shards[0], shards[1])
            at = lambda i: 4 * shard_of(i) + lax.rem(i, 4)

            def body(step, qkv_ref, do_ref, o_ref, lse_ref, d_ref):
                sums = attend_back_head(
                    qkv_ref, do_ref, o_ref, lse_ref, d_ref, hold.dk, hold.dv
                )
                row = 8 + 2 * shard_of(step) + lax.rem(step // 2, 2)
                for k in range(2):
                    where = pl.multiple_of(640 + 128 * (2 * lax.rem(step, 2) + k), 128)
                    padded = jnp.concatenate(
                        [as_row(sums[k]), jnp.zeros((1, 128 - HD), F32)], axis=1
                    )
                    vec[row, :, pl.ds(where, 128)] = padded

            flat = spec((1, HD, length), lambda i: (at(i), 0, 0))
            many = spec((1, 3, HD, length), lambda i: (at(i), 0, 0, 0))
            phase(
                8,
                body,
                [array.qkv, ref(pull), array.mixed, array.lse],
                [many, flat, flat, spec((1, 1, length), lambda i: (at(i), 0, 0))],
                [ref(d_qkv)],
                [many],
                events,
            )

        heads_back((3, 1), [(6, lambda: line[FC2].meet(0))])
        gradient(ref(d_qkv), hold.normed_one, QKV, 1, (3, 1))
        swap[QKV].start(3, 1)

        def settle(name):
            plane[name].forward()
            plane[name].settle()

        heads_back(
            (2, 0),
            [
                (2, lambda: line[FC2].meet(1)),
                (2, lambda: settle(FC1)),
                (3, lambda: line[FC2].leave(0)),
                (6, lambda: settle(OUT)),
            ],
        )
        swap[QKV].wait(3, 1)
        gradient(ref(d_qkv), hold.normed_one, QKV, 0, (3, 1), True)
        plane[QKV].send(3)
        plane[QKV].send(1)
        gradient(ref(d_qkv), hold.normed_one, QKV, 1, (2, 0))
        swap[QKV].start(2, 0)
        line[FC2].leave(1)
        plane[FC1].finish(line[FC1])
        plane[OUT].finish(line[OUT])
        stream.begin(fc2, 0)
        swap[QKV].wait(2, 0)
        gradient(ref(d_qkv), hold.normed_one, QKV, 0, (2, 0), True)
        plane[QKV].send(2)
        plane[QKV].send(0)
        line[FC2].finish(0)
        back(fc2, array.act, 2, unit, [(3, lambda: line[FC1].meet(0))])
        line[FC2].finish(1)
        for cut in columns_of(length):
            values = hold.residual[:, cut] + hold.acc[:, cut] + hold.vectors[:, 5:6]
            hold.normed_two[:, cut] = (values * live_now).astype(BF)
        store_rows(hold.normed_two, ref(block_rows), sem, share)
        settle(QKV)
        spread_block.start()
        line[FC1].meet(1)
        line[FC1].leave(0)
        line[OUT].meet(0)
        line[OUT].meet(1)
        picture_copy.wait()
        copies.stats_one.wait()
        stream.begin(attn, 0, block)
        back(attn, ref(d_qkv), 4, block, [(2, lambda: line[FC1].leave(1))])
        line[OUT].leave(0)
        line[OUT].leave(1)
        plane[QKV].finish(line[QKV])
        for cut in columns_of(length):
            inverse = hold.stats_one[1:2, cut]
            grad = hold.acc[:, cut]
            units = hold.upstream[:, cut].astype(F32) - hold.stats_one[0:1, cut]
            units = units * inverse
            d_input = hold.low[:, cut].astype(F32) + norm_back(
                grad, units, inverse, hold.vectors[:, 0:1]
            )
            hold.normed_two[:, cut] = d_input.astype(BF)
            hold.cols[:, 0:1] += total(grad * units)
            hold.cols[:, 1:2] += total(grad)
        store_rows(hold.normed_two, ref(input_rows), sem, share)
        spread_input.start()
        wide = hold.cols[...].T
        for k in range(8):
            vec[k] = wide[k : k + 1]
        line[QKV].meet(0)
        vectors.run()
        line[QKV].meet(1)
        line[QKV].leave(0)
        line[FC1].finish(0)
        line[FC1].finish(1)
        line[OUT].finish(0)
        line[OUT].finish(1)
        line[QKV].leave(1)
        spread_block.finish()
        spread_input.finish()
        line[QKV].finish(0)
        line[QKV].finish(1)
        for each in plane:
            each.drain()
        fc2.drain()

    result = p.call(script, 3, 8e10)
    sums = [(result(each.total), result(each.other)) for each in line]
    spreads = [
        (result(block_rows), result(spread_block.landed)),
        (result(input_rows), result(spread_input.landed)),
    ]
    return sums, spreads, result(vectors.total)[:, 0]


def store_rows(source, target, sem, share):
    copies = [
        fetch(source.at[pl.ds(k * share, share)], target.at[k], sem.at[k]) for k in range(4)
    ]
    for each in copies:
        each.wait()


def finish(sums, spreads, place_t, core, hidden):
    width = sums[FC2][0].shape[-1]
    share, length = spreads[0][0].shape[1:]

    def body(at, *refs):
        step = pl.program_id(0)
        same = lax.rem(step // 2 + at[1], 2) == 0
        ins, outs = refs[:12], refs[12:]
        for k in range(4):
            rows = jnp.where(same, ins[2 * k][0], ins[2 * k + 1][0]).astype(F32)
            outs[k][...] = rows.reshape(outs[k].shape)
        for k in range(2):
            rows = jnp.where(step == at[0], ins[8 + 2 * k][0], ins[9 + 2 * k][0])
            outs[4 + k][0] = rows.astype(F32)

    half = lambda array: pl.BlockSpec((1, *array.shape[1:]), lambda i, at: (lax.rem(i, 2), 0, 0))
    own = pl.BlockSpec((1, share, length), lambda i, at: (at[0], 0, 0))
    landed = pl.BlockSpec(
        (1, share, length), lambda i, at: (jnp.maximum((i ^ at[0]) - 1, 0), 0, 0)
    )
    units = [pair[0].shape[1] for pair in sums]
    rows = lambda unit: pl.BlockSpec((unit, width), lambda i, at: (i, 0))
    slot = pl.BlockSpec((1, share, length), lambda i, at: (i, 0, 0))
    shape = lambda *dims: jax.ShapeDtypeStruct(dims, F32)
    return pl.pallas_call(
        body,
        grid_spec=pltpu.PrefetchScalarGridSpec(
            num_scalar_prefetch=1,
            grid=(4,),
            in_specs=[half(array) for pair in sums for array in pair] + [own, landed] * 2,
            out_specs=[
                rows(units[FC2]),
                rows(units[FC1]),
                rows(units[OUT]),
                pl.BlockSpec((3, HD, width), lambda i, at: (0, i, 0)),
                slot,
                slot,
            ],
        ),
        out_shape=[
            shape(hidden, width),
            shape(hidden, width),
            shape(share, width),
            shape(3, share, width),
            shape(4, share, length),
            shape(4, share, length),
        ],
        compiler_params=pltpu.CompilerParams(vmem_limit_bytes=50 << 20),
        name="finish",
    )(
        jnp.stack([place_t, core]).astype(jnp.int32),
        *[array for pair in sums for array in pair],
        *spreads[0],
        *spreads[1],
    )


def whole_image(
    images,
    counts,
    ln1_gain,
    ln1_bias,
    qkv_weight,
    qv_bias,
    out_weight,
    out_bias,
    ln2_gain,
    ln2_bias,
    fc1_weight,
    fc1_bias,
    fc2_weight,
    fc2_bias,
    grad_out,
):
    slot_count, length, width = images.shape
    share = width // 4
    hidden = fc1_weight.shape[1]
    unit = -(-hidden // 64) * 16
    rows = 2 * unit
    place_t = lax.axis_index(TENSOR)
    core = lax.rem(lax.axis_index(DP), 2)
    block = 3 * HD

    qkv_rows = qkv_weight.reshape(3, width, 2, 2, HD).transpose(2, 3, 0, 4, 1)
    attn_own = jnp.concatenate(
        [qkv_rows.reshape(2, 2, block, width), out_weight.reshape(2, 2, HD, width)], axis=2
    )
    pad = 2 * rows - hidden
    fc1_own, fc2_own = (
        jnp.pad(each, ((0, pad), (0, 0))).reshape(2, 2, unit, width)
        for each in (fc1_weight.T, fc2_weight)
    )
    head_bias = qv_bias.reshape(2, 2, 2, HD).transpose(1, 2, 0, 3)
    head_bias = jnp.pad(turned(head_bias, 0, core).reshape(8, HD), ((0, 0), (0, 128 - HD)))
    hidden_bias = turned(jnp.pad(fc1_bias, (0, pad)).reshape(2, rows), 0, core)
    hidden_bias = jnp.pad(hidden_bias, ((0, 6), (0, 640 - rows)))
    bias = jnp.concatenate([head_bias, hidden_bias], axis=1).astype(F32)[:, None]
    vectors = jnp.stack(
        [ln1_gain, ln1_bias, out_bias, ln2_gain, ln2_bias, fc2_bias, fc2_bias, fc2_bias], axis=1
    ).astype(F32)
    live = (place_t < counts[0]).astype(jnp.int32)[None]

    picture, upstream, normed_one, stats_one, early, bias_far = prepare(
        images,
        grad_out,
        place_t[None].astype(jnp.int32),
        live,
        ln1_gain.astype(F32)[None],
        ln1_bias.astype(F32)[None],
        attn_own,
        bias,
    )
    attn_parts, fc1_parts, made = forward(
        attn_own, early, fc1_own, bias, bias_far, picture, normed_one, vectors
    )
    made.__dict__.update(
        upstream=upstream,
        picture=picture,
        normed_one=normed_one,
        stats_one=stats_one,
        vectors=vectors,
    )
    owns = Bag(attn=attn_own, fc1=fc1_own, fc2=fc2_own)
    sums, spreads, totals = backward(made, fc1_parts, attn_parts, owns, early, live)

    own_wide = lax.dynamic_slice_in_dim(totals[:6], place_t * share, share, 1)
    own_rows = turned(totals[8:10], 0, core)
    own_hidden = own_rows[:, :rows].reshape(-1)[:hidden]
    own_qv = own_rows[:, 640:].reshape(2, 2, 2, 128)[..., :HD].transpose(2, 0, 1, 3)
    own_qv = own_qv.reshape(2, share)

    fc2_result, fc1_result, out_result, qkv_result, block_result, input_result = finish(
        sums, spreads, place_t, core, hidden
    )
    return (
        block_result.transpose(0, 2, 1),
        input_result.transpose(0, 2, 1),
        own_wide[0],
        own_wide[1],
        qkv_result.transpose(0, 2, 1),
        own_qv,
        out_result,
        own_wide[2],
        own_wide[3],
        own_wide[4],
        fc1_result.T,
        own_hidden,
        fc2_result,
        own_wide[5],
    )


def solution(mesh):
    whole_fits = mesh.shape[TENSOR] == 4 and mesh.shape[DP] == 8
    return jax.shard_map(
        whole_image if whole_fits else local,
        mesh=mesh,
        in_specs=(
            P(DP, None, None),
            P(DP),
            P(),
            P(),
            P(None, None, TENSOR),
            P(None, TENSOR),
            P(TENSOR, None),
            P(),
            P(),
            P(),
            P(None, TENSOR),
            P(TENSOR),
            P(TENSOR, None),
            P(),
            P(DP, None, None),
        ),
        out_specs=(
            P(DP, None, TENSOR),
            P(DP, None, TENSOR),
            P(TENSOR),
            P(TENSOR),
            P(None, None, TENSOR),
            P(None, TENSOR),
            P(TENSOR, None),
            P(TENSOR),
            P(TENSOR),
            P(TENSOR),
            P(None, TENSOR),
            P(TENSOR),
            P(TENSOR, None),
            P(TENSOR),
        ),
        check_vma=False,
    )
```

```python
import math

import jax
import jax.numpy as jnp
from jax import lax
from jax.experimental import pallas as pl
from jax.experimental.pallas import tpu as pltpu
from jax.sharding import PartitionSpec as P

HD = 72


EPS = 1e-06


def own_columns(values, share_width):
    start = lax.axis_index(TENSOR) * share_width
    return lax.dynamic_slice_in_dim(values, start, share_width, values.ndim - 1)


def row_mean(values):
    return jnp.mean(values, axis=-1, keepdims=True)


def group_stats(first, second):
    return lax.psum((first, second), TENSOR)


def contract_rows(left, right):
    return lax.dot_general(
        left, right, (((0,), (0,)), ((), ())), preferred_element_type=jnp.float32
    )


def contract_cols(left, right):
    return lax.dot_general(
        left, right, (((1,), (1,)), ((), ())), preferred_element_type=jnp.float32
    )


def gelu_tanh(values):
    return jax.nn.gelu(values, approximate=True)


def local(
    images,
    counts,
    ln1_gain,
    ln1_bias,
    qkv_weight,
    qv_bias,
    out_weight,
    out_bias,
    ln2_gain,
    ln2_bias,
    fc1_weight,
    fc1_bias,
    fc2_weight,
    fc2_bias,
    grad_out,
):
    slot_count, length, full_width = images.shape
    share_width = full_width // lax.axis_size(TENSOR)
    local_width = qkv_weight.shape[2]
    local_heads = local_width // HD
    hidden_width = fc1_weight.shape[1]
    score_scale = 1.0 / math.sqrt(HD)
    gain_one = ln1_gain.astype(jnp.float32)
    shift_one = ln1_bias.astype(jnp.float32)
    gain_two = ln2_gain.astype(jnp.float32)
    shift_two = ln2_bias.astype(jnp.float32)
    bias_out = out_bias.astype(jnp.float32)
    bias_fc1 = fc1_bias.astype(jnp.float32)
    bias_fc2 = fc2_bias.astype(jnp.float32)
    bias_query = qv_bias[0].astype(jnp.float32)
    bias_value = qv_bias[1].astype(jnp.float32)
    live_count = counts[0]

    def to_heads(values):
        return values.reshape(length, local_heads, HD)

    def head_scores(query_heads, key_heads):
        return (
            jnp.einsum("qhd,khd->hqk", query_heads, key_heads, preferred_element_type=jnp.float32)
            * score_scale
        )

    def layer_step(slot_index, loop_state):
        block_acc, input_acc, grads = loop_state
        (
            grad_gain_one,
            grad_shift_one,
            grad_qkv,
            grad_qv,
            grad_out_w,
            grad_out_b,
            grad_gain_two,
            grad_shift_two,
            grad_fc1_w,
            grad_fc1_b,
            grad_fc2_w,
            grad_fc2_b,
        ) = grads
        live_flag = (slot_index < live_count).astype(jnp.float32)
        picture = lax.dynamic_index_in_dim(images, slot_index, 0, keepdims=False).astype(
            jnp.float32
        )
        upstream = (
            lax.dynamic_index_in_dim(grad_out, slot_index, 0, keepdims=False).astype(jnp.float32)
            * live_flag
        )
        upstream_low = upstream.astype(jnp.bfloat16)
        centered = picture - row_mean(picture)
        inv_one = lax.rsqrt(row_mean(centered * centered) + EPS)
        unit_one = centered * inv_one
        normed_one = (unit_one * gain_one + shift_one).astype(jnp.bfloat16)
        query_rows = (
            jnp.dot(normed_one, qkv_weight[0], preferred_element_type=jnp.float32) + bias_query
        ).astype(jnp.bfloat16)
        key_rows = jnp.dot(normed_one, qkv_weight[1], preferred_element_type=jnp.float32).astype(
            jnp.bfloat16
        )
        value_rows = (
            jnp.dot(normed_one, qkv_weight[2], preferred_element_type=jnp.float32) + bias_value
        ).astype(jnp.bfloat16)
        query_heads = to_heads(query_rows)
        key_heads = to_heads(key_rows)
        value_heads = to_heads(value_rows)
        scores = head_scores(query_heads, key_heads)
        row_top = jnp.max(scores, axis=-1, keepdims=True)
        logsum = row_top + jnp.log(jnp.sum(jnp.exp(scores - row_top), axis=-1, keepdims=True))
        probs_low = jnp.exp(scores - logsum).astype(jnp.bfloat16)
        mixed = jnp.einsum(
            "hqk,khd->qhd", probs_low, value_heads, preferred_element_type=jnp.float32
        )
        mixed = mixed.reshape(length, local_width).astype(jnp.bfloat16)
        partial_out = jnp.dot(mixed, out_weight, preferred_element_type=jnp.float32).astype(
            jnp.bfloat16
        )
        residual = (
            own_columns(picture, share_width)
            + lax.psum_scatter(partial_out, TENSOR, scatter_dimension=1, tiled=True).astype(
                jnp.float32
            )
            + own_columns(bias_out, share_width)
        )
        row_sum, row_square = group_stats(
            jnp.sum(residual, axis=-1), jnp.sum(residual * residual, axis=-1)
        )
        average = row_sum[:, None] / full_width
        inv_two = lax.rsqrt(row_square[:, None] / full_width - average * average + EPS)
        unit_two = (residual - average) * inv_two
        own_normed = (
            unit_two * own_columns(gain_two, share_width) + own_columns(shift_two, share_width)
        ).astype(jnp.bfloat16)
        normed_two = lax.all_gather(own_normed, TENSOR, axis=1, tiled=True)
        preact = jnp.dot(normed_two, fc1_weight, preferred_element_type=jnp.float32) + bias_fc1
        activated = gelu_tanh(preact).astype(jnp.bfloat16)
        partial_mlp = jnp.dot(activated, fc2_weight, preferred_element_type=jnp.float32).astype(
            jnp.bfloat16
        )
        block_rows = (
            residual
            + lax.psum_scatter(partial_mlp, TENSOR, scatter_dimension=1, tiled=True).astype(
                jnp.float32
            )
            + own_columns(bias_fc2, share_width)
        )
        block_rows = block_rows * live_flag
        grad_fc2_b = grad_fc2_b + own_columns(jnp.sum(upstream, axis=0), share_width)
        grad_fc2_w = grad_fc2_w + contract_rows(activated, upstream_low)
        d_act = contract_cols(upstream_low, fc2_weight)
        gelu_pull = jax.vjp(gelu_tanh, preact)[1]
        d_pre = gelu_pull(d_act)[0].astype(jnp.bfloat16)
        grad_fc1_b = grad_fc1_b + jnp.sum(d_pre.astype(jnp.float32), axis=0)
        grad_fc1_w = grad_fc1_w + contract_rows(normed_two, d_pre)
        back_mlp = contract_cols(d_pre, fc1_weight)
        d_norm_two = lax.psum_scatter(
            back_mlp.astype(jnp.bfloat16), TENSOR, scatter_dimension=1, tiled=True
        ).astype(jnp.float32)
        scaled_two = d_norm_two * own_columns(gain_two, share_width)
        sum_plain, sum_cross = group_stats(
            jnp.sum(scaled_two, axis=-1), jnp.sum(scaled_two * unit_two, axis=-1)
        )
        d_residual = own_columns(upstream, share_width) + inv_two * (
            scaled_two
            - sum_plain[:, None] / full_width
            - unit_two * (sum_cross[:, None] / full_width)
        )
        grad_gain_two = grad_gain_two + jnp.sum(d_norm_two * unit_two, axis=0)
        grad_shift_two = grad_shift_two + jnp.sum(d_norm_two, axis=0)
        grad_out_b = grad_out_b + jnp.sum(d_residual, axis=0)
        d_residual_low = lax.all_gather(
            d_residual.astype(jnp.bfloat16), TENSOR, axis=1, tiled=True
        )
        grad_out_w = grad_out_w + contract_rows(mixed, d_residual_low)
        d_mixed_heads = to_heads(contract_cols(d_residual_low, out_weight).astype(jnp.bfloat16))
        probs = jnp.exp(head_scores(query_heads, key_heads) - logsum)
        probs_again = probs.astype(jnp.bfloat16)
        d_value = jnp.einsum(
            "hqk,qhd->khd", probs_again, d_mixed_heads, preferred_element_type=jnp.float32
        )
        d_probs = jnp.einsum(
            "qhd,khd->hqk", d_mixed_heads, value_heads, preferred_element_type=jnp.float32
        )
        inner = jnp.sum(probs * d_probs, axis=-1, keepdims=True)
        d_scores = (probs * (d_probs - inner)).astype(jnp.bfloat16)
        d_query = (
            jnp.einsum("hqk,khd->qhd", d_scores, key_heads, preferred_element_type=jnp.float32)
            * score_scale
        )
        d_key = (
            jnp.einsum("hqk,qhd->khd", d_scores, query_heads, preferred_element_type=jnp.float32)
            * score_scale
        )
        d_stack = (
            jnp.stack([d_query, d_key, d_value], axis=1)
            .reshape(length, 3, local_width)
            .astype(jnp.bfloat16)
        )
        grad_qkv = grad_qkv + jnp.einsum(
            "ld,lje->jde", normed_one, d_stack, preferred_element_type=jnp.float32
        )
        bias_sums = jnp.sum(d_stack.astype(jnp.float32), axis=0)
        grad_qv = grad_qv + jnp.stack([bias_sums[0], bias_sums[2]])
        back_attn = jnp.einsum(
            "lje,jde->ld", d_stack, qkv_weight, preferred_element_type=jnp.float32
        )
        d_norm_one = lax.psum_scatter(
            back_attn.astype(jnp.bfloat16), TENSOR, scatter_dimension=1, tiled=True
        ).astype(jnp.float32)
        own_unit = own_columns(unit_one, share_width)
        scaled_one = d_norm_one * own_columns(gain_one, share_width)
        plain_one, cross_one = group_stats(
            jnp.sum(scaled_one, axis=-1), jnp.sum(scaled_one * own_unit, axis=-1)
        )
        d_input = d_residual + inv_one * (
            scaled_one
            - plain_one[:, None] / full_width
            - own_unit * (cross_one[:, None] / full_width)
        )
        grad_gain_one = grad_gain_one + jnp.sum(d_norm_one * own_unit, axis=0)
        grad_shift_one = grad_shift_one + jnp.sum(d_norm_one, axis=0)
        block_acc = lax.dynamic_update_index_in_dim(block_acc, block_rows, slot_index, 0)
        input_acc = lax.dynamic_update_index_in_dim(input_acc, d_input, slot_index, 0)
        new_grads = (
            grad_gain_one,
            grad_shift_one,
            grad_qkv,
            grad_qv,
            grad_out_w,
            grad_out_b,
            grad_gain_two,
            grad_shift_two,
            grad_fc1_w,
            grad_fc1_b,
            grad_fc2_w,
            grad_fc2_b,
        )
        return (block_acc, input_acc, new_grads)

    share_zeros = jnp.zeros((share_width,), jnp.float32)
    start_grads = (
        share_zeros,
        share_zeros,
        jnp.zeros((3, full_width, local_width), jnp.float32),
        jnp.zeros((2, local_width), jnp.float32),
        jnp.zeros((local_width, full_width), jnp.float32),
        share_zeros,
        share_zeros,
        share_zeros,
        jnp.zeros((full_width, hidden_width), jnp.float32),
        jnp.zeros((hidden_width,), jnp.float32),
        jnp.zeros((hidden_width, full_width), jnp.float32),
        share_zeros,
    )
    start_rows = jnp.zeros((slot_count, length, share_width), jnp.float32)
    block_acc, input_acc, grads = lax.fori_loop(
        0, slot_count, layer_step, (start_rows, start_rows, start_grads)
    )
    (
        grad_gain_one,
        grad_shift_one,
        grad_qkv,
        grad_qv,
        grad_out_w,
        grad_out_b,
        grad_gain_two,
        grad_shift_two,
        grad_fc1_w,
        grad_fc1_b,
        grad_fc2_w,
        grad_fc2_b,
    ) = grads
    summed = (
        lax.psum(grad_gain_one.astype(jnp.bfloat16), DP).astype(jnp.float32),
        lax.psum(grad_shift_one.astype(jnp.bfloat16), DP).astype(jnp.float32),
        lax.psum(grad_qkv.astype(jnp.bfloat16), DP).astype(jnp.float32),
        lax.psum(grad_qv.astype(jnp.bfloat16), DP).astype(jnp.float32),
        lax.psum(grad_out_w.astype(jnp.bfloat16), DP).astype(jnp.float32),
        lax.psum(grad_out_b.astype(jnp.bfloat16), DP).astype(jnp.float32),
        lax.psum(grad_gain_two.astype(jnp.bfloat16), DP).astype(jnp.float32),
        lax.psum(grad_shift_two.astype(jnp.bfloat16), DP).astype(jnp.float32),
        lax.psum(grad_fc1_w.astype(jnp.bfloat16), DP).astype(jnp.float32),
        lax.psum(grad_fc1_b.astype(jnp.bfloat16), DP).astype(jnp.float32),
        lax.psum(grad_fc2_w.astype(jnp.bfloat16), DP).astype(jnp.float32),
        lax.psum(grad_fc2_b.astype(jnp.bfloat16), DP).astype(jnp.float32),
    )
    return (
        block_acc,
        input_acc,
        summed[0],
        summed[1],
        summed[2],
        summed[3],
        summed[4],
        summed[5],
        summed[6],
        summed[7],
        summed[8],
        summed[9],
        summed[10],
        summed[11],
    )


LOG2E = math.log2(math.e)
LN2 = math.log(2.0)
GELU_A = math.sqrt(2.0 / math.pi)
GELU_B = 0.044715
BF = jnp.bfloat16
F32 = jnp.float32
QUERY_BLOCK = 256
MESH = pl.DeviceIdType.MESH
TENSOR, DP = "tensor", "dp"
X, Y, XY, CORE, LINE = range(5)
TURN = {X: 1, Y: 2, XY: 3}
OTHER = {X: Y, Y: X}
SIDE = {X: 0, Y: 1}
LANES = (X, Y)
FC2, FC1, OUT, QKV = range(4)
INWARD, ACROSS, BACK, SWAP = range(4)


class Bag:
    def __init__(self, **things):
        self.__dict__.update(things)

    def each(self, action):
        return Bag(**{name: action(thing) for name, thing in self.__dict__.items()})
ANYWHERE = pl.BlockSpec(memory_space=pl.ANY)


def dot_nn(left, right):
    return lax.dot_general(left, right, (((1,), (0,)), ((), ())), preferred_element_type=F32)


def place(bit):
    if bit == CORE:
        return {DP: lax.axis_index(DP) ^ 1}
    return {TENSOR: lax.axis_index(TENSOR) ^ TURN[bit]}


def hop(source, target, sems, index, to):
    return pltpu.make_async_remote_copy(
        src_ref=source,
        dst_ref=target,
        send_sem=sems.at[0, index],
        recv_sem=sems.at[1, index],
        device_id=place(to) if isinstance(to, int) else to,
        device_id_type=MESH,
    )


def line_place():
    dp = lax.axis_index(DP)
    return dp // 2, {DP: lax.rem(dp + 2, 8)}, {DP: lax.rem(dp + 6, 8)}


class Program:
    def __init__(self, name, partners):
        self.name = name
        self.partners = partners
        self.arrays, self.specs, self.shapes, self.scratches = [], [], [], []

    def input(self, array, spec=ANYWHERE):
        self.arrays.append(array)
        self.specs.append(spec)
        return (0, len(self.arrays) - 1)

    def output(self, *shape, dtype=BF):
        self.shapes.append(jax.ShapeDtypeStruct(shape, dtype))
        return (1, len(self.shapes) - 1)

    def scratch(self, spec):
        self.scratches.append(spec)
        return (2, len(self.scratches) - 1)

    def tile(self, *shape, dtype=BF):
        return self.scratch(pltpu.VMEM(shape, dtype))

    def sems(self, *shape):
        return self.scratch(pltpu.SemaphoreType.DMA(shape))

    def call(self, script, collective_id, cost):
        count_in, count_out = len(self.arrays), len(self.shapes)

        def kernel(*refs):
            pools = (
                refs[:count_in],
                refs[count_in : count_in + count_out],
                refs[count_in + count_out :],
            )
            meet(self.partners)
            script(lambda handle: pools[handle[0]][handle[1]])

        results = pl.pallas_call(
            kernel,
            in_specs=self.specs,
            out_specs=[ANYWHERE] * count_out,
            out_shape=self.shapes,
            scratch_shapes=self.scratches,
            compiler_params=pltpu.CompilerParams(
                vmem_limit_bytes=67_043_328, collective_id=collective_id, has_side_effects=True
            ),
            cost_estimate=pl.CostEstimate(
                flops=int(cost), bytes_accessed=1 << 26, transcendentals=0
            ),
            name=self.name,
        )(*self.arrays)
        return lambda handle: results[handle[1]]


def meet(partners):
    barrier = pltpu.get_barrier_semaphore()
    signal = lambda at: pl.semaphore_signal(barrier, inc=1, device_id=at, device_id_type=MESH)
    for bit in partners:
        if bit == XY:
            signal({TENSOR: lax.axis_index(TENSOR) ^ 3})
        elif bit != LINE:
            signal(place(bit))
    singles = len([bit for bit in partners if bit != LINE])
    if LINE in partners:
        z, up, down = line_place()
        pl.when(z < 3)(lambda: signal(up))
        pl.when(z > 0)(lambda: signal(down))
        inner = jnp.logical_and(z > 0, z < 3)
        pl.when(inner)(lambda: pl.semaphore_wait(barrier, singles + 2))
        pl.when(jnp.logical_not(inner))(lambda: pl.semaphore_wait(barrier, singles + 1))
    else:
        pl.semaphore_wait(barrier, singles)


def phase(steps, body, ins, in_specs, outs, out_specs, events=()):
    def inner(at, *refs):
        step = at.index[0]
        for when, event in events:
            pl.when(step == when)(event)
        body(step, *refs)

    pltpu.emit_pipeline(
        inner, grid=(steps,), in_specs=in_specs, out_specs=out_specs, _explicit_indices=True
    )(*ins, *outs)


def fetch(source, target, sem):
    copy = pltpu.make_async_copy(source, target, sem)
    copy.start()
    return copy


def spec(shape, index):
    return pl.BlockSpec(shape, index)


class Gather:
    def __init__(self, program, own, shape, early=None):
        _, count, unit, width = shape
        self.own = own
        self.early = early
        self.near = program.output(2, count, unit, width)
        self.near_part = program.output(2, count, unit, width)
        self.far = program.output(count, unit, width)
        self.far_part = program.output(count, unit, width)
        self.sems = program.sems(2, 12)

    def bind(self, ref):
        self.refs = Bag(
            own=ref(self.own),
            near=ref(self.near),
            near_part=ref(self.near_part),
            far=ref(self.far),
            far_part=ref(self.far_part),
            sems=ref(self.sems),
            early=None if self.early is None else ref(self.early),
        )
        return self

    def piece(self, shard, part, lane):
        r = self.refs
        if shard == 0:
            return r.own.at[lax.rem(lax.axis_index(DP) + part, 2), lane]
        if shard == 3:
            return (r.far_part if part else r.far).at[lane]
        if self.early is not None and part == 0 and LANES[lane] == LANES[shard - 1]:
            return r.early.at[lane]
        return (r.near_part if part else r.near).at[shard - 1, lane]

    def _near(self, bit, lane):
        r = self.refs
        k = SIDE[bit]
        own = self.piece(0, 0, lane)
        return hop(own, r.near.at[k, lane], r.sems, 2 * lane + k, bit)

    def _far(self, lane):
        first = LANES[lane]
        source = self.piece(1 + SIDE[first], 0, lane)
        return hop(source, self.refs.far.at[lane], self.refs.sems, 4 + lane, OTHER[first])

    def _swap(self, shard, lane):
        target = self.piece(shard, 1, lane)
        index = 6 + 2 * (shard - 1) + lane
        return hop(self.piece(shard, 0, lane), target, self.refs.sems, index, CORE)

    def start(self):
        for first in (True, False):
            for lane, bit in enumerate(LANES):
                if first and self.early is None:
                    self._near(bit, lane).start()
                if not first:
                    self._near(OTHER[bit], lane).start()

    def forward(self):
        for lane, first in enumerate(LANES):
            if self.early is None:
                self._near(first, lane).wait_recv()
            self._far(lane).start()
            self._swap(1 + SIDE[first], lane).start()

    def near_here(self):
        for lane, first in enumerate(LANES):
            self._near(OTHER[first], lane).wait_recv()
            self._swap(1 + SIDE[OTHER[first]], lane).start()

    def near_whole(self):
        for lane in range(2):
            for shard in (1, 2):
                self._swap(shard, lane).wait_recv()

    def far_here(self):
        for lane in range(2):
            self._far(lane).wait_recv()
            self._swap(3, lane).start()

    def far_whole(self):
        for lane in range(2):
            self._swap(3, lane).wait_recv()

    def drain(self):
        for lane, first in enumerate(LANES):
            if self.early is None:
                self._near(first, lane).wait_send()
            self._near(OTHER[first], lane).wait_send()
            self._far(lane).wait_send()
            for shard in (1, 2, 3):
                self._swap(shard, lane).wait_send()


class Plane:
    KEPT = {X: (0, 2), Y: (0, 1)}
    GONE = {X: (1, 3), Y: (2, 3)}

    def __init__(self, program, shape, share=None):
        _, count, unit, width = shape
        self.unit = unit
        if share is None:
            self.base = program.tile(count, 2, unit, width)
            self.sent = program.tile(count, 2, unit, width)
            self.got = program.tile(count, 2, unit, width)
            self.last = program.tile(count, unit, width)
        else:
            self.base, self.sent = share.base, share.sent
            self.got, self.last = share.got, share.last
        self.sems = program.sems(2, 6)
        self.swap_sems = program.sems(2, 8)

    def bind(self, ref):
        self.refs = [ref(h) for h in (self.base, self.sent, self.got, self.last, self.sems)]
        self.swaps = ref(self.swap_sems)
        return self

    def tile(self, shard, lane):
        first = LANES[lane]
        if shard in self.KEPT[first]:
            return self._part(0, lane, self.KEPT[first].index(shard))
        return self._part(1, lane, self.GONE[first].index(shard))

    def swap(self, source, shard, lane, static=0):
        return hop(source, self.tile(static, lane), self.swaps, 2 * shard + lane, CORE)

    def _part(self, which, *at):
        return self.refs[which].at[*at, pl.ds(0, self.unit)]

    def _first(self, lane, k):
        at = (lane, k)
        return hop(
            self._part(1, *at), self._part(2, *at), self.refs[4], 2 * lane + k, LANES[lane]
        )

    def _next(self, lane):
        return hop(
            self._part(0, lane, 1),
            self._part(3, lane),
            self.refs[4],
            4 + lane,
            OTHER[LANES[lane]],
        )

    def add(self, shard, lane, values, go):
        tile = self.tile(shard, lane)
        tile[...] = (values + tile[...].astype(F32)).astype(BF)
        if go and shard in self.GONE[LANES[lane]]:
            self._first(lane, self.GONE[LANES[lane]].index(shard)).start()

    def launch(self):
        for k in (1, 0):
            for lane in range(2):
                self._first(lane, k).start()

    def _add(self, lane, k):
        self._first(lane, k).wait_recv()
        base = self._part(0, lane, k)
        base[...] = base[...] + self._part(2, lane, k)[...]

    def forward(self):
        for lane in (1, 0):
            self._add(lane, 1)
            self._next(lane).start()

    def settle(self):
        for lane in range(2):
            self._add(lane, 0)

    def finish(self, line):
        for lane in range(2):
            self._next(lane).wait_recv()
            line.take(lane, self._part(0, lane, 0)[...] + self._part(3, lane)[...])

    def drain(self):
        for lane in range(2):
            self._next(lane).wait_send()
            for k in range(2):
                self._first(lane, k).wait_send()


class Line:
    def __init__(self, program, shape, share=None):
        count, unit, width = shape
        self.unit = unit
        self.total = program.output(*shape)
        self.other = program.output(*shape)
        if share is None:
            self.held = program.tile(*shape)
            self.outer = program.tile(*shape)
            self.middle = program.tile(*shape)
        else:
            self.held, self.outer, self.middle = share.held, share.outer, share.middle
        self.sems = program.sems(2, 4 * count)
        self.local = program.sems(count)
        self.count = count

    def bind(self, ref):
        self.refs = Bag(
            total=ref(self.total),
            other=ref(self.other),
            held=ref(self.held).at[:, pl.ds(0, self.unit)],
            outer=ref(self.outer).at[:, pl.ds(0, self.unit)],
            middle=ref(self.middle).at[:, pl.ds(0, self.unit)],
            sems=ref(self.sems),
            local=ref(self.local),
        )
        z, up, down = line_place()
        self.up, self.down = up, down
        self.is_outer = jnp.logical_or(z == 0, z == 3)
        self.is_inner = jnp.logical_not(self.is_outer)
        self.low = z < 2
        return self

    def _hop(self, kind, k, at):
        r = self.refs
        target = (r.outer, r.middle, r.outer, r.other)[kind]
        return hop(r.held.at[k], target.at[k], r.sems, kind * self.count + k, at)

    def _store(self, k):
        r = self.refs
        return pltpu.make_async_copy(r.held.at[k], r.total.at[k], r.local.at[k])

    def _send(self, kind, k):
        if kind == BACK:
            low, high = self.down, self.up
        else:
            low, high = self.up, self.down
        pl.when(self.low)(lambda: self._hop(kind, k, low).start())
        pl.when(jnp.logical_not(self.low))(lambda: self._hop(kind, k, high).start())

    def take(self, k, values):
        self.refs.held[k] = values
        pl.when(self.is_outer)(lambda: self._send(INWARD, k))

    def meet(self, k):
        r = self.refs

        @pl.when(self.is_inner)
        def _():
            self._hop(INWARD, k, self.up).wait_recv()
            r.held[k] += r.outer[k]
            self._send(ACROSS, k)

    def leave(self, k):
        r = self.refs

        @pl.when(self.is_inner)
        def _():
            self._hop(ACROSS, k, self.up).wait()
            r.held[k] += r.middle[k]
            self._send(BACK, k)
            self._hop(SWAP, k, CORE).start()
            self._store(k).start()

    def collect(self, k):
        r = self.refs

        @pl.when(self.is_outer)
        def _():
            self._hop(INWARD, k, self.up).wait_send()
            self._hop(BACK, k, self.up).wait_recv()
            r.held[k] = r.outer[k]
            self._hop(SWAP, k, CORE).start()
            self._store(k).start()

    def done(self, k):
        pl.when(self.is_inner)(lambda: self._hop(BACK, k, self.up).wait_send())
        self._store(k).wait()
        self._hop(SWAP, k, CORE).wait()


class Spread:
    def __init__(self, program, rows, shape):
        self.rows = rows
        self.landed = program.output(3, *shape[1:])
        self.sems = program.sems(2, 3)

    def bind(self, ref):
        self.refs = ref(self.rows), ref(self.landed), ref(self.sems)
        return self

    def _hop(self, r):
        rows, landed, sems = self.refs
        to = lax.axis_index(TENSOR) ^ r
        return hop(rows.at[to], landed.at[r - 1], sems, r - 1, {TENSOR: to})

    def start(self):
        for r in (3, 1, 2):
            self._hop(r).start()

    def finish(self):
        for r in (1, 2, 3):
            self._hop(r).wait()


class Vectors:
    def __init__(self, program, shape):
        self.total = program.output(*shape, dtype=F32)
        self.held = program.tile(*shape, dtype=F32)
        self.got = program.tile(6, *shape, dtype=F32)
        self.sems = program.sems(2, 6)
        self.local = program.sems(1)

    def bind(self, ref):
        self.refs = Bag(
            total=ref(self.total),
            held=ref(self.held),
            got=ref(self.got),
            sems=ref(self.sems),
            local=ref(self.local),
        )
        return self

    def run(self):
        r = self.refs
        held, got = r.held, r.got
        z, up, down = line_place()
        is_outer = jnp.logical_or(z == 0, z == 3)
        low = z < 2
        step = lambda k, at: hop(held, got.at[k], r.sems, k, at)

        def towards(k, first, second):
            pl.when(low)(lambda: step(k, first).start())
            pl.when(jnp.logical_not(low))(lambda: step(k, second).start())

        for k, (bit, turn) in enumerate(((CORE, 1), (X, 2), (Y, 4))):
            step(k, bit).start()
            step(k, bit).wait()
            held[0:8] += got[k, 0:8]
            for p in range(8):
                held[8 + p] += got[k, 8 + (p ^ turn)]

        @pl.when(is_outer)
        def _():
            towards(3, up, down)
            step(3, up).wait_send()
            step(5, up).wait_recv()
            held[...] = got[5]

        @pl.when(jnp.logical_not(is_outer))
        def _():
            step(3, up).wait_recv()
            held[...] += got[3]
            towards(4, up, down)
            step(4, up).wait()
            held[...] += got[4]
            towards(5, down, up)
            step(5, up).wait_send()

        fetch(held, r.total, r.local.at[0]).wait()


class Stream:
    def __init__(self, program, group, unit, width):
        self.group, self.unit = group, unit
        self.held = program.tile(2, group, 2, unit, width)
        self.sems = program.sems(2, group * 2)

    def bind(self, ref):
        self.refs = ref(self.held), ref(self.sems)
        return self

    def _copies(self, gather, index, slot, size):
        held, sems = self.refs
        return [
            pltpu.make_async_copy(
                gather.piece((index * self.group + g) // 2, (index * self.group + g) % 2, c).at[
                    pl.ds(0, size)
                ],
                held.at[slot, g, c, pl.ds(0, size)],
                sems.at[slot, 2 * g + c],
            )
            for g in range(self.group)
            for c in range(2)
        ]

    def begin(self, gather, index, size=None):
        for each in self._copies(gather, index, index % 2, size or self.unit):
            each.start()

    def bring(self, gather, step, first, last, size=None):
        size = size or self.unit
        for index in range(first + 1, last):
            pl.when(step == index - 1 - first)(
                lambda index=index: self.begin(gather, index, size)
            )
        slot = lax.rem(step + first, 2)
        for each in self._copies(gather, 0, slot, size):
            each.wait()
        held = self.refs[0]
        return held[slot, :, :, 0:size].reshape(-1, held.shape[-1])


def prepare_body(
    slot_ref, live_ref, im_ref, go_ref, gain_ref, shift_ref, own_ref, row_ref,
    x_ref, g_ref, n_ref, s_ref, early_ref, bias_ref, sems,
):
    step = pl.program_id(0)
    slot = slot_ref[0]
    hops = [lambda lane=lane: hop(own_ref.at[lax.rem(lax.axis_index(DP), 2), lane], early_ref.at[lane], sems, lane, LANES[lane]) for lane in range(2)]
    for r in range(1, 4):
        to = {TENSOR: lax.axis_index(TENSOR) ^ r}
        hops.append(lambda r=r, to=to: hop(row_ref, bias_ref.at[r - 1], sems, 1 + r, to))

    @pl.when(step == 0)
    def _():
        meet((X, Y, XY))
        for each in hops[2:] + hops[:2]:
            each().start()

    def pick(ref):
        values = ref[...].astype(F32)
        chosen = values[:, 0]
        for index in range(1, values.shape[1]):
            chosen = jnp.where(slot == index, values[:, index], chosen)
        return chosen

    picture = pick(im_ref)
    centered = picture - row_mean(picture)
    inverse = lax.rsqrt(row_mean(centered * centered) + EPS)
    normed = centered * inverse * gain_ref[...] + shift_ref[...]
    x_ref[...] = picture.T.astype(BF)
    g_ref[...] = (pick(go_ref) * live_ref[0].astype(F32)).T.astype(BF)
    n_ref[...] = normed.T.astype(BF)
    s_ref[0:1, :] = row_mean(picture).T
    s_ref[1:2, :] = inverse.T

    @pl.when(step == pl.num_programs(0) - 1)
    def _():
        for each in hops:
            each().wait()


def prepare(images, grad_out, slot, live, gain, shift, own, bias):
    slots, length, width = images.shape
    rows = 128
    scalar = pl.BlockSpec(memory_space=pltpu.SMEM)
    tokens = pl.BlockSpec((rows, slots, width), lambda i: (i, 0, 0))
    vector = pl.BlockSpec((1, width), lambda i: (0, 0))
    return pl.pallas_call(
        prepare_body,
        grid=(pl.cdiv(length, rows),),
        in_specs=[scalar, scalar, tokens, tokens, vector, vector, ANYWHERE, ANYWHERE],
        out_specs=[pl.BlockSpec((width, rows), lambda i: (0, i))] * 3
        + [pl.BlockSpec((2, rows), lambda i: (0, i)), ANYWHERE, ANYWHERE],
        out_shape=[jax.ShapeDtypeStruct((width, length), BF)] * 3
        + [
            jax.ShapeDtypeStruct((2, length), F32),
            jax.ShapeDtypeStruct(own.shape[1:], BF),
            jax.ShapeDtypeStruct((3, *bias.shape), F32),
        ],
        scratch_shapes=[pltpu.SemaphoreType.DMA((2, 5))],
        compiler_params=pltpu.CompilerParams(
            vmem_limit_bytes=50 << 20, collective_id=1, has_side_effects=True
        ),
        name="prepare",
    )(slot, live, images.transpose(1, 0, 2), grad_out.transpose(1, 0, 2), gain, shift, own, bias)


def as_column(row):
    return jnp.broadcast_to(row, (8, row.shape[1])).T[:, 0:1]


def as_row(column):
    return jnp.broadcast_to(column, (column.shape[0], 8)).T[0:1, :]


def attend_head(weight, normed, bias, qkv_ref, o_ref, lse_ref):
    length = normed.shape[1]
    rows = dot_nn(weight, normed)
    queries = ((rows[:HD] + bias[0]) * (LOG2E / math.sqrt(HD))).astype(BF)
    keys_t = rows[HD : 2 * HD].astype(BF)
    values = (rows[2 * HD :] + bias[1]).astype(BF)
    qkv_ref[0, 0] = queries
    qkv_ref[0, 1] = keys_t
    qkv_ref[0, 2] = values
    keys = keys_t.T
    for start in range(0, length, QUERY_BLOCK):
        block = slice(start, min(start + QUERY_BLOCK, length))
        scores = dot_nn(keys, queries[:, block])
        top = jnp.max(scores, axis=0, keepdims=True)
        weights = jnp.exp2(scores - top)
        total = jnp.sum(weights, axis=0, keepdims=True)
        mixed = dot_nn(values, weights.astype(BF))
        o_ref[0, :, block] = (mixed * (1.0 / total)).astype(BF)
        lse_ref[0, :, block] = top + jnp.log2(total)


def attend_back_head(qkv_ref, do_ref, o_ref, lse_ref, d_ref, dk_acc, dv_acc):
    keys_t = qkv_ref[0, 1]
    keys = keys_t.T
    values = qkv_ref[0, 2].T
    length = keys_t.shape[1]
    scale = 1.0 / math.sqrt(HD)
    for start in range(0, length, QUERY_BLOCK):
        block = slice(start, min(start + QUERY_BLOCK, length))
        queries_t = qkv_ref[0, 0, :, block]
        pull_t = do_ref[0, :, block]
        delta = jnp.sum(
            pull_t.astype(F32) * o_ref[0, :, block].astype(F32), axis=0, keepdims=True
        )
        probs = jnp.exp2(dot_nn(keys, queries_t) - lse_ref[0, :, block])
        probs_low = probs.astype(BF)
        d_probs = dot_nn(values, pull_t)
        d_scores = (probs * (d_probs - delta)).astype(BF)
        d_ref[0, 0, :, block] = (dot_nn(keys_t, d_scores) * scale).astype(BF)
        d_keys = dot_nn(d_scores, queries_t.T)
        d_values = dot_nn(probs_low, pull_t.T)
        if start == 0:
            dk_acc[...] = d_keys
            dv_acc[...] = d_values
        else:
            dk_acc[...] += d_keys
            dv_acc[...] += d_values
    d_ref[0, 1] = (dk_acc[...].T * LN2).astype(BF)
    d_ref[0, 2] = dv_acc[...].T.astype(BF)
    return [jnp.sum(d_ref[0, k].astype(F32), axis=1, keepdims=True) for k in (0, 2)]


def columns_of(length, block=128):
    return [slice(start, min(start + block, length)) for start in range(0, length, block)]


def norm_back(grad, unit_values, inverse, gain):
    scaled = grad * gain
    mean = lambda values: jnp.mean(values, axis=0, keepdims=True)
    return inverse * (scaled - mean(scaled) - unit_values * mean(scaled * unit_values))


def turned(values, axis, bit):
    return jnp.where(bit == 1, lax.rev(values, (axis,)), values)


def forward(attn_own, early, fc1_own, bias, bias_far, picture, normed_one, vectors):
    width, length = picture.shape
    chunk = attn_own.shape[2]
    unit = fc1_own.shape[2]
    rows = 2 * unit
    heads = 16
    p = Program("forward", (X, Y, CORE))
    own, soon, own_fc1 = p.input(attn_own), p.input(early), p.input(fc1_own)
    bias_in, x_in, n_in, v_in = p.input(bias), p.input(picture), p.input(normed_one), p.input(vectors)
    bias_far_in = p.input(bias_far)
    attn = Gather(p, own, attn_own.shape, soon)
    fc1 = Gather(p, own_fc1, fc1_own.shape)
    stream = Stream(p, 1, unit, width)
    qkv, mixed = p.output(heads, 3, HD, length), p.output(heads, HD, length)
    lse = p.output(heads, 1, length, dtype=F32)
    residual, normed = p.output(2, width, 384, dtype=F32), p.output(width, length)
    stats, out_all = p.output(2, length, dtype=F32), p.output(heads, HD, width)
    act, slope = p.output(8, rows, length), p.output(8, rows, length)
    held = Bag(
        bias=p.tile(4, *bias.shape, dtype=F32),
        x=p.tile(width, length),
        n=p.tile(width, length),
        v=p.tile(*vectors.shape, dtype=F32),
        o=p.tile(heads, HD, length),
        w=p.tile(heads, HD, width),
        h=p.tile(2, width, 384, dtype=F32),
        n2=p.tile(width, length),
        s=p.tile(2, length, dtype=F32),
    )
    sems, wsems = p.sems(8), p.sems(heads)

    def script(ref):
        hold = held.each(ref)
        sem, wsem = ref(sems), ref(wsems)
        attn.bind(ref)
        fc1.bind(ref)
        stream.bind(ref)
        attn.start()
        attn.forward()
        fc1.start()
        copies = [
            fetch(ref(n_in), hold.n, sem.at[0]),
            fetch(ref(bias_in), hold.bias.at[0], sem.at[1]),
            fetch(ref(bias_far_in), hold.bias.at[pl.ds(1, 3)], sem.at[2]),
            fetch(ref(x_in), hold.x, sem.at[5]),
            fetch(ref(v_in), hold.v, sem.at[6]),
        ]
        for each in copies[:3]:
            each.wait()

        def heads_of(first, count, part_of, sources, specs, events=()):
            def body(step, *refs):
                weights, (qkv_ref, o_ref, lse_ref) = refs[: len(sources)], refs[len(sources) :]
                shard, half, lane = part_of(step)
                rows_of = lambda w: w[...].reshape(chunk, width)[: 3 * HD]
                weight = rows_of(weights[0])
                if len(weights) > 2:
                    weight = jnp.where(lane == shard - 1, rows_of(weights[2]), weight)
                if len(weights) > 1:
                    weight = jnp.where(half == 0, weight, rows_of(weights[1]))
                at = 4 * half + 2 * lane
                shift = [
                    as_column(hold.bias[shard, at + k, :, 0:HD]) for k in range(2)
                ]
                attend_head(weight, hold.n[...], shift, qkv_ref, o_ref, lse_ref)
                hold.o[first + step] = o_ref[0]

            phase(
                count,
                body,
                sources,
                specs,
                [ref(qkv), ref(mixed), ref(lse)],
                [
                    spec((1, 3, HD, length), lambda i: (first + i, 0, 0, 0)),
                    spec((1, HD, length), lambda i: (first + i, 0, 0)),
                    spec((1, 1, length), lambda i: (first + i, 0, 0)),
                ],
                events,
            )

        def bring_out(shard):
            return [
                pltpu.make_async_copy(
                    attn.piece(shard, half, lane).at[pl.ds(3 * HD, HD)],
                    hold.w.at[4 * shard + 2 * half + lane],
                    wsem.at[4 * shard + 2 * half + lane],
                )
                for half in range(2)
                for lane in range(2)
            ]

        heads_of(
            0,
            4,
            lambda i: (0, i // 2, lax.rem(i, 2)),
            [ref(own).at[lax.rem(lax.axis_index(DP) + part, 2)] for part in range(2)],
            [spec((1, chunk, width), lambda i: (lax.rem(i, 2), 0, 0))] * 2,
        )
        attn.near_here()
        attn.near_whole()
        mine = lambda i: (i // 4, 1 - i // 4, 0, 0)
        heads_of(
            4,
            8,
            lambda i: (1 + i // 4, lax.rem(i // 2, 2), lax.rem(i, 2)),
            [ref(attn.near), ref(attn.near_part), ref(soon)],
            [
                spec((1, 1, chunk, width), mine),
                spec((1, 1, chunk, width), lambda i: (i // 4, lax.rem(i, 2), 0, 0)),
                spec((1, chunk, width), lambda i: (i // 4, 0, 0)),
            ],
        )
        attn.far_here()
        for shard in range(3):
            for each in bring_out(shard):
                each.start()
        attn.far_whole()
        for each in bring_out(3):
            each.start()
        heads_of(
            12,
            4,
            lambda i: (3, i // 2, lax.rem(i, 2)),
            [ref(attn.far), ref(attn.far_part)],
            [spec((1, chunk, width), lambda i: (lax.rem(i, 2), 0, 0))] * 2,
        )
        fc1.forward()
        for each in copies[3:]:
            each.wait()
        for shard in range(4):
            for each in bring_out(shard):
                each.wait()
        stream.begin(fc1, 0)
        store_w = fetch(hold.w, ref(out_all), sem.at[4])
        weight = hold.w[...].reshape(width, width)
        for block in columns_of(length, 384):
            mix = hold.o[:, :, block].reshape(width, -1)
            values = hold.x[:, block].astype(F32) + contract_rows(weight, mix)
            values = values + hold.v[:, 2:3]
            average = jnp.mean(values, axis=0, keepdims=True)
            centered = values - average
            inverse = lax.rsqrt(jnp.mean(centered * centered, axis=0, keepdims=True) + EPS)
            hold.h[block.start // 384, :, 0 : block.stop - block.start] = values
            hold.n2[:, block] = (
                centered * inverse * hold.v[:, 3:4] + hold.v[:, 4:5]
            ).astype(BF)
            hold.s[0:1, block] = average
            hold.s[1:2, block] = inverse
        stores = [store_w] + [
            fetch(source, ref(target), sem.at[k])
            for k, (source, target) in enumerate(((hold.h, residual), (hold.n2, normed), (hold.s, stats)))
        ]

        def hidden(step, act_ref, slope_ref):
            weight = stream.bring(fc1, step, 0, 8)
            shard, half = step // 2, lax.rem(step, 2)
            shift = as_column(hold.bias[shard, half, :, 128 : 128 + rows])
            preact = dot_nn(weight, hold.n2[...]) + shift
            square = preact * preact
            curve = jnp.tanh(preact * (GELU_A + (GELU_A * GELU_B) * square))
            rise = 0.5 * (1.0 + curve)
            act_ref[0] = (preact * rise).astype(BF)
            inner = GELU_A + (3.0 * GELU_A * GELU_B) * square
            slope_ref[0] = (rise + (0.5 * preact) * (1.0 - curve * curve) * inner).astype(BF)

        block = spec((1, rows, length), lambda i: (i, 0, 0))

        def near_all():
            fc1.near_here()
            fc1.near_whole()

        def far_all():
            fc1.far_here()
            fc1.far_whole()

        phase(
            8, hidden, [], [], [ref(act), ref(slope)], [block, block],
            [(1, near_all), (5, far_all)],
        )
        for each in stores:
            each.wait()
        attn.drain()
        fc1.drain()

    result = p.call(script, 2, 3e10)
    return (
        gathered(attn).each(result),
        gathered(fc1).each(result),
        Bag(
            qkv=qkv,
            mixed=mixed,
            lse=lse,
            residual=residual,
            normed_two=normed,
            stats_two=stats,
            out_all=out_all,
            act=act,
            slope=slope,
        ).each(result),
    )


def gathered(source):
    return Bag(
        near=source.near, near_part=source.near_part, far=source.far, far_part=source.far_part
    )


class Ready:
    def __init__(self, program, own, parts, early=None):
        self.handles = parts.each(program.input)
        self.handles.own = program.input(own)
        self.handles.early = None if early is None else program.input(early)
        self.early = early

    def bind(self, ref):
        self.refs = self.handles.each(lambda h: None if h is None else ref(h))
        return self

    piece = Gather.piece


def backward(arrays, fc1_parts, attn_parts, owns, early, live):
    width, length = arrays.picture.shape
    share = width // 4
    unit = owns.fc2.shape[2]
    rows = 2 * unit
    block = 3 * HD
    p = Program("backward", (X, Y, XY, CORE, LINE))
    into = arrays.each(p.input)
    live_in = p.input(live, pl.BlockSpec(memory_space=pltpu.SMEM))
    fc1 = Ready(p, owns.fc1, fc1_parts)
    attn = Ready(p, owns.attn, attn_parts, early)
    fc2 = Gather(p, p.input(owns.fc2), owns.fc2.shape)
    stream = Stream(p, 2, unit, width)

    fc_shape, out_shape, qkv_shape = ((4, 2, u, width) for u in (unit, HD, block))
    shapes = (fc_shape, fc_shape, out_shape, qkv_shape)
    plane = [Plane(p, shape) for shape in shapes[:QKV]]
    plane.append(Plane(p, shapes[QKV], plane[FC2]))
    line = [Line(p, shape[1:]) for shape in shapes[:QKV]]
    line.append(Line(p, shapes[QKV][1:], line[FC2]))
    d_pre = p.output(8, rows, length)
    pull = p.output(16, HD, length)
    d_qkv = p.output(16, 3, HD, length)
    block_rows, input_rows = p.output(4, share, length), p.output(4, share, length)
    spread_block = Spread(p, block_rows, (4, share, length))
    spread_input = Spread(p, input_rows, (4, share, length))
    vectors = Vectors(p, (16, 1, width))
    held = Bag(
        upstream=p.tile(width, length),
        normed_two=p.tile(width, length),
        normed_one=p.tile(width, length),
        low=p.tile(width, length),
        residual=p.tile(width, 384, dtype=F32),
        acc=p.tile(width, length, dtype=F32),
        vectors=p.tile(*arrays.vectors.shape, dtype=F32),
        cols=p.tile(width, 8, dtype=F32),
        stats_two=p.tile(2, length, dtype=F32),
        stats_one=p.tile(2, length, dtype=F32),
        dk=p.tile(length, HD, dtype=F32),
        dv=p.tile(length, HD, dtype=F32),
        rows=p.tile(2, rows, length),
        heads=p.tile(2, 2, 3, HD, length),
        part=p.tile(2, 2, unit, width),
    )
    tile_sems = p.sems(2)
    sems = p.sems(12)

    def script(ref):
        hold = held.each(ref)
        sem = ref(sems)
        for each in (fc1, attn, fc2, stream, spread_block, spread_input, vectors):
            each.bind(ref)
        for group in (plane, line):
            for each in group:
                each.bind(ref)
        vec = vectors.refs.held
        array = into.each(ref)
        live_now = ref(live_in)[0].astype(F32)

        copies = Bag(
            upstream=fetch(array.upstream, hold.upstream, sem.at[0]),
            normed_two=fetch(array.normed_two, hold.normed_two, sem.at[1]),
            vectors=fetch(array.vectors, hold.vectors, sem.at[3]),
            stats_two=fetch(array.stats_two, hold.stats_two, sem.at[4]),
            normed_one=fetch(array.normed_one, hold.normed_one, sem.at[5]),
            stats_one=fetch(array.stats_one, hold.stats_one, sem.at[6]),
        )
        fc2.start()
        stream.begin(fc2, 0)
        vec[...] = jnp.zeros(vec.shape, F32)
        hold.cols[...] = jnp.zeros(hold.cols.shape, F32)
        copies.upstream.wait()
        copies.normed_two.wait()

        tile_sem = ref(tile_sems)

        def rows_in(source, index, slot):
            if len(source.shape) == 3 and source.shape[0] == 8:
                target = hold.rows.at[slot]
                source = source.at[index]
            elif len(source.shape) == 3:
                target = hold.heads.at[slot, :, 0]
                source = source.at[pl.ds(2 * index, 2)]
            else:
                target = hold.heads.at[slot]
                source = source.at[pl.ds(2 * index, 2)]
            return pltpu.make_async_copy(source, target, tile_sem.at[slot])

        def rows_of(source, slot, count):
            if len(source.shape) == 3 and source.shape[0] == 8:
                return hold.rows[slot]
            if len(source.shape) == 3:
                return hold.heads[slot, :, 0].reshape(count, length)
            return hold.heads[slot].reshape(count, length)

        def gradient(source, other, name, shards, go=True):
            _, _, size, _ = shapes[name]
            count = 2 * size
            total = len(shards)

            def pick(i):
                if total == 1:
                    return shards[0]
                if total == 2:
                    return jnp.where(i == 0, shards[0], shards[1])
                return jnp.where(
                    i < 2,
                    jnp.where(i == 0, shards[0], shards[1]),
                    jnp.where(i == 2, shards[2], shards[3]),
                )

            part_of = lambda slot, lane: hold.part.at[slot, lane, pl.ds(0, size)]
            sums_of = plane[name]
            piece = lambda k: jnp.where(
                k < total, 2 * pick(k) + 1, 2 * pick(jnp.maximum(k - total, 0))
            )
            rows_in(source, 2 * shards[0] + 1, 0).start()

            def product(k):
                slot = lax.rem(k, 2)

                @pl.when(k + 1 < 2 * total)
                def _():
                    rows_in(source, piece(k + 1), 1 - slot).start()

                rows_in(source, 0, slot).wait()
                return contract_cols(rows_of(source, slot, count), other[...])

            def give(i, _):
                slot = lax.rem(i, 2)
                sums = product(i).astype(BF).reshape(2, size, width)
                shard = pick(i)

                @pl.when(i >= 2)
                def _():
                    for lane in range(2):
                        sums_of.swap(
                            part_of(slot, lane), pick(jnp.maximum(i - 2, 0)), lane
                        ).wait_send()

                for lane in range(2):
                    part_of(slot, lane)[...] = sums[lane]
                for each in shards:

                    @pl.when(shard == each)
                    def _():
                        for lane in range(2):
                            sums_of.swap(part_of(slot, lane), each, lane, each).start()

                return 0

            def keep(i, _):
                shard = pick(i)
                sums = product(total + i).reshape(2, size, width)
                for each in shards:

                    @pl.when(shard == each)
                    def _():
                        for lane in range(2):
                            sums_of.swap(part_of(0, lane), each, lane, each).wait_recv()
                            sums_of.add(each, lane, sums[lane], go)

                return 0

            lax.fori_loop(0, total, give, 0)
            lax.fori_loop(0, total, keep, 0)
            for i in range(max(total - 2, 0), total):
                for lane in range(2):
                    sums_of.swap(part_of(i % 2, lane), shards[i], lane).wait_send()

        every = (3, 1, 2, 0)
        gradient(array.act, hold.upstream, FC2, every, False)

        def hidden(first, count, events=()):
            def body(step, slope_ref, d_ref):
                weight = stream.bring(fc2, step, first, first + count)
                for half in range(2):
                    values = dot_nn(weight[half * rows : (half + 1) * rows], hold.upstream[...])
                    values = (values * slope_ref[half].astype(F32)).astype(BF)
                    d_ref[half] = values
                    sums = jnp.sum(values.astype(F32), axis=1, keepdims=True)
                    vec[8 + 2 * (first + step) + half, :, 0:rows] = as_row(sums)

            pair = spec((2, rows, length), lambda i: (first + i, 0, 0))
            phase(count, body, [array.slope], [pair], [ref(d_pre)], [pair], events)

        fc2.forward()
        plane[FC2].launch()
        hidden(0, 1)
        fc2.near_here()
        fc2.near_whole()
        stream.begin(fc2, 1)
        hidden(1, 2)
        fc2.far_here()
        fc2.far_whole()
        stream.begin(fc2, 3)
        hidden(3, 1)

        def back(weights, values, lead, size, events=()):
            def body(step, d_ref):
                weight = stream.bring(weights, step, 0, 4, size)
                values = d_ref[...].reshape(4 * size, length)
                sums = contract_rows(weight, values)

                @pl.when(step == 0)
                def _():
                    hold.acc[...] = sums

                @pl.when(step > 0)
                def _():
                    hold.acc[...] += sums

            tail = values.shape[1:]
            zeros = (0,) * len(tail)
            phase(4, body, [values], [spec((lead, *tail), lambda i: (i, *zeros))], [], [], events)

        stream.begin(fc1, 0)
        back(fc1, ref(d_pre), 2, unit)
        for each in (copies.vectors, copies.stats_two):
            each.wait()
        total = lambda values: jnp.sum(values, axis=1, keepdims=True)
        residual_of = halves_of(array.residual, hold.residual, sem.at[2])
        for cut in columns_of(length):
            inverse = hold.stats_two[1:2, cut]
            grad = hold.acc[:, cut]
            units = (residual_of(cut) - hold.stats_two[0:1, cut]) * inverse
            up = hold.upstream[:, cut].astype(F32)
            d_residual = up + norm_back(grad, units, inverse, hold.vectors[:, 3:4])
            hold.low[:, cut] = d_residual.astype(BF)
            hold.cols[:, 2:3] += total(d_residual)
            hold.cols[:, 3:4] += total(grad * units)
            hold.cols[:, 4:5] += total(grad)
            hold.cols[:, 5:6] += total(up)

        plane[FC2].forward()
        plane[FC2].settle()
        picture_copy = fetch(array.picture, hold.upstream, sem.at[7])

        def pull_body(step, w_ref, o_ref):
            weight = w_ref[...].reshape(4 * HD, width)
            o_ref[...] = dot_nn(weight, hold.low[...]).reshape(4, HD, length).astype(BF)

        quarter = lambda *tail: spec((4, *tail), lambda i: (i, *(0 for _ in tail)))
        phase(
            4, pull_body, [array.out_all], [quarter(HD, width)], [ref(pull)], [quarter(HD, length)]
        )
        gradient(ref(d_pre), hold.normed_two, FC1, every)
        plane[FC2].finish(line[FC2])
        plane[FC2].drain()
        gradient(array.mixed, hold.low, OUT, every)
        copies.normed_one.wait()

        def heads_back(shards, events):
            shard_of = lambda i: jnp.where(i < 4, shards[0], shards[-1])
            at = lambda i: 4 * shard_of(i) + lax.rem(i, 4)

            def body(step, qkv_ref, do_ref, o_ref, lse_ref, d_ref):
                sums = attend_back_head(
                    qkv_ref, do_ref, o_ref, lse_ref, d_ref, hold.dk, hold.dv
                )
                row = 8 + 2 * shard_of(step) + lax.rem(step // 2, 2)
                for k in range(2):
                    where = pl.multiple_of(640 + 128 * (2 * lax.rem(step, 2) + k), 128)
                    padded = jnp.concatenate(
                        [as_row(sums[k]), jnp.zeros((1, 128 - HD), F32)], axis=1
                    )
                    vec[row, :, pl.ds(where, 128)] = padded

            flat = spec((1, HD, length), lambda i: (at(i), 0, 0))
            many = spec((1, 3, HD, length), lambda i: (at(i), 0, 0, 0))
            phase(
                4 * len(shards),
                body,
                [array.qkv, ref(pull), array.mixed, array.lse],
                [many, flat, flat, spec((1, 1, length), lambda i: (at(i), 0, 0))],
                [ref(d_qkv)],
                [many],
                events,
            )

        def settle(name):
            plane[name].forward()
            plane[name].settle()

        heads_back((3, 1), [(6, lambda: line[FC2].meet(0))])
        settle(FC1)
        gradient(ref(d_qkv), hold.normed_one, QKV, (3, 1))
        heads_back((2,), [(1, lambda: line[FC2].meet(1)), (3, lambda: line[FC2].leave(0))])
        gradient(ref(d_qkv), hold.normed_one, QKV, (2,))
        settle(OUT)
        plane[FC1].finish(line[FC1])
        heads_back((0,), [(1, lambda: line[FC2].leave(1)), (3, lambda: line[FC2].collect(0))])
        gradient(ref(d_qkv), hold.normed_one, QKV, (0,))
        plane[QKV].forward()
        line[FC1].meet(0)
        plane[OUT].finish(line[OUT])
        stream.begin(fc2, 0)
        back(
            fc2,
            array.act,
            2,
            unit,
            [(2, lambda: plane[QKV].settle()), (2, lambda: line[FC2].collect(1)), (3, lambda: line[FC1].meet(1))],
        )
        for k in range(2):
            line[FC2].done(k)
        plane[QKV].finish(line[QKV])
        stream.begin(attn, 0, block)
        residual_of = halves_of(array.residual, hold.residual, sem.at[2])
        for cut in columns_of(length):
            values = residual_of(cut) + hold.acc[:, cut] + hold.vectors[:, 5:6]
            hold.normed_two[:, cut] = (values * live_now).astype(BF)
        store_rows(hold.normed_two, ref(block_rows), sem, share)
        spread_block.start()
        line[FC1].leave(0)
        line[OUT].meet(0)
        line[OUT].meet(1)
        picture_copy.wait()
        copies.stats_one.wait()
        back(
            attn,
            ref(d_qkv),
            4,
            block,
            [(2, lambda: line[FC1].leave(1)), (3, lambda: line[QKV].meet(0))],
        )
        line[OUT].leave(0)
        line[OUT].leave(1)
        line[FC1].collect(0)
        for cut in columns_of(length):
            inverse = hold.stats_one[1:2, cut]
            grad = hold.acc[:, cut]
            units = hold.upstream[:, cut].astype(F32) - hold.stats_one[0:1, cut]
            units = units * inverse
            d_input = hold.low[:, cut].astype(F32) + norm_back(
                grad, units, inverse, hold.vectors[:, 0:1]
            )
            hold.normed_two[:, cut] = d_input.astype(BF)
            hold.cols[:, 0:1] += total(grad * units)
            hold.cols[:, 1:2] += total(grad)
        store_rows(hold.normed_two, ref(input_rows), sem, share)
        spread_input.start()
        line[QKV].meet(1)
        line[QKV].leave(0)
        wide = hold.cols[...].T
        for k in range(8):
            vec[k] = wide[k : k + 1]
        vectors.run()
        line[QKV].leave(1)
        line[FC1].collect(1)
        for k in range(2):
            line[OUT].collect(k)
        for k in range(2):
            line[QKV].collect(k)
        spread_block.finish()
        spread_input.finish()
        for each in line[1:]:
            for k in range(2):
                each.done(k)
        for each in plane[1:]:
            each.drain()
        fc2.drain()

    result = p.call(script, 3, 8e10)
    sums = [(result(each.total), result(each.other)) for each in line]
    spreads = [
        (result(block_rows), result(spread_block.landed)),
        (result(input_rows), result(spread_input.landed)),
    ]
    return sums, spreads, result(vectors.total)[:, 0]


def halves_of(source, held, sem):
    width = held.shape[1]

    def bring(part):
        return fetch(source.at[part], held, sem)

    bring(0).wait()

    def columns(cut):
        if cut.start == width:
            bring(1).wait()
        first = cut.start % width
        return held[:, first : first + cut.stop - cut.start]

    return columns


def store_rows(source, target, sem, share):
    copies = [
        fetch(source.at[pl.ds(k * share, share)], target.at[k], sem.at[k]) for k in range(4)
    ]
    for each in copies:
        each.wait()


def finish(sums, spreads, place_t, core, hidden):
    width = sums[FC2][0].shape[-1]
    share, length = spreads[0][0].shape[1:]

    def body(at, *refs):
        step = pl.program_id(0)
        same = lax.rem(step // 2 + at[1], 2) == 0
        ins, outs = refs[:12], refs[12:]
        for k in range(4):
            rows = jnp.where(same, ins[2 * k][0], ins[2 * k + 1][0]).astype(F32)
            outs[k][...] = rows.reshape(outs[k].shape)
        for k in range(2):
            rows = jnp.where(step == at[0], ins[8 + 2 * k][0], ins[9 + 2 * k][0])
            outs[4 + k][0] = rows.astype(F32)

    half = lambda array: pl.BlockSpec((1, *array.shape[1:]), lambda i, at: (lax.rem(i, 2), 0, 0))
    own = pl.BlockSpec((1, share, length), lambda i, at: (at[0], 0, 0))
    landed = pl.BlockSpec(
        (1, share, length), lambda i, at: (jnp.maximum((i ^ at[0]) - 1, 0), 0, 0)
    )
    units = [pair[0].shape[1] for pair in sums]
    rows = lambda unit: pl.BlockSpec((unit, width), lambda i, at: (i, 0))
    slot = pl.BlockSpec((1, share, length), lambda i, at: (i, 0, 0))
    shape = lambda *dims: jax.ShapeDtypeStruct(dims, F32)
    return pl.pallas_call(
        body,
        grid_spec=pltpu.PrefetchScalarGridSpec(
            num_scalar_prefetch=1,
            grid=(4,),
            in_specs=[half(array) for pair in sums for array in pair] + [own, landed] * 2,
            out_specs=[
                rows(units[FC2]),
                rows(units[FC1]),
                rows(units[OUT]),
                pl.BlockSpec((3, HD, width), lambda i, at: (0, i, 0)),
                slot,
                slot,
            ],
        ),
        out_shape=[
            shape(hidden, width),
            shape(hidden, width),
            shape(share, width),
            shape(3, share, width),
            shape(4, share, length),
            shape(4, share, length),
        ],
        compiler_params=pltpu.CompilerParams(vmem_limit_bytes=50 << 20),
        name="finish",
    )(
        jnp.stack([place_t, core]).astype(jnp.int32),
        *[array for pair in sums for array in pair],
        *spreads[0],
        *spreads[1],
    )


def whole_image(
    images,
    counts,
    ln1_gain,
    ln1_bias,
    qkv_weight,
    qv_bias,
    out_weight,
    out_bias,
    ln2_gain,
    ln2_bias,
    fc1_weight,
    fc1_bias,
    fc2_weight,
    fc2_bias,
    grad_out,
):
    slot_count, length, width = images.shape
    share = width // 4
    hidden = fc1_weight.shape[1]
    unit = -(-hidden // 64) * 16
    rows = 2 * unit
    place_t = lax.axis_index(TENSOR)
    core = lax.rem(lax.axis_index(DP), 2)
    block = 3 * HD

    qkv_rows = qkv_weight.reshape(3, width, 2, 2, HD).transpose(2, 3, 0, 4, 1)
    attn_own = jnp.concatenate(
        [qkv_rows.reshape(2, 2, block, width), out_weight.reshape(2, 2, HD, width)], axis=2
    )
    pad = 2 * rows - hidden
    fc1_own, fc2_own = (
        jnp.pad(each, ((0, pad), (0, 0))).reshape(2, 2, unit, width)
        for each in (fc1_weight.T, fc2_weight)
    )
    head_bias = qv_bias.reshape(2, 2, 2, HD).transpose(1, 2, 0, 3)
    head_bias = jnp.pad(turned(head_bias, 0, core).reshape(8, HD), ((0, 0), (0, 128 - HD)))
    hidden_bias = turned(jnp.pad(fc1_bias, (0, pad)).reshape(2, rows), 0, core)
    hidden_bias = jnp.pad(hidden_bias, ((0, 6), (0, 640 - rows)))
    bias = jnp.concatenate([head_bias, hidden_bias], axis=1).astype(F32)[:, None]
    vectors = jnp.stack(
        [ln1_gain, ln1_bias, out_bias, ln2_gain, ln2_bias, fc2_bias, fc2_bias, fc2_bias], axis=1
    ).astype(F32)
    live = (place_t < counts[0]).astype(jnp.int32)[None]

    picture, upstream, normed_one, stats_one, early, bias_far = prepare(
        images,
        grad_out,
        place_t[None].astype(jnp.int32),
        live,
        ln1_gain.astype(F32)[None],
        ln1_bias.astype(F32)[None],
        attn_own,
        bias,
    )
    attn_parts, fc1_parts, made = forward(
        attn_own, early, fc1_own, bias, bias_far, picture, normed_one, vectors
    )
    made.__dict__.update(
        upstream=upstream,
        picture=picture,
        normed_one=normed_one,
        stats_one=stats_one,
        vectors=vectors,
    )
    owns = Bag(attn=attn_own, fc1=fc1_own, fc2=fc2_own)
    sums, spreads, totals = backward(made, fc1_parts, attn_parts, owns, early, live)

    own_wide = lax.dynamic_slice_in_dim(totals[:6], place_t * share, share, 1)
    own_rows = turned(totals[8:10], 0, core)
    own_hidden = own_rows[:, :rows].reshape(-1)[:hidden]
    own_qv = own_rows[:, 640:].reshape(2, 2, 2, 128)[..., :HD].transpose(2, 0, 1, 3)
    own_qv = own_qv.reshape(2, share)

    fc2_result, fc1_result, out_result, qkv_result, block_result, input_result = finish(
        sums, spreads, place_t, core, hidden
    )
    return (
        block_result.transpose(0, 2, 1),
        input_result.transpose(0, 2, 1),
        own_wide[0],
        own_wide[1],
        qkv_result.transpose(0, 2, 1),
        own_qv,
        out_result,
        own_wide[2],
        own_wide[3],
        own_wide[4],
        fc1_result.T,
        own_hidden,
        fc2_result,
        own_wide[5],
    )


def solution(mesh):
    whole_fits = mesh.shape[TENSOR] == 4 and mesh.shape[DP] == 8
    return jax.shard_map(
        whole_image if whole_fits else local,
        mesh=mesh,
        in_specs=(
            P(DP, None, None),
            P(DP),
            P(),
            P(),
            P(None, None, TENSOR),
            P(None, TENSOR),
            P(TENSOR, None),
            P(),
            P(),
            P(),
            P(None, TENSOR),
            P(TENSOR),
            P(TENSOR, None),
            P(),
            P(DP, None, None),
        ),
        out_specs=(
            P(DP, None, TENSOR),
            P(DP, None, TENSOR),
            P(TENSOR),
            P(TENSOR),
            P(None, None, TENSOR),
            P(None, TENSOR),
            P(TENSOR, None),
            P(TENSOR),
            P(TENSOR),
            P(TENSOR),
            P(None, TENSOR),
            P(TENSOR),
            P(TENSOR, None),
            P(TENSOR),
        ),
        check_vma=False,
    )
```

```python
import math

import jax
import jax.numpy as jnp
from jax import lax
from jax.experimental import pallas as pl
from jax.experimental.pallas import tpu as pltpu
from jax.sharding import PartitionSpec as P

HD = 72


EPS = 1e-06


def own_columns(values, share_width):
    start = lax.axis_index(TENSOR) * share_width
    return lax.dynamic_slice_in_dim(values, start, share_width, values.ndim - 1)


def row_mean(values):
    return jnp.mean(values, axis=-1, keepdims=True)


def group_stats(first, second):
    return lax.psum((first, second), TENSOR)


def contract_rows(left, right):
    return lax.dot_general(
        left, right, (((0,), (0,)), ((), ())), preferred_element_type=jnp.float32
    )


def contract_cols(left, right):
    return lax.dot_general(
        left, right, (((1,), (1,)), ((), ())), preferred_element_type=jnp.float32
    )


def gelu_tanh(values):
    return jax.nn.gelu(values, approximate=True)


def local(
    images,
    counts,
    ln1_gain,
    ln1_bias,
    qkv_weight,
    qv_bias,
    out_weight,
    out_bias,
    ln2_gain,
    ln2_bias,
    fc1_weight,
    fc1_bias,
    fc2_weight,
    fc2_bias,
    grad_out,
):
    slot_count, length, full_width = images.shape
    share_width = full_width // lax.axis_size(TENSOR)
    local_width = qkv_weight.shape[2]
    local_heads = local_width // HD
    hidden_width = fc1_weight.shape[1]
    score_scale = 1.0 / math.sqrt(HD)
    gain_one = ln1_gain.astype(jnp.float32)
    shift_one = ln1_bias.astype(jnp.float32)
    gain_two = ln2_gain.astype(jnp.float32)
    shift_two = ln2_bias.astype(jnp.float32)
    bias_out = out_bias.astype(jnp.float32)
    bias_fc1 = fc1_bias.astype(jnp.float32)
    bias_fc2 = fc2_bias.astype(jnp.float32)
    bias_query = qv_bias[0].astype(jnp.float32)
    bias_value = qv_bias[1].astype(jnp.float32)
    live_count = counts[0]

    def to_heads(values):
        return values.reshape(length, local_heads, HD)

    def head_scores(query_heads, key_heads):
        return (
            jnp.einsum("qhd,khd->hqk", query_heads, key_heads, preferred_element_type=jnp.float32)
            * score_scale
        )

    def layer_step(slot_index, loop_state):
        block_acc, input_acc, grads = loop_state
        (
            grad_gain_one,
            grad_shift_one,
            grad_qkv,
            grad_qv,
            grad_out_w,
            grad_out_b,
            grad_gain_two,
            grad_shift_two,
            grad_fc1_w,
            grad_fc1_b,
            grad_fc2_w,
            grad_fc2_b,
        ) = grads
        live_flag = (slot_index < live_count).astype(jnp.float32)
        picture = lax.dynamic_index_in_dim(images, slot_index, 0, keepdims=False).astype(
            jnp.float32
        )
        upstream = (
            lax.dynamic_index_in_dim(grad_out, slot_index, 0, keepdims=False).astype(jnp.float32)
            * live_flag
        )
        upstream_low = upstream.astype(jnp.bfloat16)
        centered = picture - row_mean(picture)
        inv_one = lax.rsqrt(row_mean(centered * centered) + EPS)
        unit_one = centered * inv_one
        normed_one = (unit_one * gain_one + shift_one).astype(jnp.bfloat16)
        query_rows = (
            jnp.dot(normed_one, qkv_weight[0], preferred_element_type=jnp.float32) + bias_query
        ).astype(jnp.bfloat16)
        key_rows = jnp.dot(normed_one, qkv_weight[1], preferred_element_type=jnp.float32).astype(
            jnp.bfloat16
        )
        value_rows = (
            jnp.dot(normed_one, qkv_weight[2], preferred_element_type=jnp.float32) + bias_value
        ).astype(jnp.bfloat16)
        query_heads = to_heads(query_rows)
        key_heads = to_heads(key_rows)
        value_heads = to_heads(value_rows)
        scores = head_scores(query_heads, key_heads)
        row_top = jnp.max(scores, axis=-1, keepdims=True)
        logsum = row_top + jnp.log(jnp.sum(jnp.exp(scores - row_top), axis=-1, keepdims=True))
        probs_low = jnp.exp(scores - logsum).astype(jnp.bfloat16)
        mixed = jnp.einsum(
            "hqk,khd->qhd", probs_low, value_heads, preferred_element_type=jnp.float32
        )
        mixed = mixed.reshape(length, local_width).astype(jnp.bfloat16)
        partial_out = jnp.dot(mixed, out_weight, preferred_element_type=jnp.float32).astype(
            jnp.bfloat16
        )
        residual = (
            own_columns(picture, share_width)
            + lax.psum_scatter(partial_out, TENSOR, scatter_dimension=1, tiled=True).astype(
                jnp.float32
            )
            + own_columns(bias_out, share_width)
        )
        row_sum, row_square = group_stats(
            jnp.sum(residual, axis=-1), jnp.sum(residual * residual, axis=-1)
        )
        average = row_sum[:, None] / full_width
        inv_two = lax.rsqrt(row_square[:, None] / full_width - average * average + EPS)
        unit_two = (residual - average) * inv_two
        own_normed = (
            unit_two * own_columns(gain_two, share_width) + own_columns(shift_two, share_width)
        ).astype(jnp.bfloat16)
        normed_two = lax.all_gather(own_normed, TENSOR, axis=1, tiled=True)
        preact = jnp.dot(normed_two, fc1_weight, preferred_element_type=jnp.float32) + bias_fc1
        activated = gelu_tanh(preact).astype(jnp.bfloat16)
        partial_mlp = jnp.dot(activated, fc2_weight, preferred_element_type=jnp.float32).astype(
            jnp.bfloat16
        )
        block_rows = (
            residual
            + lax.psum_scatter(partial_mlp, TENSOR, scatter_dimension=1, tiled=True).astype(
                jnp.float32
            )
            + own_columns(bias_fc2, share_width)
        )
        block_rows = block_rows * live_flag
        grad_fc2_b = grad_fc2_b + own_columns(jnp.sum(upstream, axis=0), share_width)
        grad_fc2_w = grad_fc2_w + contract_rows(activated, upstream_low)
        d_act = contract_cols(upstream_low, fc2_weight)
        gelu_pull = jax.vjp(gelu_tanh, preact)[1]
        d_pre = gelu_pull(d_act)[0].astype(jnp.bfloat16)
        grad_fc1_b = grad_fc1_b + jnp.sum(d_pre.astype(jnp.float32), axis=0)
        grad_fc1_w = grad_fc1_w + contract_rows(normed_two, d_pre)
        back_mlp = contract_cols(d_pre, fc1_weight)
        d_norm_two = lax.psum_scatter(
            back_mlp.astype(jnp.bfloat16), TENSOR, scatter_dimension=1, tiled=True
        ).astype(jnp.float32)
        scaled_two = d_norm_two * own_columns(gain_two, share_width)
        sum_plain, sum_cross = group_stats(
            jnp.sum(scaled_two, axis=-1), jnp.sum(scaled_two * unit_two, axis=-1)
        )
        d_residual = own_columns(upstream, share_width) + inv_two * (
            scaled_two
            - sum_plain[:, None] / full_width
            - unit_two * (sum_cross[:, None] / full_width)
        )
        grad_gain_two = grad_gain_two + jnp.sum(d_norm_two * unit_two, axis=0)
        grad_shift_two = grad_shift_two + jnp.sum(d_norm_two, axis=0)
        grad_out_b = grad_out_b + jnp.sum(d_residual, axis=0)
        d_residual_low = lax.all_gather(
            d_residual.astype(jnp.bfloat16), TENSOR, axis=1, tiled=True
        )
        grad_out_w = grad_out_w + contract_rows(mixed, d_residual_low)
        d_mixed_heads = to_heads(contract_cols(d_residual_low, out_weight).astype(jnp.bfloat16))
        probs = jnp.exp(head_scores(query_heads, key_heads) - logsum)
        probs_again = probs.astype(jnp.bfloat16)
        d_value = jnp.einsum(
            "hqk,qhd->khd", probs_again, d_mixed_heads, preferred_element_type=jnp.float32
        )
        d_probs = jnp.einsum(
            "qhd,khd->hqk", d_mixed_heads, value_heads, preferred_element_type=jnp.float32
        )
        inner = jnp.sum(probs * d_probs, axis=-1, keepdims=True)
        d_scores = (probs * (d_probs - inner)).astype(jnp.bfloat16)
        d_query = (
            jnp.einsum("hqk,khd->qhd", d_scores, key_heads, preferred_element_type=jnp.float32)
            * score_scale
        )
        d_key = (
            jnp.einsum("hqk,qhd->khd", d_scores, query_heads, preferred_element_type=jnp.float32)
            * score_scale
        )
        d_stack = (
            jnp.stack([d_query, d_key, d_value], axis=1)
            .reshape(length, 3, local_width)
            .astype(jnp.bfloat16)
        )
        grad_qkv = grad_qkv + jnp.einsum(
            "ld,lje->jde", normed_one, d_stack, preferred_element_type=jnp.float32
        )
        bias_sums = jnp.sum(d_stack.astype(jnp.float32), axis=0)
        grad_qv = grad_qv + jnp.stack([bias_sums[0], bias_sums[2]])
        back_attn = jnp.einsum(
            "lje,jde->ld", d_stack, qkv_weight, preferred_element_type=jnp.float32
        )
        d_norm_one = lax.psum_scatter(
            back_attn.astype(jnp.bfloat16), TENSOR, scatter_dimension=1, tiled=True
        ).astype(jnp.float32)
        own_unit = own_columns(unit_one, share_width)
        scaled_one = d_norm_one * own_columns(gain_one, share_width)
        plain_one, cross_one = group_stats(
            jnp.sum(scaled_one, axis=-1), jnp.sum(scaled_one * own_unit, axis=-1)
        )
        d_input = d_residual + inv_one * (
            scaled_one
            - plain_one[:, None] / full_width
            - own_unit * (cross_one[:, None] / full_width)
        )
        grad_gain_one = grad_gain_one + jnp.sum(d_norm_one * own_unit, axis=0)
        grad_shift_one = grad_shift_one + jnp.sum(d_norm_one, axis=0)
        block_acc = lax.dynamic_update_index_in_dim(block_acc, block_rows, slot_index, 0)
        input_acc = lax.dynamic_update_index_in_dim(input_acc, d_input, slot_index, 0)
        new_grads = (
            grad_gain_one,
            grad_shift_one,
            grad_qkv,
            grad_qv,
            grad_out_w,
            grad_out_b,
            grad_gain_two,
            grad_shift_two,
            grad_fc1_w,
            grad_fc1_b,
            grad_fc2_w,
            grad_fc2_b,
        )
        return (block_acc, input_acc, new_grads)

    share_zeros = jnp.zeros((share_width,), jnp.float32)
    start_grads = (
        share_zeros,
        share_zeros,
        jnp.zeros((3, full_width, local_width), jnp.float32),
        jnp.zeros((2, local_width), jnp.float32),
        jnp.zeros((local_width, full_width), jnp.float32),
        share_zeros,
        share_zeros,
        share_zeros,
        jnp.zeros((full_width, hidden_width), jnp.float32),
        jnp.zeros((hidden_width,), jnp.float32),
        jnp.zeros((hidden_width, full_width), jnp.float32),
        share_zeros,
    )
    start_rows = jnp.zeros((slot_count, length, share_width), jnp.float32)
    block_acc, input_acc, grads = lax.fori_loop(
        0, slot_count, layer_step, (start_rows, start_rows, start_grads)
    )
    (
        grad_gain_one,
        grad_shift_one,
        grad_qkv,
        grad_qv,
        grad_out_w,
        grad_out_b,
        grad_gain_two,
        grad_shift_two,
        grad_fc1_w,
        grad_fc1_b,
        grad_fc2_w,
        grad_fc2_b,
    ) = grads
    summed = (
        lax.psum(grad_gain_one.astype(jnp.bfloat16), DP).astype(jnp.float32),
        lax.psum(grad_shift_one.astype(jnp.bfloat16), DP).astype(jnp.float32),
        lax.psum(grad_qkv.astype(jnp.bfloat16), DP).astype(jnp.float32),
        lax.psum(grad_qv.astype(jnp.bfloat16), DP).astype(jnp.float32),
        lax.psum(grad_out_w.astype(jnp.bfloat16), DP).astype(jnp.float32),
        lax.psum(grad_out_b.astype(jnp.bfloat16), DP).astype(jnp.float32),
        lax.psum(grad_gain_two.astype(jnp.bfloat16), DP).astype(jnp.float32),
        lax.psum(grad_shift_two.astype(jnp.bfloat16), DP).astype(jnp.float32),
        lax.psum(grad_fc1_w.astype(jnp.bfloat16), DP).astype(jnp.float32),
        lax.psum(grad_fc1_b.astype(jnp.bfloat16), DP).astype(jnp.float32),
        lax.psum(grad_fc2_w.astype(jnp.bfloat16), DP).astype(jnp.float32),
        lax.psum(grad_fc2_b.astype(jnp.bfloat16), DP).astype(jnp.float32),
    )
    return (
        block_acc,
        input_acc,
        summed[0],
        summed[1],
        summed[2],
        summed[3],
        summed[4],
        summed[5],
        summed[6],
        summed[7],
        summed[8],
        summed[9],
        summed[10],
        summed[11],
    )


LOG2E = math.log2(math.e)
LN2 = math.log(2.0)
GELU_A = math.sqrt(2.0 / math.pi)
GELU_B = 0.044715
BF = jnp.bfloat16
F32 = jnp.float32
QUERY_BLOCK = 256
MESH = pl.DeviceIdType.MESH
TENSOR, DP = "tensor", "dp"
X, Y, XY, CORE, LINE = range(5)
TURN = {X: 1, Y: 2, XY: 3}
OTHER = {X: Y, Y: X}
SIDE = {X: 0, Y: 1}
LANES = (X, Y)
FC2, FC1, OUT, QKV = range(4)
INWARD, ACROSS, BACK, SWAP = range(4)


class Bag:
    def __init__(self, **things):
        self.__dict__.update(things)

    def each(self, action):
        return Bag(**{name: action(thing) for name, thing in self.__dict__.items()})
ANYWHERE = pl.BlockSpec(memory_space=pl.ANY)


def dot_nn(left, right):
    return lax.dot_general(left, right, (((1,), (0,)), ((), ())), preferred_element_type=F32)


def place(bit):
    if bit == CORE:
        return {DP: lax.axis_index(DP) ^ 1}
    return {TENSOR: lax.axis_index(TENSOR) ^ TURN[bit]}


def hop(source, target, sems, index, to):
    return pltpu.make_async_remote_copy(
        src_ref=source,
        dst_ref=target,
        send_sem=sems.at[0, index],
        recv_sem=sems.at[1, index],
        device_id=place(to) if isinstance(to, int) else to,
        device_id_type=MESH,
    )


def line_place():
    dp = lax.axis_index(DP)
    return dp // 2, {DP: lax.rem(dp + 2, 8)}, {DP: lax.rem(dp + 6, 8)}


class Program:
    def __init__(self, name, partners):
        self.name = name
        self.partners = partners
        self.arrays, self.specs, self.shapes, self.scratches = [], [], [], []

    def input(self, array, spec=ANYWHERE):
        self.arrays.append(array)
        self.specs.append(spec)
        return (0, len(self.arrays) - 1)

    def output(self, *shape, dtype=BF):
        self.shapes.append(jax.ShapeDtypeStruct(shape, dtype))
        return (1, len(self.shapes) - 1)

    def scratch(self, spec):
        self.scratches.append(spec)
        return (2, len(self.scratches) - 1)

    def tile(self, *shape, dtype=BF):
        return self.scratch(pltpu.VMEM(shape, dtype))

    def sems(self, *shape):
        return self.scratch(pltpu.SemaphoreType.DMA(shape))

    def call(self, script, collective_id, cost):
        count_in, count_out = len(self.arrays), len(self.shapes)

        def kernel(*refs):
            pools = (
                refs[:count_in],
                refs[count_in : count_in + count_out],
                refs[count_in + count_out :],
            )
            meet(self.partners)
            script(lambda handle: pools[handle[0]][handle[1]])

        results = pl.pallas_call(
            kernel,
            in_specs=self.specs,
            out_specs=[ANYWHERE] * count_out,
            out_shape=self.shapes,
            scratch_shapes=self.scratches,
            compiler_params=pltpu.CompilerParams(
                vmem_limit_bytes=67_043_328, collective_id=collective_id, has_side_effects=True
            ),
            cost_estimate=pl.CostEstimate(
                flops=int(cost), bytes_accessed=1 << 26, transcendentals=0
            ),
            name=self.name,
        )(*self.arrays)
        return lambda handle: results[handle[1]]


def meet(partners):
    barrier = pltpu.get_barrier_semaphore()
    signal = lambda at: pl.semaphore_signal(barrier, inc=1, device_id=at, device_id_type=MESH)
    for bit in partners:
        if bit == XY:
            signal({TENSOR: lax.axis_index(TENSOR) ^ 3})
        elif bit != LINE:
            signal(place(bit))
    singles = len([bit for bit in partners if bit != LINE])
    if LINE in partners:
        z, up, down = line_place()
        pl.when(z < 3)(lambda: signal(up))
        pl.when(z > 0)(lambda: signal(down))
        inner = jnp.logical_and(z > 0, z < 3)
        pl.when(inner)(lambda: pl.semaphore_wait(barrier, singles + 2))
        pl.when(jnp.logical_not(inner))(lambda: pl.semaphore_wait(barrier, singles + 1))
    else:
        pl.semaphore_wait(barrier, singles)


def phase(steps, body, ins, in_specs, outs, out_specs, events=()):
    def inner(at, *refs):
        step = at.index[0]
        for when, event in events:
            pl.when(step == when)(event)
        body(step, *refs)

    pltpu.emit_pipeline(
        inner, grid=(steps,), in_specs=in_specs, out_specs=out_specs, _explicit_indices=True
    )(*ins, *outs)


def fetch(source, target, sem):
    copy = pltpu.make_async_copy(source, target, sem)
    copy.start()
    return copy


def spec(shape, index):
    return pl.BlockSpec(shape, index)


class Gather:
    def __init__(self, program, own, shape, early=None):
        _, count, unit, width = shape
        self.own = own
        self.early = early
        self.near = program.output(2, count, unit, width)
        self.near_part = program.output(2, count, unit, width)
        self.far = program.output(count, unit, width)
        self.far_part = program.output(count, unit, width)
        self.sems = program.sems(2, 12)

    def bind(self, ref):
        self.refs = Bag(
            own=ref(self.own),
            near=ref(self.near),
            near_part=ref(self.near_part),
            far=ref(self.far),
            far_part=ref(self.far_part),
            sems=ref(self.sems),
            early=None if self.early is None else ref(self.early),
        )
        return self

    def piece(self, shard, part, lane):
        r = self.refs
        if shard == 0:
            return r.own.at[lax.rem(lax.axis_index(DP) + part, 2), lane]
        if shard == 3:
            return (r.far_part if part else r.far).at[lane]
        if self.early is not None and part == 0 and LANES[lane] == LANES[shard - 1]:
            return r.early.at[lane]
        return (r.near_part if part else r.near).at[shard - 1, lane]

    def _near(self, bit, lane):
        r = self.refs
        k = SIDE[bit]
        own = self.piece(0, 0, lane)
        return hop(own, r.near.at[k, lane], r.sems, 2 * lane + k, bit)

    def _far(self, lane):
        first = LANES[lane]
        source = self.piece(1 + SIDE[first], 0, lane)
        return hop(source, self.refs.far.at[lane], self.refs.sems, 4 + lane, OTHER[first])

    def _swap(self, shard, lane):
        target = self.piece(shard, 1, lane)
        index = 6 + 2 * (shard - 1) + lane
        return hop(self.piece(shard, 0, lane), target, self.refs.sems, index, CORE)

    def start(self):
        for first in (True, False):
            for lane, bit in enumerate(LANES):
                if first and self.early is None:
                    self._near(bit, lane).start()
                if not first:
                    self._near(OTHER[bit], lane).start()

    def forward(self):
        for lane, first in enumerate(LANES):
            if self.early is None:
                self._near(first, lane).wait_recv()
            self._far(lane).start()
            self._swap(1 + SIDE[first], lane).start()

    def near_here(self):
        for lane, first in enumerate(LANES):
            self._near(OTHER[first], lane).wait_recv()
            self._swap(1 + SIDE[OTHER[first]], lane).start()

    def near_whole(self):
        for lane in range(2):
            for shard in (1, 2):
                self._swap(shard, lane).wait_recv()

    def far_here(self):
        for lane in range(2):
            self._far(lane).wait_recv()
            self._swap(3, lane).start()

    def far_whole(self):
        for lane in range(2):
            self._swap(3, lane).wait_recv()

    def drain(self):
        for lane, first in enumerate(LANES):
            if self.early is None:
                self._near(first, lane).wait_send()
            self._near(OTHER[first], lane).wait_send()
            self._far(lane).wait_send()
            for shard in (1, 2, 3):
                self._swap(shard, lane).wait_send()


class Plane:
    def __init__(self, program, shape, share=None):
        _, count, unit, width = shape
        self.unit = unit
        if share is None:
            self.both = program.tile(2, count, 2, unit, width)
            self.got = program.tile(count, 2, unit, width)
            self.last = program.tile(count, unit, width)
        else:
            self.both, self.got, self.last = share.both, share.got, share.last
        self.sems = program.sems(2, 6)
        self.swap_sems = program.sems(2, 8)

    def bind(self, ref):
        self.refs = [ref(h) for h in (self.both, self.got, self.last, self.sems)]
        self.swaps = ref(self.swap_sems)
        return self

    def _part(self, which, *at):
        return self.refs[which].at[*at, pl.ds(0, self.unit)]

    @staticmethod
    def entry(shard, lane):
        odd, high = lax.rem(shard, 2), shard // 2
        return (odd, high) if LANES[lane] == X else (high, odd)

    def tile(self, shard, lane):
        gone, k = self.entry(shard, lane)
        return self._part(0, gone, lane, k)

    def swap(self, source, shard, lane):
        return hop(source, self.tile(shard, lane), self.swaps, 2 * shard + lane, CORE)

    def _first(self, lane, k):
        source = self._part(0, 1, lane, k)
        return hop(source, self._part(1, lane, k), self.refs[3], 2 * lane + k, LANES[lane])

    def _next(self, lane):
        source = self._part(0, 0, lane, 1)
        return hop(
            source, self._part(2, lane), self.refs[3], 4 + lane, OTHER[LANES[lane]]
        )

    def add(self, shard, sums, go):
        for lane in range(2):
            tile = self.tile(shard, lane)
            tile[...] = (sums[lane] + tile[...].astype(F32)).astype(BF)
        if go:
            for lane in range(2):
                gone, k = self.entry(shard, lane)
                pl.when(gone == 1)(lambda lane=lane, k=k: self._first(lane, k).start())

    def launch(self):
        for k in (1, 0):
            for lane in range(2):
                self._first(lane, k).start()

    def _add(self, lane, k):
        self._first(lane, k).wait_recv()
        base = self._part(0, 0, lane, k)
        base[...] = base[...] + self._part(1, lane, k)[...]

    def forward(self):
        for lane in (1, 0):
            self._add(lane, 1)
            self._next(lane).start()

    def settle(self):
        for lane in range(2):
            self._add(lane, 0)

    def finish(self, line):
        for lane in range(2):
            self._next(lane).wait_recv()
            line.take(lane, self._part(0, 0, lane, 0)[...] + self._part(2, lane)[...])

    def drain(self):
        for lane in range(2):
            self._next(lane).wait_send()
            for k in range(2):
                self._first(lane, k).wait_send()


class Line:
    def __init__(self, program, shape, share=None):
        count, unit, width = shape
        self.unit = unit
        self.total = program.output(*shape)
        self.other = program.output(*shape)
        if share is None:
            self.held = program.tile(*shape)
            self.outer = program.tile(*shape)
            self.middle = program.tile(*shape)
        else:
            self.held, self.outer, self.middle = share.held, share.outer, share.middle
        self.sems = program.sems(2, 4 * count)
        self.local = program.sems(count)
        self.count = count

    def bind(self, ref):
        self.refs = Bag(
            total=ref(self.total),
            other=ref(self.other),
            held=ref(self.held).at[:, pl.ds(0, self.unit)],
            outer=ref(self.outer).at[:, pl.ds(0, self.unit)],
            middle=ref(self.middle).at[:, pl.ds(0, self.unit)],
            sems=ref(self.sems),
            local=ref(self.local),
        )
        z, up, down = line_place()
        self.up, self.down = up, down
        self.is_outer = jnp.logical_or(z == 0, z == 3)
        self.is_inner = jnp.logical_not(self.is_outer)
        self.low = z < 2
        return self

    def _hop(self, kind, k, at):
        r = self.refs
        target = (r.outer, r.middle, r.outer, r.other)[kind]
        return hop(r.held.at[k], target.at[k], r.sems, kind * self.count + k, at)

    def _store(self, k):
        r = self.refs
        return pltpu.make_async_copy(r.held.at[k], r.total.at[k], r.local.at[k])

    def _send(self, kind, k):
        if kind == BACK:
            low, high = self.down, self.up
        else:
            low, high = self.up, self.down
        pl.when(self.low)(lambda: self._hop(kind, k, low).start())
        pl.when(jnp.logical_not(self.low))(lambda: self._hop(kind, k, high).start())

    def take(self, k, values):
        self.refs.held[k] = values
        pl.when(self.is_outer)(lambda: self._send(INWARD, k))

    def meet(self, k):
        r = self.refs

        @pl.when(self.is_inner)
        def _():
            self._hop(INWARD, k, self.up).wait_recv()
            r.held[k] += r.outer[k]
            self._send(ACROSS, k)

    def leave(self, k):
        r = self.refs

        @pl.when(self.is_inner)
        def _():
            self._hop(ACROSS, k, self.up).wait()
            r.held[k] += r.middle[k]
            self._send(BACK, k)
            self._hop(SWAP, k, CORE).start()
            self._store(k).start()

    def collect(self, k):
        r = self.refs

        @pl.when(self.is_outer)
        def _():
            self._hop(INWARD, k, self.up).wait_send()
            self._hop(BACK, k, self.up).wait_recv()
            r.held[k] = r.outer[k]
            self._hop(SWAP, k, CORE).start()
            self._store(k).start()

    def done(self, k):
        pl.when(self.is_inner)(lambda: self._hop(BACK, k, self.up).wait_send())
        self._store(k).wait()
        self._hop(SWAP, k, CORE).wait()


class Spread:
    def __init__(self, program, rows, shape):
        self.rows = rows
        self.landed = program.output(3, *shape[1:])
        self.sems = program.sems(2, 3)

    def bind(self, ref):
        self.refs = ref(self.rows), ref(self.landed), ref(self.sems)
        return self

    def _hop(self, r):
        rows, landed, sems = self.refs
        to = lax.axis_index(TENSOR) ^ r
        return hop(rows.at[to], landed.at[r - 1], sems, r - 1, {TENSOR: to})

    def start(self):
        for r in (3, 1, 2):
            self._hop(r).start()

    def finish(self):
        for r in (1, 2, 3):
            self._hop(r).wait()


class Vectors:
    def __init__(self, program, shape):
        self.total = program.output(*shape, dtype=F32)
        self.held = program.tile(*shape, dtype=F32)
        self.got = program.tile(6, *shape, dtype=F32)
        self.sems = program.sems(2, 6)
        self.local = program.sems(1)

    def bind(self, ref):
        self.refs = Bag(
            total=ref(self.total),
            held=ref(self.held),
            got=ref(self.got),
            sems=ref(self.sems),
            local=ref(self.local),
        )
        return self

    def _step(self, k, at):
        r = self.refs
        return hop(r.held, r.got.at[k], r.sems, k, at)

    def plane(self):
        held, got = self.refs.held, self.refs.got
        for k, (bit, turn) in enumerate(((CORE, 1), (X, 2), (Y, 4))):
            self._step(k, bit).start()
            self._step(k, bit).wait()
            held[0:8] += got[k, 0:8]
            for p in range(8):
                held[8 + p] += got[k, 8 + (p ^ turn)]

    def line(self):
        r = self.refs
        held, got = r.held, r.got
        z, up, down = line_place()
        is_outer = jnp.logical_or(z == 0, z == 3)
        low = z < 2

        def towards(k, first, second):
            pl.when(low)(lambda: self._step(k, first).start())
            pl.when(jnp.logical_not(low))(lambda: self._step(k, second).start())

        @pl.when(is_outer)
        def _():
            towards(3, up, down)
            self._step(3, up).wait_send()

        @pl.when(jnp.logical_not(is_outer))
        def _():
            self._step(3, up).wait_recv()
            held[...] += got[3]
            towards(4, up, down)
            self._step(4, up).wait()
            held[...] += got[4]
            towards(5, down, up)

        def last():
            @pl.when(is_outer)
            def _():
                self._step(5, up).wait_recv()
                held[...] = got[5]

            pl.when(jnp.logical_not(is_outer))(lambda: self._step(5, up).wait_send())
            fetch(held, r.total, r.local.at[0]).wait()

        return last


class Stream:
    def __init__(self, program, group, unit, width):
        self.group, self.unit = group, unit
        self.held = program.tile(2, group, 2, unit, width)
        self.sems = program.sems(2, group * 2)

    def bind(self, ref):
        self.refs = ref(self.held), ref(self.sems)
        return self

    def _copies(self, gather, index, slot, size):
        held, sems = self.refs
        return [
            pltpu.make_async_copy(
                gather.piece((index * self.group + g) // 2, (index * self.group + g) % 2, c).at[
                    pl.ds(0, size)
                ],
                held.at[slot, g, c, pl.ds(0, size)],
                sems.at[slot, 2 * g + c],
            )
            for g in range(self.group)
            for c in range(2)
        ]

    def begin(self, gather, index, size=None):
        for each in self._copies(gather, index, index % 2, size or self.unit):
            each.start()

    def here(self, gather, slot):
        for each in self._copies(gather, 0, slot, self.unit):
            each.wait()

    def bring(self, gather, step, first, last, size=None):
        size = size or self.unit
        for index in range(first + 1, last):
            pl.when(step == index - 1 - first)(
                lambda index=index: self.begin(gather, index, size)
            )
        slot = lax.rem(step + first, 2)
        for each in self._copies(gather, 0, slot, size):
            each.wait()
        held = self.refs[0]
        return held[slot, :, :, 0:size].reshape(-1, held.shape[-1])


def prepare_body(
    slot_ref, live_ref, im_ref, go_ref, gain_ref, shift_ref, own_ref, row_ref,
    x_ref, g_ref, n_ref, s_ref, early_ref, bias_ref, sems,
):
    step = pl.program_id(0)
    slot = slot_ref[0]
    hops = [lambda lane=lane: hop(own_ref.at[lax.rem(lax.axis_index(DP), 2), lane], early_ref.at[lane], sems, lane, LANES[lane]) for lane in range(2)]
    for r in range(1, 4):
        to = {TENSOR: lax.axis_index(TENSOR) ^ r}
        hops.append(lambda r=r, to=to: hop(row_ref, bias_ref.at[r - 1], sems, 1 + r, to))

    @pl.when(step == 0)
    def _():
        meet((X, Y, XY))
        for each in hops[2:] + hops[:2]:
            each().start()

    def pick(ref):
        values = ref[...].astype(F32)
        chosen = values[:, 0]
        for index in range(1, values.shape[1]):
            chosen = jnp.where(slot == index, values[:, index], chosen)
        return chosen

    picture = pick(im_ref)
    centered = picture - row_mean(picture)
    inverse = lax.rsqrt(row_mean(centered * centered) + EPS)
    normed = centered * inverse * gain_ref[...] + shift_ref[...]
    x_ref[...] = picture.T.astype(BF)
    g_ref[...] = (pick(go_ref) * live_ref[0].astype(F32)).T.astype(BF)
    n_ref[...] = normed.T.astype(BF)
    s_ref[0:1, :] = row_mean(picture).T
    s_ref[1:2, :] = inverse.T

    @pl.when(step == pl.num_programs(0) - 1)
    def _():
        for each in hops:
            each().wait()


def prepare(images, grad_out, slot, live, gain, shift, own, bias):
    slots, length, width = images.shape
    rows = 128
    scalar = pl.BlockSpec(memory_space=pltpu.SMEM)
    tokens = pl.BlockSpec((rows, slots, width), lambda i: (i, 0, 0))
    vector = pl.BlockSpec((1, width), lambda i: (0, 0))
    return pl.pallas_call(
        prepare_body,
        grid=(pl.cdiv(length, rows),),
        in_specs=[scalar, scalar, tokens, tokens, vector, vector, ANYWHERE, ANYWHERE],
        out_specs=[pl.BlockSpec((width, rows), lambda i: (0, i))] * 3
        + [pl.BlockSpec((2, rows), lambda i: (0, i)), ANYWHERE, ANYWHERE],
        out_shape=[jax.ShapeDtypeStruct((width, length), BF)] * 3
        + [
            jax.ShapeDtypeStruct((2, length), F32),
            jax.ShapeDtypeStruct(own.shape[1:], BF),
            jax.ShapeDtypeStruct((3, *bias.shape), F32),
        ],
        scratch_shapes=[pltpu.SemaphoreType.DMA((2, 5))],
        compiler_params=pltpu.CompilerParams(
            vmem_limit_bytes=67_043_328, collective_id=1, has_side_effects=True
        ),
        name="prepare",
    )(slot, live, images.transpose(1, 0, 2), grad_out.transpose(1, 0, 2), gain, shift, own, bias)


def as_column(row):
    return jnp.broadcast_to(row, (8, row.shape[1])).T[:, 0:1]


def as_row(column):
    return jnp.broadcast_to(column, (column.shape[0], 8)).T[0:1, :]


def attend_head(weight, normed, bias, qkv_ref, o_ref, lse_ref):
    length = normed.shape[1]
    rows = dot_nn(weight, normed)
    queries = ((rows[:HD] + bias[0]) * (LOG2E / math.sqrt(HD))).astype(BF)
    keys_t = rows[HD : 2 * HD].astype(BF)
    values = (rows[2 * HD :] + bias[1]).astype(BF)
    qkv_ref[0, 0] = queries
    qkv_ref[0, 1] = keys_t
    qkv_ref[0, 2] = values
    keys = keys_t.T
    for start in range(0, length, QUERY_BLOCK):
        block = slice(start, min(start + QUERY_BLOCK, length))
        scores = dot_nn(keys, queries[:, block])
        top = jnp.max(scores, axis=0, keepdims=True)
        weights = jnp.exp2(scores - top)
        total = jnp.sum(weights, axis=0, keepdims=True)
        mixed = dot_nn(values, weights.astype(BF))
        o_ref[0, :, block] = (mixed * (1.0 / total)).astype(BF)
        lse_ref[0, :, block] = top + jnp.log2(total)


def attend_back_head(qkv_ref, do_ref, o_ref, lse_ref, d_ref, dk_acc, dv_acc):
    keys_t = qkv_ref[0, 1]
    keys = keys_t.T
    values = qkv_ref[0, 2].T
    length = keys_t.shape[1]
    scale = 1.0 / math.sqrt(HD)
    for start in range(0, length, QUERY_BLOCK):
        block = slice(start, min(start + QUERY_BLOCK, length))
        queries_t = qkv_ref[0, 0, :, block]
        pull_t = do_ref[0, :, block]
        delta = jnp.sum(
            pull_t.astype(F32) * o_ref[0, :, block].astype(F32), axis=0, keepdims=True
        )
        probs = jnp.exp2(dot_nn(keys, queries_t) - lse_ref[0, :, block])
        probs_low = probs.astype(BF)
        d_probs = dot_nn(values, pull_t)
        d_scores = (probs * (d_probs - delta)).astype(BF)
        d_ref[0, 0, :, block] = (dot_nn(keys_t, d_scores) * scale).astype(BF)
        d_keys = dot_nn(d_scores, queries_t.T)
        d_values = dot_nn(probs_low, pull_t.T)
        if start == 0:
            dk_acc[...] = d_keys
            dv_acc[...] = d_values
        else:
            dk_acc[...] += d_keys
            dv_acc[...] += d_values
    d_ref[0, 1] = (dk_acc[...].T * LN2).astype(BF)
    d_ref[0, 2] = dv_acc[...].T.astype(BF)
    return [jnp.sum(d_ref[0, k].astype(F32), axis=1, keepdims=True) for k in (0, 2)]


def columns_of(length, block=128):
    return [slice(start, min(start + block, length)) for start in range(0, length, block)]


def norm_back(grad, unit_values, inverse, gain):
    scaled = grad * gain
    mean = lambda values: jnp.mean(values, axis=0, keepdims=True)
    return inverse * (scaled - mean(scaled) - unit_values * mean(scaled * unit_values))


def turned(values, axis, bit):
    return jnp.where(bit == 1, lax.rev(values, (axis,)), values)


def forward(attn_own, early, fc1_own, bias, bias_far, picture, normed_one, vectors):
    width, length = picture.shape
    chunk = attn_own.shape[2]
    unit = fc1_own.shape[2]
    rows = 2 * unit
    heads = 16
    p = Program("forward", (X, Y, CORE))
    own, soon, own_fc1 = p.input(attn_own), p.input(early), p.input(fc1_own)
    bias_in, x_in, n_in, v_in = p.input(bias), p.input(picture), p.input(normed_one), p.input(vectors)
    bias_far_in = p.input(bias_far)
    attn = Gather(p, own, attn_own.shape, soon)
    fc1 = Gather(p, own_fc1, fc1_own.shape)
    stream = Stream(p, 1, unit, width)
    qkv, mixed = p.output(heads, 3, HD, length), p.output(heads, HD, length)
    lse = p.output(heads, 1, length, dtype=F32)
    residual, normed = p.output(3, width, 256, dtype=F32), p.output(width, length)
    stats, out_all = p.output(2, length, dtype=F32), p.output(heads, HD, width)
    act, slope = p.output(8, rows, length), p.output(8, rows, length)
    held = Bag(
        bias=p.tile(4, *bias.shape, dtype=F32),
        x=p.tile(width, length),
        n=p.tile(width, length),
        v=p.tile(*vectors.shape, dtype=F32),
        o=p.tile(heads, HD, length),
        w=p.tile(heads, HD, width),
        h=p.tile(3, width, 256, dtype=F32),
        n2=p.tile(width, length),
        s=p.tile(2, length, dtype=F32),
        rows=p.tile(2, 3 * HD, width),
    )
    sems, wsems, hsems = p.sems(8), p.sems(heads), p.sems(2)

    def script(ref):
        hold = held.each(ref)
        sem, wsem, hsem = ref(sems), ref(wsems), ref(hsems)
        attn.bind(ref)
        fc1.bind(ref)
        stream.bind(ref)
        attn.start()
        attn.forward()
        fc1.start()
        copies = [
            fetch(ref(n_in), hold.n, sem.at[0]),
            fetch(ref(bias_in), hold.bias.at[0], sem.at[1]),
            fetch(ref(bias_far_in), hold.bias.at[pl.ds(1, 3)], sem.at[2]),
            fetch(ref(x_in), hold.x, sem.at[5]),
            fetch(ref(v_in), hold.v, sem.at[6]),
        ]
        for each in copies[:3]:
            each.wait()

        def weights_in(head, slot):
            shard, half, lane = head // 4, (head // 2) % 2, head % 2
            return pltpu.make_async_copy(
                attn.piece(shard, half, lane).at[pl.ds(0, 3 * HD)], hold.rows.at[slot], hsem.at[slot]
            )

        def near_all():
            attn.near_here()
            attn.near_whole()

        def far_all():
            attn.far_here()
            attn.far_whole()

        def head(step, qkv_ref, o_ref, lse_ref):
            pl.when(step == 3)(near_all)
            pl.when(step == 11)(far_all)
            slot = lax.rem(step, 2)
            for each in range(1, heads):
                pl.when(step == each - 1)(
                    lambda each=each: weights_in(each, each % 2).start()
                )
            weights_in(0, slot).wait()
            shard, half, lane = step // 4, lax.rem(step // 2, 2), lax.rem(step, 2)
            at = 4 * half + 2 * lane
            shift = [as_column(hold.bias[shard, at + k, :, 0:HD]) for k in range(2)]
            attend_head(hold.rows[slot], hold.n[...], shift, qkv_ref, o_ref, lse_ref)
            hold.o[step] = o_ref[0]

        def bring_out(shard):
            return [
                pltpu.make_async_copy(
                    attn.piece(shard, half, lane).at[pl.ds(3 * HD, HD)],
                    hold.w.at[4 * shard + 2 * half + lane],
                    wsem.at[4 * shard + 2 * half + lane],
                )
                for half in range(2)
                for lane in range(2)
            ]

        weights_in(0, 0).start()
        phase(
            heads,
            head,
            [],
            [],
            [ref(qkv), ref(mixed), ref(lse)],
            [
                spec((1, 3, HD, length), lambda i: (i, 0, 0, 0)),
                spec((1, HD, length), lambda i: (i, 0, 0)),
                spec((1, 1, length), lambda i: (i, 0, 0)),
            ],
        )
        for shard in range(4):
            for each in bring_out(shard):
                each.start()
        fc1.forward()
        for each in copies[3:]:
            each.wait()
        for shard in range(4):
            for each in bring_out(shard):
                each.wait()
        stream.begin(fc1, 0)
        store_w = fetch(hold.w, ref(out_all), sem.at[4])
        weight = hold.w[...].reshape(width, width)
        for block in columns_of(length, 256):
            mix = hold.o[:, :, block].reshape(width, -1)
            values = hold.x[:, block].astype(F32) + contract_rows(weight, mix)
            values = values + hold.v[:, 2:3]
            average = jnp.mean(values, axis=0, keepdims=True)
            centered = values - average
            inverse = lax.rsqrt(jnp.mean(centered * centered, axis=0, keepdims=True) + EPS)
            hold.h[block.start // 256, :, 0 : block.stop - block.start] = values
            hold.n2[:, block] = (
                centered * inverse * hold.v[:, 3:4] + hold.v[:, 4:5]
            ).astype(BF)
            hold.s[0:1, block] = average
            hold.s[1:2, block] = inverse
        stores = [store_w] + [
            fetch(source, ref(target), sem.at[k])
            for k, (source, target) in enumerate(((hold.h, residual), (hold.n2, normed), (hold.s, stats)))
        ]

        def hidden(step, act_ref, slope_ref):
            weight = stream.bring(fc1, step, 0, 8)
            shard, half = step // 2, lax.rem(step, 2)
            shift = as_column(hold.bias[shard, half, :, 128 : 128 + rows])
            preact = dot_nn(weight, hold.n2[...]) + shift
            square = preact * preact
            curve = jnp.tanh(preact * (GELU_A + (GELU_A * GELU_B) * square))
            rise = 0.5 * (1.0 + curve)
            act_ref[0] = (preact * rise).astype(BF)
            inner = GELU_A + (3.0 * GELU_A * GELU_B) * square
            slope_ref[0] = (rise + (0.5 * preact) * (1.0 - curve * curve) * inner).astype(BF)

        block = spec((1, rows, length), lambda i: (i, 0, 0))

        def fc1_near():
            fc1.near_here()
            fc1.near_whole()

        def fc1_far():
            fc1.far_here()
            fc1.far_whole()

        phase(
            8, hidden, [], [], [ref(act), ref(slope)], [block, block],
            [(1, fc1_near), (5, fc1_far)],
        )
        for each in stores:
            each.wait()
        attn.drain()
        fc1.drain()

    result = p.call(script, 2, 3e10)
    return (
        gathered(attn).each(result),
        gathered(fc1).each(result),
        Bag(
            qkv=qkv,
            mixed=mixed,
            lse=lse,
            residual=residual,
            normed_two=normed,
            stats_two=stats,
            out_all=out_all,
            act=act,
            slope=slope,
        ).each(result),
    )


def gathered(source):
    return Bag(
        near=source.near, near_part=source.near_part, far=source.far, far_part=source.far_part
    )


class Ready:
    def __init__(self, program, own, parts, early=None):
        self.handles = parts.each(program.input)
        self.handles.own = program.input(own)
        self.handles.early = None if early is None else program.input(early)
        self.early = early

    def bind(self, ref):
        self.refs = self.handles.each(lambda h: None if h is None else ref(h))
        return self

    piece = Gather.piece


def backward(arrays, fc1_parts, attn_parts, owns, early, live):
    width, length = arrays.picture.shape
    share = width // 4
    unit = owns.fc2.shape[2]
    rows = 2 * unit
    block = 3 * HD
    p = Program("backward", (X, Y, XY, CORE, LINE))
    into = arrays.each(p.input)
    live_in = p.input(live, pl.BlockSpec(memory_space=pltpu.SMEM))
    fc1 = Ready(p, owns.fc1, fc1_parts)
    attn = Ready(p, owns.attn, attn_parts, early)
    fc2 = Gather(p, p.input(owns.fc2), owns.fc2.shape)
    stream = Stream(p, 2, unit, width)

    fc_shape, out_shape, qkv_shape = ((4, 2, u, width) for u in (unit, HD, block))
    shapes = (fc_shape, fc_shape, out_shape, qkv_shape)
    plane = [Plane(p, shape) for shape in shapes[:QKV]]
    plane.append(Plane(p, shapes[QKV], plane[FC2]))
    line = [Line(p, shape[1:]) for shape in shapes[:QKV]]
    line.append(Line(p, shapes[QKV][1:], line[FC2]))
    d_pre = p.output(8, rows, length)
    pull = p.output(16, HD, length)
    d_qkv = p.output(16, 3, HD, length)
    block_rows, input_rows = p.output(4, share, length), p.output(4, share, length)
    spread_block = Spread(p, block_rows, (4, share, length))
    spread_input = Spread(p, input_rows, (4, share, length))
    vectors = Vectors(p, (16, 1, width))
    held = Bag(
        upstream=p.tile(width, length),
        normed_two=p.tile(width, length),
        normed_one=p.tile(width, length),
        low=p.tile(width, length),
        residual=p.tile(width, 256, dtype=F32),
        acc=p.tile(width, length, dtype=F32),
        vectors=p.tile(*arrays.vectors.shape, dtype=F32),
        stats_two=p.tile(2, length, dtype=F32),
        stats_one=p.tile(2, length, dtype=F32),
        rows=p.tile(2, rows, length),
        heads=p.tile(3, 2, 3, HD, length),
        part=p.tile(2, 2, unit, width),
    )
    tile_sems = p.sems(2)
    sems = p.sems(12)

    def script(ref):
        hold = held.each(ref)
        sem = ref(sems)
        for each in (fc1, attn, fc2, stream, spread_block, spread_input, vectors):
            each.bind(ref)
        for group in (plane, line):
            for each in group:
                each.bind(ref)
        vec = vectors.refs.held
        array = into.each(ref)
        live_now = ref(live_in)[0].astype(F32)

        copies = Bag(
            upstream=fetch(array.upstream, hold.upstream, sem.at[0]),
            normed_two=fetch(array.normed_two, hold.normed_two, sem.at[1]),
            vectors=fetch(array.vectors, hold.vectors, sem.at[3]),
            stats_two=fetch(array.stats_two, hold.stats_two, sem.at[4]),
            normed_one=fetch(array.normed_one, hold.normed_one, sem.at[5]),
            stats_one=fetch(array.stats_one, hold.stats_one, sem.at[6]),
        )
        fc2.start()
        stream.begin(fc2, 0)
        vec[...] = jnp.zeros(vec.shape, F32)
        copies.upstream.wait()
        copies.normed_two.wait()

        tile_sem = ref(tile_sems)

        def rows_in(source, index, slot):
            if len(source.shape) == 3 and source.shape[0] == 8:
                target = hold.rows.at[slot]
                source = source.at[index]
            else:
                target = hold.heads.at[slot, :, 0]
                source = source.at[pl.ds(2 * index, 2)]
            return pltpu.make_async_copy(source, target, tile_sem.at[slot])

        def rows_of(source, slot, count):
            if len(source.shape) == 3 and source.shape[0] == 8:
                return hold.rows[slot]
            return hold.heads[slot, :, 0].reshape(count, length)

        def gradient(source, other, name, shards, go=True):
            _, _, size, _ = shapes[name]
            count = 2 * size
            total = len(shards)

            def pick(i):
                if total == 1:
                    return shards[0]
                if total == 2:
                    return jnp.where(i == 0, shards[0], shards[1])
                return jnp.where(
                    i < 2,
                    jnp.where(i == 0, shards[0], shards[1]),
                    jnp.where(i == 2, shards[2], shards[3]),
                )

            part_of = lambda slot, lane: hold.part.at[slot, lane, pl.ds(0, size)]
            sums_of = plane[name]
            piece = lambda k: jnp.where(
                k < total, 2 * pick(k) + 1, 2 * pick(jnp.maximum(k - total, 0))
            )
            rows_in(source, 2 * shards[0] + 1, 0).start()

            def product(k):
                slot = lax.rem(k, 2)

                @pl.when(k + 1 < 2 * total)
                def _():
                    rows_in(source, piece(k + 1), 1 - slot).start()

                rows_in(source, 0, slot).wait()
                return contract_cols(rows_of(source, slot, count), other[...])

            def give(i, _):
                slot = lax.rem(i, 2)
                shard = pick(i)

                @pl.when(i >= 2)
                def _():
                    for lane in range(2):
                        before = pick(jnp.maximum(i - 2, 0))
                        sums_of.swap(part_of(slot, lane), before, lane).wait_send()

                sums = product(i).astype(BF).reshape(2, size, width)
                for lane in range(2):
                    part_of(slot, lane)[...] = sums[lane]
                for lane in range(2):
                    sums_of.swap(part_of(slot, lane), shard, lane).start()
                return 0

            def keep(i, _):
                shard = pick(i)
                for lane in range(2):
                    sums_of.swap(part_of(0, lane), shard, lane).wait_recv()
                sums_of.add(shard, product(total + i).reshape(2, size, width), go)
                return 0

            lax.fori_loop(0, total, give, 0)
            lax.fori_loop(0, total, keep, 0)
            for i in range(max(total - 2, 0), total):
                for lane in range(2):
                    sums_of.swap(
                        part_of(i % 2, lane), jnp.int32(shards[i]), lane
                    ).wait_send()

        every = (3, 1, 2, 0)
        gradient(array.act, hold.upstream, FC2, every, False)

        def hidden(step, slope_ref, d_ref):
            slot = lax.rem(step, 2)
            stream.here(fc2, slot)
            pl.when(step == 1)(lambda: stream.begin(fc2, 2))
            for half in range(2):
                weight = stream.refs[0][slot, half].reshape(rows, width)
                values = dot_nn(weight, hold.upstream[...])
                values = (values * slope_ref[half].astype(F32)).astype(BF)
                d_ref[half] = values
                sums = jnp.sum(values.astype(F32), axis=1, keepdims=True)
                vec[8 + 2 * step + half, :, 0:rows] = as_row(sums)

            @pl.when(step == 0)
            def _():
                fc2.near_here()
                fc2.near_whole()
                stream.begin(fc2, 1)

            @pl.when(step == 2)
            def _():
                fc2.far_here()
                fc2.far_whole()
                stream.begin(fc2, 3)

        fc2.forward()
        plane[FC2].launch()
        pair = spec((2, rows, length), lambda i: (i, 0, 0))
        phase(4, hidden, [array.slope], [pair], [ref(d_pre)], [pair])

        def back(weights, values, lead, size, events=()):
            def body(step, d_ref):
                weight = stream.bring(weights, step, 0, 4, size)
                values = d_ref[...].reshape(4 * size, length)
                hold.acc[...] += contract_rows(weight, values)

            hold.acc[...] = jnp.zeros(hold.acc.shape, F32)
            tail = values.shape[1:]
            zeros = (0,) * len(tail)
            phase(4, body, [values], [spec((lead, *tail), lambda i: (i, *zeros))], [], [], events)

        stream.begin(fc1, 0)
        back(fc1, ref(d_pre), 2, unit)
        for each in (copies.vectors, copies.stats_two):
            each.wait()
        total = lambda values: jnp.sum(values, axis=1, keepdims=True)
        residual_of = parts_of(array.residual, hold.residual, sem.at[2])
        for cut in columns_of(length):
            inverse = hold.stats_two[1:2, cut]
            grad = hold.acc[:, cut]
            units = (residual_of(cut) - hold.stats_two[0:1, cut]) * inverse
            up = hold.upstream[:, cut].astype(F32)
            d_residual = up + norm_back(grad, units, inverse, hold.vectors[:, 3:4])
            hold.low[:, cut] = d_residual.astype(BF)
            hold.vectors[:, 10:11] += total(d_residual)
            hold.vectors[:, 11:12] += total(grad * units)
            hold.vectors[:, 12:13] += total(grad)
            hold.vectors[:, 13:14] += total(up)

        plane[FC2].forward()
        plane[FC2].settle()
        picture_copy = fetch(array.picture, hold.upstream, sem.at[7])

        def pull_body(step, w_ref, o_ref):
            weight = w_ref[...].reshape(4 * HD, width)
            o_ref[...] = dot_nn(weight, hold.low[...]).reshape(4, HD, length).astype(BF)

        quarter = lambda *tail: spec((4, *tail), lambda i: (i, *(0 for _ in tail)))
        phase(
            4, pull_body, [array.out_all], [quarter(HD, width)], [ref(pull)], [quarter(HD, length)]
        )
        gradient(ref(d_pre), hold.normed_two, FC1, every)
        plane[FC2].finish(line[FC2])
        plane[FC2].drain()
        gradient(array.mixed, hold.low, OUT, every)
        copies.normed_one.wait()

        def settle(name):
            plane[name].forward()
            plane[name].settle()

        events = [
            (1, 0, lambda: line[FC2].meet(0)),
            (2, 0, lambda: line[FC2].meet(1)),
            (2, 0, lambda: line[FC2].leave(0)),
            (1, 2, lambda: settle(FC1)),
            (2, 2, lambda: settle(OUT)),
            (3, 0, lambda: plane[FC1].finish(line[FC1])),
            (3, 0, lambda: line[FC2].leave(1)),
            (3, 1, lambda: line[FC2].collect(0)),
        ]
        part_of = lambda lane: hold.part.at[0, lane, pl.ds(0, block)]
        sums_of = plane[QKV]

        def qkv_rows(slot):
            values = hold.heads[slot].reshape(2 * block, length)
            return contract_cols(values, hold.normed_one[...]).reshape(2, block, width)

        def keep_rows(shard, slot):
            for lane in range(2):
                sums_of.swap(part_of(lane), shard, lane).wait()
            sums_of.add(shard, qkv_rows(slot), True)

        order = lambda g: jnp.where(
            g < 2, jnp.where(g == 0, every[0], every[1]), jnp.where(g == 2, every[2], every[3])
        )

        dk_acc = hold.acc.at[pl.ds(0, length), pl.ds(0, HD)]
        dv_acc = hold.acc.at[pl.ds(0, length), pl.ds(128, HD)]

        def shard_back(g, _):
            shard = order(g)
            at = lambda i: 4 * shard + i

            def body(step, qkv_ref, do_ref, o_ref, lse_ref, d_ref):
                for when, now, event in events:
                    pl.when(jnp.logical_and(g == when, step == now))(event)
                sums = attend_back_head(
                    qkv_ref, do_ref, o_ref, lse_ref, d_ref, dk_acc, dv_acc
                )
                half, lane = step // 2, lax.rem(step, 2)
                hold.heads[jnp.where(half == 1, 0, 1 + lax.rem(g, 2)), lane] = d_ref[0]
                for k in range(2):
                    where = pl.multiple_of(640 + 128 * (2 * lane + k), 128)
                    padded = jnp.concatenate(
                        [as_row(sums[k]), jnp.zeros((1, 128 - HD), F32)], axis=1
                    )
                    vec[8 + 2 * shard + half, :, pl.ds(where, 128)] = padded

            flat = spec((1, HD, length), lambda i: (at(i), 0, 0))
            many = spec((1, 3, HD, length), lambda i: (at(i), 0, 0, 0))
            phase(
                4,
                body,
                [array.qkv, ref(pull), array.mixed, array.lse],
                [many, flat, flat, spec((1, 1, length), lambda i: (at(i), 0, 0))],
                [ref(d_qkv)],
                [many],
            )
            pl.when(g > 0)(lambda: keep_rows(order(g - 1), 1 + lax.rem(g + 1, 2)))
            sums = qkv_rows(0).astype(BF)
            for lane in range(2):
                part_of(lane)[...] = sums[lane]
            for lane in range(2):
                sums_of.swap(part_of(lane), shard, lane).start()
            return 0

        lax.fori_loop(0, 4, shard_back, 0)
        plane[OUT].finish(line[OUT])
        stream.begin(fc2, 0)
        keep_rows(jnp.int32(every[3]), 2)
        plane[QKV].forward()
        line[FC1].meet(0)
        back(
            fc2,
            array.act,
            2,
            unit,
            [
                (1, lambda: line[FC2].collect(1)),
                (2, plane[QKV].settle),
                (3, lambda: line[FC1].meet(1)),
            ],
        )
        line[FC1].leave(0)
        stream.begin(attn, 0, block)
        residual_of = parts_of(array.residual, hold.residual, sem.at[2])
        for cut in columns_of(length):
            values = residual_of(cut) + hold.acc[:, cut] + hold.vectors[:, 5:6]
            hold.normed_two[:, cut] = (values * live_now).astype(BF)
        store_rows(hold.normed_two, ref(block_rows), sem, share)
        for k in range(2):
            line[FC2].done(k)
        plane[QKV].finish(line[QKV])
        spread_block.start()
        line[OUT].meet(0)
        line[OUT].meet(1)
        picture_copy.wait()
        copies.stats_one.wait()
        back(
            attn,
            ref(d_qkv),
            4,
            block,
            [(2, lambda: line[FC1].leave(1)), (3, lambda: line[QKV].meet(0))],
        )
        line[OUT].leave(0)
        line[OUT].leave(1)
        for cut in columns_of(length):
            inverse = hold.stats_one[1:2, cut]
            grad = hold.acc[:, cut]
            units = hold.upstream[:, cut].astype(F32) - hold.stats_one[0:1, cut]
            units = units * inverse
            d_input = hold.low[:, cut].astype(F32) + norm_back(
                grad, units, inverse, hold.vectors[:, 0:1]
            )
            hold.normed_two[:, cut] = d_input.astype(BF)
            hold.vectors[:, 8:9] += total(grad * units)
            hold.vectors[:, 9:10] += total(grad)
        line[QKV].meet(1)
        line[QKV].leave(0)
        wide = hold.vectors[:, 8:16].T
        for k in range(8):
            vec[k] = wide[k : k + 1]
        vectors.plane()
        store_rows(hold.normed_two, ref(input_rows), sem, share)
        spread_input.start()
        line[QKV].leave(1)
        last = vectors.line()
        for each in (line[FC1], line[OUT], line[QKV]):
            for k in range(2):
                each.collect(k)
        last()
        spread_block.finish()
        spread_input.finish()
        for each in line[1:]:
            for k in range(2):
                each.done(k)
        for each in plane[1:]:
            each.drain()
        fc2.drain()

    result = p.call(script, 3, 8e10)
    sums = [(result(each.total), result(each.other)) for each in line]
    spreads = [
        (result(block_rows), result(spread_block.landed)),
        (result(input_rows), result(spread_input.landed)),
    ]
    return sums, spreads, result(vectors.total)[:, 0]


def parts_of(source, held, sem):
    width = held.shape[1]

    def bring(part):
        return fetch(source.at[part], held, sem)

    bring(0).wait()

    def columns(cut):
        if cut.start > 0 and cut.start % width == 0:
            bring(cut.start // width).wait()
        first = cut.start % width
        return held[:, first : first + cut.stop - cut.start]

    return columns


def store_rows(source, target, sem, share):
    copies = [
        fetch(source.at[pl.ds(k * share, share)], target.at[k], sem.at[k]) for k in range(4)
    ]
    for each in copies:
        each.wait()


def finish(sums, spreads, place_t, core, hidden):
    width = sums[FC2][0].shape[-1]
    share, length = spreads[0][0].shape[1:]

    def body(at, *refs):
        step = pl.program_id(0)
        same = lax.rem(step // 2 + at[1], 2) == 0
        ins, outs = refs[:12], refs[12:]
        for k in range(4):
            rows = jnp.where(same, ins[2 * k][0], ins[2 * k + 1][0]).astype(F32)
            outs[k][...] = rows.reshape(outs[k].shape)
        for k in range(2):
            rows = jnp.where(step == at[0], ins[8 + 2 * k][0], ins[9 + 2 * k][0])
            outs[4 + k][0] = rows.astype(F32)

    half = lambda array: pl.BlockSpec((1, *array.shape[1:]), lambda i, at: (lax.rem(i, 2), 0, 0))
    own = pl.BlockSpec((1, share, length), lambda i, at: (at[0], 0, 0))
    landed = pl.BlockSpec(
        (1, share, length), lambda i, at: (jnp.maximum((i ^ at[0]) - 1, 0), 0, 0)
    )
    units = [pair[0].shape[1] for pair in sums]
    rows = lambda unit: pl.BlockSpec((unit, width), lambda i, at: (i, 0))
    slot = pl.BlockSpec((1, share, length), lambda i, at: (i, 0, 0))
    shape = lambda *dims: jax.ShapeDtypeStruct(dims, F32)
    return pl.pallas_call(
        body,
        grid_spec=pltpu.PrefetchScalarGridSpec(
            num_scalar_prefetch=1,
            grid=(4,),
            in_specs=[half(array) for pair in sums for array in pair] + [own, landed] * 2,
            out_specs=[
                rows(units[FC2]),
                rows(units[FC1]),
                rows(units[OUT]),
                pl.BlockSpec((3, HD, width), lambda i, at: (0, i, 0)),
                slot,
                slot,
            ],
        ),
        out_shape=[
            shape(hidden, width),
            shape(hidden, width),
            shape(share, width),
            shape(3, share, width),
            shape(4, share, length),
            shape(4, share, length),
        ],
        compiler_params=pltpu.CompilerParams(vmem_limit_bytes=67_043_328),
        name="finish",
    )(
        jnp.stack([place_t, core]).astype(jnp.int32),
        *[array for pair in sums for array in pair],
        *spreads[0],
        *spreads[1],
    )


def whole_image(
    images,
    counts,
    ln1_gain,
    ln1_bias,
    qkv_weight,
    qv_bias,
    out_weight,
    out_bias,
    ln2_gain,
    ln2_bias,
    fc1_weight,
    fc1_bias,
    fc2_weight,
    fc2_bias,
    grad_out,
):
    slot_count, length, width = images.shape
    share = width // 4
    hidden = fc1_weight.shape[1]
    unit = -(-hidden // 64) * 16
    rows = 2 * unit
    place_t = lax.axis_index(TENSOR)
    core = lax.rem(lax.axis_index(DP), 2)
    block = 3 * HD

    qkv_rows = qkv_weight.reshape(3, width, 2, 2, HD).transpose(2, 3, 0, 4, 1)
    attn_own = jnp.concatenate(
        [qkv_rows.reshape(2, 2, block, width), out_weight.reshape(2, 2, HD, width)], axis=2
    )
    pad = 2 * rows - hidden
    fc1_own, fc2_own = (
        jnp.pad(each, ((0, pad), (0, 0))).reshape(2, 2, unit, width)
        for each in (fc1_weight.T, fc2_weight)
    )
    head_bias = qv_bias.reshape(2, 2, 2, HD).transpose(1, 2, 0, 3)
    head_bias = jnp.pad(turned(head_bias, 0, core).reshape(8, HD), ((0, 0), (0, 128 - HD)))
    hidden_bias = turned(jnp.pad(fc1_bias, (0, pad)).reshape(2, rows), 0, core)
    hidden_bias = jnp.pad(hidden_bias, ((0, 6), (0, 640 - rows)))
    bias = jnp.concatenate([head_bias, hidden_bias], axis=1).astype(F32)[:, None]
    vectors = jnp.stack(
        [ln1_gain, ln1_bias, out_bias, ln2_gain, ln2_bias, fc2_bias, fc2_bias, fc2_bias], axis=1
    )
    vectors = jnp.pad(vectors, ((0, 0), (0, 8))).astype(F32)
    live = (place_t < counts[0]).astype(jnp.int32)[None]

    picture, upstream, normed_one, stats_one, early, bias_far = prepare(
        images,
        grad_out,
        place_t[None].astype(jnp.int32),
        live,
        ln1_gain.astype(F32)[None],
        ln1_bias.astype(F32)[None],
        attn_own,
        bias,
    )
    attn_parts, fc1_parts, made = forward(
        attn_own, early, fc1_own, bias, bias_far, picture, normed_one, vectors
    )
    made.__dict__.update(
        upstream=upstream,
        picture=picture,
        normed_one=normed_one,
        stats_one=stats_one,
        vectors=vectors,
    )
    owns = Bag(attn=attn_own, fc1=fc1_own, fc2=fc2_own)
    sums, spreads, totals = backward(made, fc1_parts, attn_parts, owns, early, live)

    own_wide = lax.dynamic_slice_in_dim(totals[:6], place_t * share, share, 1)
    own_rows = turned(totals[8:10], 0, core)
    own_hidden = own_rows[:, :rows].reshape(-1)[:hidden]
    own_qv = own_rows[:, 640:].reshape(2, 2, 2, 128)[..., :HD].transpose(2, 0, 1, 3)
    own_qv = own_qv.reshape(2, share)

    fc2_result, fc1_result, out_result, qkv_result, block_result, input_result = finish(
        sums, spreads, place_t, core, hidden
    )
    return (
        block_result.transpose(0, 2, 1),
        input_result.transpose(0, 2, 1),
        own_wide[0],
        own_wide[1],
        qkv_result.transpose(0, 2, 1),
        own_qv,
        out_result,
        own_wide[2],
        own_wide[3],
        own_wide[4],
        fc1_result.T,
        own_hidden,
        fc2_result,
        own_wide[5],
    )


def solution(mesh):
    whole_fits = mesh.shape[TENSOR] == 4 and mesh.shape[DP] == 8
    return jax.shard_map(
        whole_image if whole_fits else local,
        mesh=mesh,
        in_specs=(
            P(DP, None, None),
            P(DP),
            P(),
            P(),
            P(None, None, TENSOR),
            P(None, TENSOR),
            P(TENSOR, None),
            P(),
            P(),
            P(),
            P(None, TENSOR),
            P(TENSOR),
            P(TENSOR, None),
            P(),
            P(DP, None, None),
        ),
        out_specs=(
            P(DP, None, TENSOR),
            P(DP, None, TENSOR),
            P(TENSOR),
            P(TENSOR),
            P(None, None, TENSOR),
            P(None, TENSOR),
            P(TENSOR, None),
            P(TENSOR),
            P(TENSOR),
            P(TENSOR),
            P(None, TENSOR),
            P(TENSOR),
            P(TENSOR, None),
            P(TENSOR),
        ),
        check_vma=False,
    )
```

```python
import math

import jax
import jax.numpy as jnp
from jax import lax
from jax.experimental import pallas as pl
from jax.experimental.pallas import tpu as pltpu
from jax.sharding import PartitionSpec as P

HD = 72


EPS = 1e-06


def own_columns(values, share_width):
    start = lax.axis_index(TENSOR) * share_width
    return lax.dynamic_slice_in_dim(values, start, share_width, values.ndim - 1)


def row_mean(values):
    return jnp.mean(values, axis=-1, keepdims=True)


def group_stats(first, second):
    return lax.psum((first, second), TENSOR)


def contract_rows(left, right):
    return lax.dot_general(
        left, right, (((0,), (0,)), ((), ())), preferred_element_type=jnp.float32
    )


def contract_cols(left, right):
    return lax.dot_general(
        left, right, (((1,), (1,)), ((), ())), preferred_element_type=jnp.float32
    )


def gelu_tanh(values):
    return jax.nn.gelu(values, approximate=True)


def local(
    images,
    counts,
    ln1_gain,
    ln1_bias,
    qkv_weight,
    qv_bias,
    out_weight,
    out_bias,
    ln2_gain,
    ln2_bias,
    fc1_weight,
    fc1_bias,
    fc2_weight,
    fc2_bias,
    grad_out,
):
    slot_count, length, full_width = images.shape
    share_width = full_width // lax.axis_size(TENSOR)
    local_width = qkv_weight.shape[2]
    local_heads = local_width // HD
    hidden_width = fc1_weight.shape[1]
    score_scale = 1.0 / math.sqrt(HD)
    gain_one = ln1_gain.astype(jnp.float32)
    shift_one = ln1_bias.astype(jnp.float32)
    gain_two = ln2_gain.astype(jnp.float32)
    shift_two = ln2_bias.astype(jnp.float32)
    bias_out = out_bias.astype(jnp.float32)
    bias_fc1 = fc1_bias.astype(jnp.float32)
    bias_fc2 = fc2_bias.astype(jnp.float32)
    bias_query = qv_bias[0].astype(jnp.float32)
    bias_value = qv_bias[1].astype(jnp.float32)
    live_count = counts[0]

    def to_heads(values):
        return values.reshape(length, local_heads, HD)

    def head_scores(query_heads, key_heads):
        return (
            jnp.einsum("qhd,khd->hqk", query_heads, key_heads, preferred_element_type=jnp.float32)
            * score_scale
        )

    def layer_step(slot_index, loop_state):
        block_acc, input_acc, grads = loop_state
        (
            grad_gain_one,
            grad_shift_one,
            grad_qkv,
            grad_qv,
            grad_out_w,
            grad_out_b,
            grad_gain_two,
            grad_shift_two,
            grad_fc1_w,
            grad_fc1_b,
            grad_fc2_w,
            grad_fc2_b,
        ) = grads
        live_flag = (slot_index < live_count).astype(jnp.float32)
        picture = lax.dynamic_index_in_dim(images, slot_index, 0, keepdims=False).astype(
            jnp.float32
        )
        upstream = (
            lax.dynamic_index_in_dim(grad_out, slot_index, 0, keepdims=False).astype(jnp.float32)
            * live_flag
        )
        upstream_low = upstream.astype(jnp.bfloat16)
        centered = picture - row_mean(picture)
        inv_one = lax.rsqrt(row_mean(centered * centered) + EPS)
        unit_one = centered * inv_one
        normed_one = (unit_one * gain_one + shift_one).astype(jnp.bfloat16)
        query_rows = (
            jnp.dot(normed_one, qkv_weight[0], preferred_element_type=jnp.float32) + bias_query
        ).astype(jnp.bfloat16)
        key_rows = jnp.dot(normed_one, qkv_weight[1], preferred_element_type=jnp.float32).astype(
            jnp.bfloat16
        )
        value_rows = (
            jnp.dot(normed_one, qkv_weight[2], preferred_element_type=jnp.float32) + bias_value
        ).astype(jnp.bfloat16)
        query_heads = to_heads(query_rows)
        key_heads = to_heads(key_rows)
        value_heads = to_heads(value_rows)
        scores = head_scores(query_heads, key_heads)
        row_top = jnp.max(scores, axis=-1, keepdims=True)
        logsum = row_top + jnp.log(jnp.sum(jnp.exp(scores - row_top), axis=-1, keepdims=True))
        probs_low = jnp.exp(scores - logsum).astype(jnp.bfloat16)
        mixed = jnp.einsum(
            "hqk,khd->qhd", probs_low, value_heads, preferred_element_type=jnp.float32
        )
        mixed = mixed.reshape(length, local_width).astype(jnp.bfloat16)
        partial_out = jnp.dot(mixed, out_weight, preferred_element_type=jnp.float32).astype(
            jnp.bfloat16
        )
        residual = (
            own_columns(picture, share_width)
            + lax.psum_scatter(partial_out, TENSOR, scatter_dimension=1, tiled=True).astype(
                jnp.float32
            )
            + own_columns(bias_out, share_width)
        )
        row_sum, row_square = group_stats(
            jnp.sum(residual, axis=-1), jnp.sum(residual * residual, axis=-1)
        )
        average = row_sum[:, None] / full_width
        inv_two = lax.rsqrt(row_square[:, None] / full_width - average * average + EPS)
        unit_two = (residual - average) * inv_two
        own_normed = (
            unit_two * own_columns(gain_two, share_width) + own_columns(shift_two, share_width)
        ).astype(jnp.bfloat16)
        normed_two = lax.all_gather(own_normed, TENSOR, axis=1, tiled=True)
        preact = jnp.dot(normed_two, fc1_weight, preferred_element_type=jnp.float32) + bias_fc1
        activated = gelu_tanh(preact).astype(jnp.bfloat16)
        partial_mlp = jnp.dot(activated, fc2_weight, preferred_element_type=jnp.float32).astype(
            jnp.bfloat16
        )
        block_rows = (
            residual
            + lax.psum_scatter(partial_mlp, TENSOR, scatter_dimension=1, tiled=True).astype(
                jnp.float32
            )
            + own_columns(bias_fc2, share_width)
        )
        block_rows = block_rows * live_flag
        grad_fc2_b = grad_fc2_b + own_columns(jnp.sum(upstream, axis=0), share_width)
        grad_fc2_w = grad_fc2_w + contract_rows(activated, upstream_low)
        d_act = contract_cols(upstream_low, fc2_weight)
        gelu_pull = jax.vjp(gelu_tanh, preact)[1]
        d_pre = gelu_pull(d_act)[0].astype(jnp.bfloat16)
        grad_fc1_b = grad_fc1_b + jnp.sum(d_pre.astype(jnp.float32), axis=0)
        grad_fc1_w = grad_fc1_w + contract_rows(normed_two, d_pre)
        back_mlp = contract_cols(d_pre, fc1_weight)
        d_norm_two = lax.psum_scatter(
            back_mlp.astype(jnp.bfloat16), TENSOR, scatter_dimension=1, tiled=True
        ).astype(jnp.float32)
        scaled_two = d_norm_two * own_columns(gain_two, share_width)
        sum_plain, sum_cross = group_stats(
            jnp.sum(scaled_two, axis=-1), jnp.sum(scaled_two * unit_two, axis=-1)
        )
        d_residual = own_columns(upstream, share_width) + inv_two * (
            scaled_two
            - sum_plain[:, None] / full_width
            - unit_two * (sum_cross[:, None] / full_width)
        )
        grad_gain_two = grad_gain_two + jnp.sum(d_norm_two * unit_two, axis=0)
        grad_shift_two = grad_shift_two + jnp.sum(d_norm_two, axis=0)
        grad_out_b = grad_out_b + jnp.sum(d_residual, axis=0)
        d_residual_low = lax.all_gather(
            d_residual.astype(jnp.bfloat16), TENSOR, axis=1, tiled=True
        )
        grad_out_w = grad_out_w + contract_rows(mixed, d_residual_low)
        d_mixed_heads = to_heads(contract_cols(d_residual_low, out_weight).astype(jnp.bfloat16))
        probs = jnp.exp(head_scores(query_heads, key_heads) - logsum)
        probs_again = probs.astype(jnp.bfloat16)
        d_value = jnp.einsum(
            "hqk,qhd->khd", probs_again, d_mixed_heads, preferred_element_type=jnp.float32
        )
        d_probs = jnp.einsum(
            "qhd,khd->hqk", d_mixed_heads, value_heads, preferred_element_type=jnp.float32
        )
        inner = jnp.sum(probs * d_probs, axis=-1, keepdims=True)
        d_scores = (probs * (d_probs - inner)).astype(jnp.bfloat16)
        d_query = (
            jnp.einsum("hqk,khd->qhd", d_scores, key_heads, preferred_element_type=jnp.float32)
            * score_scale
        )
        d_key = (
            jnp.einsum("hqk,qhd->khd", d_scores, query_heads, preferred_element_type=jnp.float32)
            * score_scale
        )
        d_stack = (
            jnp.stack([d_query, d_key, d_value], axis=1)
            .reshape(length, 3, local_width)
            .astype(jnp.bfloat16)
        )
        grad_qkv = grad_qkv + jnp.einsum(
            "ld,lje->jde", normed_one, d_stack, preferred_element_type=jnp.float32
        )
        bias_sums = jnp.sum(d_stack.astype(jnp.float32), axis=0)
        grad_qv = grad_qv + jnp.stack([bias_sums[0], bias_sums[2]])
        back_attn = jnp.einsum(
            "lje,jde->ld", d_stack, qkv_weight, preferred_element_type=jnp.float32
        )
        d_norm_one = lax.psum_scatter(
            back_attn.astype(jnp.bfloat16), TENSOR, scatter_dimension=1, tiled=True
        ).astype(jnp.float32)
        own_unit = own_columns(unit_one, share_width)
        scaled_one = d_norm_one * own_columns(gain_one, share_width)
        plain_one, cross_one = group_stats(
            jnp.sum(scaled_one, axis=-1), jnp.sum(scaled_one * own_unit, axis=-1)
        )
        d_input = d_residual + inv_one * (
            scaled_one
            - plain_one[:, None] / full_width
            - own_unit * (cross_one[:, None] / full_width)
        )
        grad_gain_one = grad_gain_one + jnp.sum(d_norm_one * own_unit, axis=0)
        grad_shift_one = grad_shift_one + jnp.sum(d_norm_one, axis=0)
        block_acc = lax.dynamic_update_index_in_dim(block_acc, block_rows, slot_index, 0)
        input_acc = lax.dynamic_update_index_in_dim(input_acc, d_input, slot_index, 0)
        new_grads = (
            grad_gain_one,
            grad_shift_one,
            grad_qkv,
            grad_qv,
            grad_out_w,
            grad_out_b,
            grad_gain_two,
            grad_shift_two,
            grad_fc1_w,
            grad_fc1_b,
            grad_fc2_w,
            grad_fc2_b,
        )
        return (block_acc, input_acc, new_grads)

    share_zeros = jnp.zeros((share_width,), jnp.float32)
    start_grads = (
        share_zeros,
        share_zeros,
        jnp.zeros((3, full_width, local_width), jnp.float32),
        jnp.zeros((2, local_width), jnp.float32),
        jnp.zeros((local_width, full_width), jnp.float32),
        share_zeros,
        share_zeros,
        share_zeros,
        jnp.zeros((full_width, hidden_width), jnp.float32),
        jnp.zeros((hidden_width,), jnp.float32),
        jnp.zeros((hidden_width, full_width), jnp.float32),
        share_zeros,
    )
    start_rows = jnp.zeros((slot_count, length, share_width), jnp.float32)
    block_acc, input_acc, grads = lax.fori_loop(
        0, slot_count, layer_step, (start_rows, start_rows, start_grads)
    )
    (
        grad_gain_one,
        grad_shift_one,
        grad_qkv,
        grad_qv,
        grad_out_w,
        grad_out_b,
        grad_gain_two,
        grad_shift_two,
        grad_fc1_w,
        grad_fc1_b,
        grad_fc2_w,
        grad_fc2_b,
    ) = grads
    summed = (
        lax.psum(grad_gain_one.astype(jnp.bfloat16), DP).astype(jnp.float32),
        lax.psum(grad_shift_one.astype(jnp.bfloat16), DP).astype(jnp.float32),
        lax.psum(grad_qkv.astype(jnp.bfloat16), DP).astype(jnp.float32),
        lax.psum(grad_qv.astype(jnp.bfloat16), DP).astype(jnp.float32),
        lax.psum(grad_out_w.astype(jnp.bfloat16), DP).astype(jnp.float32),
        lax.psum(grad_out_b.astype(jnp.bfloat16), DP).astype(jnp.float32),
        lax.psum(grad_gain_two.astype(jnp.bfloat16), DP).astype(jnp.float32),
        lax.psum(grad_shift_two.astype(jnp.bfloat16), DP).astype(jnp.float32),
        lax.psum(grad_fc1_w.astype(jnp.bfloat16), DP).astype(jnp.float32),
        lax.psum(grad_fc1_b.astype(jnp.bfloat16), DP).astype(jnp.float32),
        lax.psum(grad_fc2_w.astype(jnp.bfloat16), DP).astype(jnp.float32),
        lax.psum(grad_fc2_b.astype(jnp.bfloat16), DP).astype(jnp.float32),
    )
    return (
        block_acc,
        input_acc,
        summed[0],
        summed[1],
        summed[2],
        summed[3],
        summed[4],
        summed[5],
        summed[6],
        summed[7],
        summed[8],
        summed[9],
        summed[10],
        summed[11],
    )


LOG2E = math.log2(math.e)
LN2 = math.log(2.0)
GELU_A = math.sqrt(2.0 / math.pi)
GELU_B = 0.044715
BF = jnp.bfloat16
F32 = jnp.float32
QUERY_BLOCK = 256
MESH = pl.DeviceIdType.MESH
TENSOR, DP = "tensor", "dp"
X, Y, XY, CORE, LINE = range(5)
TURN = {X: 1, Y: 2, XY: 3}
OTHER = {X: Y, Y: X}
SIDE = {X: 0, Y: 1}
LANES = (X, Y)
FC2, FC1, OUT, QKV = range(4)
INWARD, ACROSS, BACK, SWAP = range(4)


class Bag:
    def __init__(self, **things):
        self.__dict__.update(things)

    def each(self, action):
        return Bag(**{name: action(thing) for name, thing in self.__dict__.items()})
ANYWHERE = pl.BlockSpec(memory_space=pl.ANY)


def dot_nn(left, right):
    return lax.dot_general(left, right, (((1,), (0,)), ((), ())), preferred_element_type=F32)


def place(bit):
    if bit == CORE:
        return {DP: lax.axis_index(DP) ^ 1}
    return {TENSOR: lax.axis_index(TENSOR) ^ TURN[bit]}


def hop(source, target, sems, index, to):
    return pltpu.make_async_remote_copy(
        src_ref=source,
        dst_ref=target,
        send_sem=sems.at[0, index],
        recv_sem=sems.at[1, index],
        device_id=place(to) if isinstance(to, int) else to,
        device_id_type=MESH,
    )


def line_place():
    dp = lax.axis_index(DP)
    return dp // 2, {DP: lax.rem(dp + 2, 8)}, {DP: lax.rem(dp + 6, 8)}


class Program:
    def __init__(self, name, partners):
        self.name = name
        self.partners = partners
        self.arrays, self.specs, self.shapes, self.scratches = [], [], [], []

    def input(self, array, spec=ANYWHERE):
        self.arrays.append(array)
        self.specs.append(spec)
        return (0, len(self.arrays) - 1)

    def output(self, *shape, dtype=BF):
        self.shapes.append(jax.ShapeDtypeStruct(shape, dtype))
        return (1, len(self.shapes) - 1)

    def scratch(self, spec):
        self.scratches.append(spec)
        return (2, len(self.scratches) - 1)

    def tile(self, *shape, dtype=BF):
        return self.scratch(pltpu.VMEM(shape, dtype))

    def sems(self, *shape):
        return self.scratch(pltpu.SemaphoreType.DMA(shape))

    def call(self, script, collective_id, cost):
        count_in, count_out = len(self.arrays), len(self.shapes)

        def kernel(*refs):
            pools = (
                refs[:count_in],
                refs[count_in : count_in + count_out],
                refs[count_in + count_out :],
            )
            meet(self.partners)
            script(lambda handle: pools[handle[0]][handle[1]])

        results = pl.pallas_call(
            kernel,
            in_specs=self.specs,
            out_specs=[ANYWHERE] * count_out,
            out_shape=self.shapes,
            scratch_shapes=self.scratches,
            compiler_params=pltpu.CompilerParams(
                vmem_limit_bytes=67_043_328, collective_id=collective_id, has_side_effects=True
            ),
            cost_estimate=pl.CostEstimate(
                flops=int(cost), bytes_accessed=1 << 26, transcendentals=0
            ),
            name=self.name,
        )(*self.arrays)
        return lambda handle: results[handle[1]]


def meet(partners):
    barrier = pltpu.get_barrier_semaphore()
    signal = lambda at: pl.semaphore_signal(barrier, inc=1, device_id=at, device_id_type=MESH)
    for bit in partners:
        if bit == XY:
            signal({TENSOR: lax.axis_index(TENSOR) ^ 3})
        elif bit != LINE:
            signal(place(bit))
    singles = len([bit for bit in partners if bit != LINE])
    if LINE in partners:
        z, up, down = line_place()
        pl.when(z < 3)(lambda: signal(up))
        pl.when(z > 0)(lambda: signal(down))
        inner = jnp.logical_and(z > 0, z < 3)
        pl.when(inner)(lambda: pl.semaphore_wait(barrier, singles + 2))
        pl.when(jnp.logical_not(inner))(lambda: pl.semaphore_wait(barrier, singles + 1))
    else:
        pl.semaphore_wait(barrier, singles)


def phase(steps, body, ins, in_specs, outs, out_specs, events=()):
    def inner(at, *refs):
        step = at.index[0]
        for when, event in events:
            pl.when(step == when)(event)
        body(step, *refs)

    pltpu.emit_pipeline(
        inner, grid=(steps,), in_specs=in_specs, out_specs=out_specs, _explicit_indices=True
    )(*ins, *outs)


def fetch(source, target, sem):
    copy = pltpu.make_async_copy(source, target, sem)
    copy.start()
    return copy


def spec(shape, index):
    return pl.BlockSpec(shape, index)


class Gather:
    def __init__(self, program, own, shape, early=None):
        _, count, unit, width = shape
        self.own = own
        self.early = early
        self.near = program.output(2, count, unit, width)
        self.near_part = program.output(2, count, unit, width)
        self.far = program.output(count, unit, width)
        self.far_part = program.output(count, unit, width)
        self.sems = program.sems(2, 12)

    def bind(self, ref):
        self.refs = Bag(
            own=ref(self.own),
            near=ref(self.near),
            near_part=ref(self.near_part),
            far=ref(self.far),
            far_part=ref(self.far_part),
            sems=ref(self.sems),
            early=None if self.early is None else ref(self.early),
        )
        return self

    def piece(self, shard, part, lane):
        r = self.refs
        if shard == 0:
            return r.own.at[lax.rem(lax.axis_index(DP) + part, 2), lane]
        if shard == 3:
            return (r.far_part if part else r.far).at[lane]
        if self.early is not None and part == 0 and LANES[lane] == LANES[shard - 1]:
            return r.early.at[lane]
        return (r.near_part if part else r.near).at[shard - 1, lane]

    def _near(self, bit, lane):
        r = self.refs
        k = SIDE[bit]
        own = self.piece(0, 0, lane)
        return hop(own, r.near.at[k, lane], r.sems, 2 * lane + k, bit)

    def _far(self, lane):
        first = LANES[lane]
        source = self.piece(1 + SIDE[first], 0, lane)
        return hop(source, self.refs.far.at[lane], self.refs.sems, 4 + lane, OTHER[first])

    def _swap(self, shard, lane):
        target = self.piece(shard, 1, lane)
        index = 6 + 2 * (shard - 1) + lane
        return hop(self.piece(shard, 0, lane), target, self.refs.sems, index, CORE)

    def start(self):
        for first in (True, False):
            for lane, bit in enumerate(LANES):
                if first and self.early is None:
                    self._near(bit, lane).start()
                if not first:
                    self._near(OTHER[bit], lane).start()

    def forward(self):
        for lane, first in enumerate(LANES):
            if self.early is None:
                self._near(first, lane).wait_recv()
            self._far(lane).start()
            self._swap(1 + SIDE[first], lane).start()

    def near_here(self):
        for lane, first in enumerate(LANES):
            self._near(OTHER[first], lane).wait_recv()
            self._swap(1 + SIDE[OTHER[first]], lane).start()

    def near_whole(self):
        for lane in range(2):
            for shard in (1, 2):
                self._swap(shard, lane).wait_recv()

    def far_here(self):
        for lane in range(2):
            self._far(lane).wait_recv()
            self._swap(3, lane).start()

    def far_whole(self):
        for lane in range(2):
            self._swap(3, lane).wait_recv()

    def drain(self):
        for lane, first in enumerate(LANES):
            if self.early is None:
                self._near(first, lane).wait_send()
            self._near(OTHER[first], lane).wait_send()
            self._far(lane).wait_send()
            for shard in (1, 2, 3):
                self._swap(shard, lane).wait_send()


class Plane:
    def __init__(self, program, shape, share=None):
        _, count, unit, width = shape
        self.unit = unit
        if share is None:
            self.both = program.tile(2, count, 2, unit, width)
            self.got = program.tile(count, 2, unit, width)
            self.last = program.tile(count, unit, width)
        else:
            self.both, self.got, self.last = share.both, share.got, share.last
        self.sems = program.sems(2, 6)
        self.swap_sems = program.sems(2, 8)

    def bind(self, ref):
        self.refs = [ref(h) for h in (self.both, self.got, self.last, self.sems)]
        self.swaps = ref(self.swap_sems)
        return self

    def _part(self, which, *at):
        return self.refs[which].at[*at, pl.ds(0, self.unit)]

    @staticmethod
    def entry(shard, lane):
        odd, high = lax.rem(shard, 2), shard // 2
        return (odd, high) if LANES[lane] == X else (high, odd)

    def tile(self, shard, lane):
        gone, k = self.entry(shard, lane)
        return self._part(0, gone, lane, k)

    def swap(self, source, shard, lane):
        return hop(source, self.tile(shard, lane), self.swaps, 2 * shard + lane, CORE)

    def _first(self, lane, k):
        source = self._part(0, 1, lane, k)
        return hop(source, self._part(1, lane, k), self.refs[3], 2 * lane + k, LANES[lane])

    def _next(self, lane):
        source = self._part(0, 0, lane, 1)
        return hop(
            source, self._part(2, lane), self.refs[3], 4 + lane, OTHER[LANES[lane]]
        )

    def add(self, shard, sums, go):
        for lane in range(2):
            tile = self.tile(shard, lane)
            tile[...] = (sums[lane] + tile[...].astype(F32)).astype(BF)
        if go:
            for lane in range(2):
                gone, k = self.entry(shard, lane)
                pl.when(gone == 1)(lambda lane=lane, k=k: self._first(lane, k).start())

    def launch(self):
        for k in (1, 0):
            for lane in range(2):
                self._first(lane, k).start()

    def _add(self, lane, k):
        self._first(lane, k).wait_recv()
        base = self._part(0, 0, lane, k)
        base[...] = base[...] + self._part(1, lane, k)[...]

    def forward(self):
        for lane in (1, 0):
            self._add(lane, 1)
            self._next(lane).start()

    def settle(self):
        for lane in range(2):
            self._add(lane, 0)

    def finish(self, line):
        for lane in range(2):
            self._next(lane).wait_recv()
            line.take(lane, self._part(0, 0, lane, 0)[...] + self._part(2, lane)[...])

    def drain(self):
        for lane in range(2):
            self._next(lane).wait_send()
            for k in range(2):
                self._first(lane, k).wait_send()


class Line:
    def __init__(self, program, shape, share=None):
        count, unit, width = shape
        self.unit = unit
        self.total = program.output(*shape)
        self.other = program.output(*shape)
        if share is None:
            self.held = program.tile(*shape)
            self.outer = program.tile(*shape)
            self.middle = program.tile(*shape)
        else:
            self.held, self.outer, self.middle = share.held, share.outer, share.middle
        self.sems = program.sems(2, 4 * count)
        self.local = program.sems(count)
        self.count = count

    def bind(self, ref):
        self.refs = Bag(
            total=ref(self.total),
            other=ref(self.other),
            held=ref(self.held).at[:, pl.ds(0, self.unit)],
            outer=ref(self.outer).at[:, pl.ds(0, self.unit)],
            middle=ref(self.middle).at[:, pl.ds(0, self.unit)],
            sems=ref(self.sems),
            local=ref(self.local),
        )
        z, up, down = line_place()
        self.up, self.down = up, down
        self.is_outer = jnp.logical_or(z == 0, z == 3)
        self.is_inner = jnp.logical_not(self.is_outer)
        self.low = z < 2
        return self

    def _hop(self, kind, k, at):
        r = self.refs
        target = (r.outer, r.middle, r.outer, r.other)[kind]
        return hop(r.held.at[k], target.at[k], r.sems, kind * self.count + k, at)

    def _store(self, k):
        r = self.refs
        return pltpu.make_async_copy(r.held.at[k], r.total.at[k], r.local.at[k])

    def _send(self, kind, k):
        if kind == BACK:
            low, high = self.down, self.up
        else:
            low, high = self.up, self.down
        pl.when(self.low)(lambda: self._hop(kind, k, low).start())
        pl.when(jnp.logical_not(self.low))(lambda: self._hop(kind, k, high).start())

    def take(self, k, values):
        self.refs.held[k] = values
        pl.when(self.is_outer)(lambda: self._send(INWARD, k))

    def meet(self, k):
        r = self.refs

        @pl.when(self.is_inner)
        def _():
            self._hop(INWARD, k, self.up).wait_recv()
            r.held[k] += r.outer[k]
            self._send(ACROSS, k)

    def leave(self, k):
        r = self.refs

        @pl.when(self.is_inner)
        def _():
            self._hop(ACROSS, k, self.up).wait()
            r.held[k] += r.middle[k]
            self._send(BACK, k)
            self._hop(SWAP, k, CORE).start()
            self._store(k).start()

    def collect(self, k):
        r = self.refs

        @pl.when(self.is_outer)
        def _():
            self._hop(INWARD, k, self.up).wait_send()
            self._hop(BACK, k, self.up).wait_recv()
            r.held[k] = r.outer[k]
            self._hop(SWAP, k, CORE).start()
            self._store(k).start()

    def done(self, k):
        pl.when(self.is_inner)(lambda: self._hop(BACK, k, self.up).wait_send())
        self._store(k).wait()
        self._hop(SWAP, k, CORE).wait()


class Spread:
    def __init__(self, program, rows, shape):
        self.rows = rows
        self.landed = program.output(3, *shape[1:])
        self.sems = program.sems(2, 3)

    def bind(self, ref):
        self.refs = ref(self.rows), ref(self.landed), ref(self.sems)
        return self

    def _hop(self, r):
        rows, landed, sems = self.refs
        to = lax.axis_index(TENSOR) ^ r
        return hop(rows.at[to], landed.at[r - 1], sems, r - 1, {TENSOR: to})

    def start(self):
        for r in (3, 1, 2):
            self._hop(r).start()

    def finish(self):
        for r in (1, 2, 3):
            self._hop(r).wait()


class Vectors:
    def __init__(self, program, shape):
        self.total = program.output(*shape, dtype=F32)
        self.held = program.tile(*shape, dtype=F32)
        self.got = program.tile(6, *shape, dtype=F32)
        self.sems = program.sems(2, 6)
        self.local = program.sems(1)

    def bind(self, ref):
        self.refs = Bag(
            total=ref(self.total),
            held=ref(self.held),
            got=ref(self.got),
            sems=ref(self.sems),
            local=ref(self.local),
        )
        return self

    def _step(self, k, at):
        r = self.refs
        return hop(r.held, r.got.at[k], r.sems, k, at)

    def plane(self):
        held, got = self.refs.held, self.refs.got
        for k, (bit, turn) in enumerate(((CORE, 1), (X, 2), (Y, 4))):
            self._step(k, bit).start()
            self._step(k, bit).wait()
            held[0:8] += got[k, 0:8]
            for p in range(8):
                held[8 + p] += got[k, 8 + (p ^ turn)]

    def line(self):
        r = self.refs
        held, got = r.held, r.got
        z, up, down = line_place()
        is_outer = jnp.logical_or(z == 0, z == 3)
        low = z < 2

        def towards(k, first, second):
            pl.when(low)(lambda: self._step(k, first).start())
            pl.when(jnp.logical_not(low))(lambda: self._step(k, second).start())

        @pl.when(is_outer)
        def _():
            towards(3, up, down)
            self._step(3, up).wait_send()

        @pl.when(jnp.logical_not(is_outer))
        def _():
            self._step(3, up).wait_recv()
            held[...] += got[3]
            towards(4, up, down)
            self._step(4, up).wait()
            held[...] += got[4]
            towards(5, down, up)

        def last():
            @pl.when(is_outer)
            def _():
                self._step(5, up).wait_recv()
                held[...] = got[5]

            pl.when(jnp.logical_not(is_outer))(lambda: self._step(5, up).wait_send())
            fetch(held, r.total, r.local.at[0]).wait()

        return last


class Stream:
    def __init__(self, program, group, unit, width):
        self.group, self.unit = group, unit
        self.held = program.tile(2, group, 2, unit, width)
        self.sems = program.sems(2, group * 2)

    def bind(self, ref):
        self.refs = ref(self.held), ref(self.sems)
        return self

    def _copies(self, gather, index, slot, size):
        held, sems = self.refs
        return [
            pltpu.make_async_copy(
                gather.piece((index * self.group + g) // 2, (index * self.group + g) % 2, c).at[
                    pl.ds(0, size)
                ],
                held.at[slot, g, c, pl.ds(0, size)],
                sems.at[slot, 2 * g + c],
            )
            for g in range(self.group)
            for c in range(2)
        ]

    def begin(self, gather, index, size=None):
        for each in self._copies(gather, index, index % 2, size or self.unit):
            each.start()

    def here(self, gather, slot):
        for each in self._copies(gather, 0, slot, self.unit):
            each.wait()

    def bring(self, gather, step, first, last, size=None):
        size = size or self.unit
        for index in range(first + 1, last):
            pl.when(step == index - 1 - first)(
                lambda index=index: self.begin(gather, index, size)
            )
        slot = lax.rem(step + first, 2)
        for each in self._copies(gather, 0, slot, size):
            each.wait()
        held = self.refs[0]
        return held[slot, :, :, 0:size].reshape(-1, held.shape[-1])


def prepare_body(
    slot_ref, live_ref, im_ref, go_ref, gain_ref, shift_ref, own_ref, row_ref,
    x_ref, g_ref, n_ref, s_ref, early_ref, bias_ref, sems,
):
    step = pl.program_id(0)
    slot = slot_ref[0]
    hops = [lambda lane=lane: hop(own_ref.at[lax.rem(lax.axis_index(DP), 2), lane], early_ref.at[lane], sems, lane, LANES[lane]) for lane in range(2)]
    for r in range(1, 4):
        to = {TENSOR: lax.axis_index(TENSOR) ^ r}
        hops.append(lambda r=r, to=to: hop(row_ref, bias_ref.at[r - 1], sems, 1 + r, to))

    @pl.when(step == 0)
    def _():
        meet((X, Y, XY))
        for each in hops[2:] + hops[:2]:
            each().start()

    def pick(ref):
        values = ref[...].astype(F32)
        chosen = values[:, 0]
        for index in range(1, values.shape[1]):
            chosen = jnp.where(slot == index, values[:, index], chosen)
        return chosen

    picture = pick(im_ref)
    centered = picture - row_mean(picture)
    inverse = lax.rsqrt(row_mean(centered * centered) + EPS)
    normed = centered * inverse * gain_ref[...] + shift_ref[...]
    x_ref[...] = picture.T.astype(BF)
    g_ref[...] = (pick(go_ref) * live_ref[0].astype(F32)).T.astype(BF)
    n_ref[...] = normed.T.astype(BF)
    s_ref[0:1, :] = row_mean(picture).T
    s_ref[1:2, :] = inverse.T

    @pl.when(step == pl.num_programs(0) - 1)
    def _():
        for each in hops:
            each().wait()


def prepare(images, grad_out, slot, live, gain, shift, own, bias):
    slots, length, width = images.shape
    rows = 128
    scalar = pl.BlockSpec(memory_space=pltpu.SMEM)
    tokens = pl.BlockSpec((rows, slots, width), lambda i: (i, 0, 0))
    vector = pl.BlockSpec((1, width), lambda i: (0, 0))
    return pl.pallas_call(
        prepare_body,
        grid=(pl.cdiv(length, rows),),
        in_specs=[scalar, scalar, tokens, tokens, vector, vector, ANYWHERE, ANYWHERE],
        out_specs=[pl.BlockSpec((width, rows), lambda i: (0, i))] * 3
        + [pl.BlockSpec((2, rows), lambda i: (0, i)), ANYWHERE, ANYWHERE],
        out_shape=[jax.ShapeDtypeStruct((width, length), BF)] * 3
        + [
            jax.ShapeDtypeStruct((2, length), F32),
            jax.ShapeDtypeStruct(own.shape[1:], BF),
            jax.ShapeDtypeStruct((3, *bias.shape), F32),
        ],
        scratch_shapes=[pltpu.SemaphoreType.DMA((2, 5))],
        compiler_params=pltpu.CompilerParams(
            vmem_limit_bytes=67_043_328, collective_id=1, has_side_effects=True
        ),
        name="prepare",
    )(slot, live, images.transpose(1, 0, 2), grad_out.transpose(1, 0, 2), gain, shift, own, bias)


def as_column(row):
    return jnp.broadcast_to(row, (8, row.shape[1])).T[:, 0:1]


def as_row(column):
    return jnp.broadcast_to(column, (column.shape[0], 8)).T[0:1, :]


def attend_head(weight, normed, bias, qkv_ref, o_ref, lse_ref):
    length = normed.shape[1]
    rows = dot_nn(weight, normed)
    queries = ((rows[:HD] + bias[0]) * (LOG2E / math.sqrt(HD))).astype(BF)
    keys_t = rows[HD : 2 * HD].astype(BF)
    values = (rows[2 * HD :] + bias[1]).astype(BF)
    qkv_ref[0, 0] = queries
    qkv_ref[0, 1] = keys_t
    qkv_ref[0, 2] = values
    keys = keys_t.T
    for start in range(0, length, QUERY_BLOCK):
        block = slice(start, min(start + QUERY_BLOCK, length))
        scores = dot_nn(keys, queries[:, block])
        top = jnp.max(scores, axis=0, keepdims=True)
        weights = jnp.exp2(scores - top)
        total = jnp.sum(weights, axis=0, keepdims=True)
        mixed = dot_nn(values, weights.astype(BF))
        o_ref[0, :, block] = (mixed * (1.0 / total)).astype(BF)
        lse_ref[0, :, block] = top + jnp.log2(total)


def attend_back_head(qkv_ref, do_ref, o_ref, lse_ref, d_ref, dk_acc, dv_acc):
    keys_t = qkv_ref[0, 1]
    keys = keys_t.T
    values = qkv_ref[0, 2].T
    length = keys_t.shape[1]
    scale = 1.0 / math.sqrt(HD)
    for start in range(0, length, QUERY_BLOCK):
        block = slice(start, min(start + QUERY_BLOCK, length))
        queries_t = qkv_ref[0, 0, :, block]
        pull_t = do_ref[0, :, block]
        delta = jnp.sum(
            pull_t.astype(F32) * o_ref[0, :, block].astype(F32), axis=0, keepdims=True
        )
        probs = jnp.exp2(dot_nn(keys, queries_t) - lse_ref[0, :, block])
        probs_low = probs.astype(BF)
        d_probs = dot_nn(values, pull_t)
        d_scores = (probs * (d_probs - delta)).astype(BF)
        d_ref[0, 0, :, block] = (dot_nn(keys_t, d_scores) * scale).astype(BF)
        d_keys = dot_nn(d_scores, queries_t.T)
        d_values = dot_nn(probs_low, pull_t.T)
        if start == 0:
            dk_acc[...] = d_keys
            dv_acc[...] = d_values
        else:
            dk_acc[...] += d_keys
            dv_acc[...] += d_values
    d_ref[0, 1] = (dk_acc[...].T * LN2).astype(BF)
    d_ref[0, 2] = dv_acc[...].T.astype(BF)
    return [jnp.sum(d_ref[0, k].astype(F32), axis=1, keepdims=True) for k in (0, 2)]


def columns_of(length, block=128):
    return [slice(start, min(start + block, length)) for start in range(0, length, block)]


def norm_back(grad, unit_values, inverse, gain):
    scaled = grad * gain
    mean = lambda values: jnp.mean(values, axis=0, keepdims=True)
    return inverse * (scaled - mean(scaled) - unit_values * mean(scaled * unit_values))


def turned(values, axis, bit):
    return jnp.where(bit == 1, lax.rev(values, (axis,)), values)


def forward(attn_own, early, fc1_own, fc2_own, bias, bias_far, picture, normed_one, vectors):
    width, length = picture.shape
    chunk = attn_own.shape[2]
    unit = fc1_own.shape[2]
    rows = 2 * unit
    heads = 16
    p = Program("forward", (X, Y, CORE))
    own, soon, own_fc1 = p.input(attn_own), p.input(early), p.input(fc1_own)
    bias_in, x_in, n_in, v_in = p.input(bias), p.input(picture), p.input(normed_one), p.input(vectors)
    bias_far_in = p.input(bias_far)
    attn = Gather(p, own, attn_own.shape, soon)
    fc1 = Gather(p, own_fc1, fc1_own.shape)
    own_fc2, soon_fc2 = p.input(fc2_own), p.output(*fc2_own.shape[1:])
    soon_sems = p.sems(2, 2)
    stream = Stream(p, 1, unit, width)
    qkv, mixed = p.output(heads, 3, HD, length), p.output(heads, HD, length)
    lse = p.output(heads, 1, length, dtype=F32)
    residual, normed = p.output(3, width, 256, dtype=F32), p.output(width, length)
    stats, out_all = p.output(2, length, dtype=F32), p.output(heads, HD, width)
    act, slope = p.output(8, rows, length), p.output(8, rows, length)
    held = Bag(
        bias=p.tile(4, *bias.shape, dtype=F32),
        x=p.tile(width, length),
        n=p.tile(width, length),
        v=p.tile(*vectors.shape, dtype=F32),
        o=p.tile(heads, HD, length),
        w=p.tile(heads, HD, width),
        h=p.tile(3, width, 256, dtype=F32),
        n2=p.tile(width, length),
        s=p.tile(2, length, dtype=F32),
        rows=p.tile(2, 3 * HD, width),
    )
    sems, wsems, hsems = p.sems(8), p.sems(heads), p.sems(2)

    def script(ref):
        hold = held.each(ref)
        sem, wsem, hsem = ref(sems), ref(wsems), ref(hsems)
        attn.bind(ref)
        fc1.bind(ref)
        stream.bind(ref)
        attn.start()
        attn.forward()
        fc1.start()
        copies = [
            fetch(ref(n_in), hold.n, sem.at[0]),
            fetch(ref(bias_in), hold.bias.at[0], sem.at[1]),
            fetch(ref(bias_far_in), hold.bias.at[pl.ds(1, 3)], sem.at[2]),
            fetch(ref(x_in), hold.x, sem.at[5]),
            fetch(ref(v_in), hold.v, sem.at[6]),
        ]
        for each in copies[:3]:
            each.wait()

        def weights_in(head, slot):
            shard, half, lane = head // 4, (head // 2) % 2, head % 2
            return pltpu.make_async_copy(
                attn.piece(shard, half, lane).at[pl.ds(0, 3 * HD)], hold.rows.at[slot], hsem.at[slot]
            )

        def near_all():
            attn.near_here()
            attn.near_whole()

        def far_all():
            attn.far_here()
            attn.far_whole()

        def head(step, qkv_ref, o_ref, lse_ref):
            pl.when(step == 3)(near_all)
            pl.when(step == 11)(far_all)
            slot = lax.rem(step, 2)
            for each in range(1, heads):
                pl.when(step == each - 1)(
                    lambda each=each: weights_in(each, each % 2).start()
                )
            weights_in(0, slot).wait()
            shard, half, lane = step // 4, lax.rem(step // 2, 2), lax.rem(step, 2)
            at = 4 * half + 2 * lane
            shift = [as_column(hold.bias[shard, at + k, :, 0:HD]) for k in range(2)]
            attend_head(hold.rows[slot], hold.n[...], shift, qkv_ref, o_ref, lse_ref)
            hold.o[step] = o_ref[0]

        def bring_out(shard):
            return [
                pltpu.make_async_copy(
                    attn.piece(shard, half, lane).at[pl.ds(3 * HD, HD)],
                    hold.w.at[4 * shard + 2 * half + lane],
                    wsem.at[4 * shard + 2 * half + lane],
                )
                for half in range(2)
                for lane in range(2)
            ]

        weights_in(0, 0).start()
        phase(
            heads,
            head,
            [],
            [],
            [ref(qkv), ref(mixed), ref(lse)],
            [
                spec((1, 3, HD, length), lambda i: (i, 0, 0, 0)),
                spec((1, HD, length), lambda i: (i, 0, 0)),
                spec((1, 1, length), lambda i: (i, 0, 0)),
            ],
        )
        for shard in range(4):
            for each in bring_out(shard):
                each.start()
        fc1.forward()
        core = lax.rem(lax.axis_index(DP), 2)
        ahead = lambda lane: hop(
            ref(own_fc2).at[core, lane], ref(soon_fc2).at[lane], ref(soon_sems), lane, LANES[lane]
        )
        for lane in range(2):
            ahead(lane).start()
        for each in copies[3:]:
            each.wait()
        for shard in range(4):
            for each in bring_out(shard):
                each.wait()
        stream.begin(fc1, 0)
        store_w = fetch(hold.w, ref(out_all), sem.at[4])
        weight = hold.w[...].reshape(width, width)
        for block in columns_of(length, 256):
            mix = hold.o[:, :, block].reshape(width, -1)
            values = hold.x[:, block].astype(F32) + contract_rows(weight, mix)
            values = values + hold.v[:, 2:3]
            average = jnp.mean(values, axis=0, keepdims=True)
            centered = values - average
            inverse = lax.rsqrt(jnp.mean(centered * centered, axis=0, keepdims=True) + EPS)
            hold.h[block.start // 256, :, 0 : block.stop - block.start] = values
            hold.n2[:, block] = (
                centered * inverse * hold.v[:, 3:4] + hold.v[:, 4:5]
            ).astype(BF)
            hold.s[0:1, block] = average
            hold.s[1:2, block] = inverse
        stores = [store_w] + [
            fetch(source, ref(target), sem.at[k])
            for k, (source, target) in enumerate(((hold.h, residual), (hold.n2, normed), (hold.s, stats)))
        ]

        def hidden(step, act_ref, slope_ref):
            weight = stream.bring(fc1, step, 0, 8)
            shard, half = step // 2, lax.rem(step, 2)
            shift = as_column(hold.bias[shard, half, :, 128 : 128 + rows])
            preact = dot_nn(weight, hold.n2[...]) + shift
            square = preact * preact
            curve = jnp.tanh(preact * (GELU_A + (GELU_A * GELU_B) * square))
            rise = 0.5 * (1.0 + curve)
            act_ref[0] = (preact * rise).astype(BF)
            inner = GELU_A + (3.0 * GELU_A * GELU_B) * square
            slope_ref[0] = (rise + (0.5 * preact) * (1.0 - curve * curve) * inner).astype(BF)

        block = spec((1, rows, length), lambda i: (i, 0, 0))

        def fc1_near():
            fc1.near_here()
            fc1.near_whole()

        def fc1_far():
            fc1.far_here()
            fc1.far_whole()

        phase(
            8, hidden, [], [], [ref(act), ref(slope)], [block, block],
            [(1, fc1_near), (5, fc1_far)],
        )
        for each in stores:
            each.wait()
        attn.drain()
        fc1.drain()
        for lane in range(2):
            ahead(lane).wait()

    result = p.call(script, 2, 3e10)
    return (
        gathered(attn).each(result),
        gathered(fc1).each(result),
        Bag(
            qkv=qkv,
            mixed=mixed,
            lse=lse,
            residual=residual,
            normed_two=normed,
            stats_two=stats,
            out_all=out_all,
            act=act,
            slope=slope,
        ).each(result),
        result(soon_fc2),
    )


def gathered(source):
    return Bag(
        near=source.near, near_part=source.near_part, far=source.far, far_part=source.far_part
    )


class Ready:
    def __init__(self, program, own, parts, early=None):
        self.handles = parts.each(program.input)
        self.handles.own = program.input(own)
        self.handles.early = None if early is None else program.input(early)
        self.early = early

    def bind(self, ref):
        self.refs = self.handles.each(lambda h: None if h is None else ref(h))
        return self

    piece = Gather.piece


def backward(arrays, fc1_parts, attn_parts, owns, early, fc2_early, live):
    width, length = arrays.picture.shape
    share = width // 4
    unit = owns.fc2.shape[2]
    rows = 2 * unit
    block = 3 * HD
    p = Program("backward", (X, Y, XY, CORE, LINE))
    into = arrays.each(p.input)
    live_in = p.input(live, pl.BlockSpec(memory_space=pltpu.SMEM))
    fc1 = Ready(p, owns.fc1, fc1_parts)
    attn = Ready(p, owns.attn, attn_parts, early)
    fc2 = Gather(p, p.input(owns.fc2), owns.fc2.shape, p.input(fc2_early))
    stream = Stream(p, 2, unit, width)

    fc_shape, out_shape, qkv_shape = ((4, 2, u, width) for u in (unit, HD, block))
    shapes = (fc_shape, fc_shape, out_shape, qkv_shape)
    plane = [Plane(p, shape) for shape in shapes[:QKV]]
    plane.append(Plane(p, shapes[QKV], plane[FC2]))
    line = [Line(p, shape[1:]) for shape in shapes[:QKV]]
    line.append(Line(p, shapes[QKV][1:], line[FC2]))
    d_pre = p.output(8, rows, length)
    pull = p.output(16, HD, length)
    d_qkv = p.output(16, 3, HD, length)
    block_rows, input_rows = p.output(4, share, length), p.output(4, share, length)
    spread_block = Spread(p, block_rows, (4, share, length))
    spread_input = Spread(p, input_rows, (4, share, length))
    vectors = Vectors(p, (16, 1, width))
    held = Bag(
        upstream=p.tile(width, length),
        normed_two=p.tile(width, length),
        normed_one=p.tile(width, length),
        low=p.tile(width, length),
        residual=p.tile(width, 256, dtype=F32),
        acc=p.tile(width, length, dtype=F32),
        vectors=p.tile(*arrays.vectors.shape, dtype=F32),
        stats_two=p.tile(2, length, dtype=F32),
        stats_one=p.tile(2, length, dtype=F32),
        rows=p.tile(2, rows, length),
        heads=p.tile(3, 2, 3, HD, length),
        part=p.tile(2, 2, unit, width),
    )
    tile_sems = p.sems(2)
    sems = p.sems(12)

    def script(ref):
        hold = held.each(ref)
        sem = ref(sems)
        for each in (fc1, attn, fc2, stream, spread_block, spread_input, vectors):
            each.bind(ref)
        for group in (plane, line):
            for each in group:
                each.bind(ref)
        vec = vectors.refs.held
        array = into.each(ref)
        live_now = ref(live_in)[0].astype(F32)

        copies = Bag(
            upstream=fetch(array.upstream, hold.upstream, sem.at[0]),
            normed_two=fetch(array.normed_two, hold.normed_two, sem.at[1]),
            vectors=fetch(array.vectors, hold.vectors, sem.at[3]),
            stats_two=fetch(array.stats_two, hold.stats_two, sem.at[4]),
            normed_one=fetch(array.normed_one, hold.normed_one, sem.at[5]),
            stats_one=fetch(array.stats_one, hold.stats_one, sem.at[6]),
        )
        fc2.start()
        fc2.forward()
        stream.begin(fc2, 0)
        vec[...] = jnp.zeros(vec.shape, F32)
        copies.upstream.wait()
        copies.normed_two.wait()

        tile_sem = ref(tile_sems)

        def rows_in(source, index, slot):
            if len(source.shape) == 3 and source.shape[0] == 8:
                target = hold.rows.at[slot]
                source = source.at[index]
            else:
                target = hold.heads.at[slot, :, 0]
                source = source.at[pl.ds(2 * index, 2)]
            return pltpu.make_async_copy(source, target, tile_sem.at[slot])

        def rows_of(source, slot, count):
            if len(source.shape) == 3 and source.shape[0] == 8:
                return hold.rows[slot]
            return hold.heads[slot, :, 0].reshape(count, length)

        def gradient(source, other, name, shards, go=True):
            _, _, size, _ = shapes[name]
            count = 2 * size
            total = len(shards)

            def pick(i):
                if total == 1:
                    return shards[0]
                if total == 2:
                    return jnp.where(i == 0, shards[0], shards[1])
                return jnp.where(
                    i < 2,
                    jnp.where(i == 0, shards[0], shards[1]),
                    jnp.where(i == 2, shards[2], shards[3]),
                )

            part_of = lambda slot, lane: hold.part.at[slot, lane, pl.ds(0, size)]
            sums_of = plane[name]
            piece = lambda k: jnp.where(
                k < total, 2 * pick(k) + 1, 2 * pick(jnp.maximum(k - total, 0))
            )
            rows_in(source, 2 * shards[0] + 1, 0).start()

            def product(k):
                slot = lax.rem(k, 2)

                @pl.when(k + 1 < 2 * total)
                def _():
                    rows_in(source, piece(k + 1), 1 - slot).start()

                rows_in(source, 0, slot).wait()
                return contract_cols(rows_of(source, slot, count), other[...])

            def give(i, _):
                slot = lax.rem(i, 2)
                shard = pick(i)

                @pl.when(i >= 2)
                def _():
                    for lane in range(2):
                        before = pick(jnp.maximum(i - 2, 0))
                        sums_of.swap(part_of(slot, lane), before, lane).wait_send()

                sums = product(i).astype(BF).reshape(2, size, width)
                for lane in range(2):
                    part_of(slot, lane)[...] = sums[lane]
                for lane in range(2):
                    sums_of.swap(part_of(slot, lane), shard, lane).start()
                return 0

            def keep(i, _):
                shard = pick(i)
                for lane in range(2):
                    sums_of.swap(part_of(0, lane), shard, lane).wait_recv()
                sums_of.add(shard, product(total + i).reshape(2, size, width), go)
                return 0

            lax.fori_loop(0, total, give, 0)
            lax.fori_loop(0, total, keep, 0)
            for i in range(max(total - 2, 0), total):
                for lane in range(2):
                    sums_of.swap(
                        part_of(i % 2, lane), jnp.int32(shards[i]), lane
                    ).wait_send()

        every = (3, 1, 2, 0)
        gradient(array.act, hold.upstream, FC2, every, False)

        def hidden(step, slope_ref, d_ref):
            slot = lax.rem(step, 2)
            stream.here(fc2, slot)
            pl.when(step == 1)(lambda: stream.begin(fc2, 2))
            for half in range(2):
                weight = stream.refs[0][slot, half].reshape(rows, width)
                values = dot_nn(weight, hold.upstream[...])
                values = (values * slope_ref[half].astype(F32)).astype(BF)
                d_ref[half] = values
                sums = jnp.sum(values.astype(F32), axis=1, keepdims=True)
                vec[8 + 2 * step + half, :, 0:rows] = as_row(sums)

            @pl.when(step == 0)
            def _():
                fc2.near_here()
                fc2.near_whole()
                stream.begin(fc2, 1)

            @pl.when(step == 2)
            def _():
                fc2.far_here()
                fc2.far_whole()
                stream.begin(fc2, 3)

        plane[FC2].launch()
        pair = spec((2, rows, length), lambda i: (i, 0, 0))
        phase(4, hidden, [array.slope], [pair], [ref(d_pre)], [pair])

        def back(weights, values, lead, size, events=()):
            def body(step, d_ref):
                weight = stream.bring(weights, step, 0, 4, size)
                values = d_ref[...].reshape(4 * size, length)
                hold.acc[...] += contract_rows(weight, values)

            hold.acc[...] = jnp.zeros(hold.acc.shape, F32)
            tail = values.shape[1:]
            zeros = (0,) * len(tail)
            phase(4, body, [values], [spec((lead, *tail), lambda i: (i, *zeros))], [], [], events)

        stream.begin(fc1, 0)
        back(fc1, ref(d_pre), 2, unit)
        for each in (copies.vectors, copies.stats_two):
            each.wait()
        total = lambda values: jnp.sum(values, axis=1, keepdims=True)
        residual_of = parts_of(array.residual, hold.residual, sem.at[2])
        for cut in columns_of(length):
            inverse = hold.stats_two[1:2, cut]
            grad = hold.acc[:, cut]
            units = (residual_of(cut) - hold.stats_two[0:1, cut]) * inverse
            up = hold.upstream[:, cut].astype(F32)
            d_residual = up + norm_back(grad, units, inverse, hold.vectors[:, 3:4])
            hold.low[:, cut] = d_residual.astype(BF)
            hold.vectors[:, 10:11] += total(d_residual)
            hold.vectors[:, 11:12] += total(grad * units)
            hold.vectors[:, 12:13] += total(grad)
            hold.vectors[:, 13:14] += total(up)

        plane[FC2].forward()
        plane[FC2].settle()
        picture_copy = fetch(array.picture, hold.upstream, sem.at[7])

        def pull_body(step, w_ref, o_ref):
            weight = w_ref[...].reshape(4 * HD, width)
            o_ref[...] = dot_nn(weight, hold.low[...]).reshape(4, HD, length).astype(BF)

        quarter = lambda *tail: spec((4, *tail), lambda i: (i, *(0 for _ in tail)))
        phase(
            4, pull_body, [array.out_all], [quarter(HD, width)], [ref(pull)], [quarter(HD, length)]
        )
        gradient(ref(d_pre), hold.normed_two, FC1, every)
        plane[FC2].finish(line[FC2])
        plane[FC2].drain()
        gradient(array.mixed, hold.low, OUT, every)
        copies.normed_one.wait()

        def settle(name):
            plane[name].forward()
            plane[name].settle()

        events = [
            (1, 0, lambda: line[FC2].meet(0)),
            (2, 0, lambda: line[FC2].meet(1)),
            (2, 0, lambda: line[FC2].leave(0)),
            (1, 2, lambda: settle(FC1)),
            (2, 2, lambda: settle(OUT)),
            (3, 0, lambda: plane[FC1].finish(line[FC1])),
            (3, 0, lambda: line[FC2].leave(1)),
            (3, 1, lambda: line[FC2].collect(0)),
        ]
        part_of = lambda lane: hold.part.at[0, lane, pl.ds(0, block)]
        sums_of = plane[QKV]

        def qkv_rows(slot):
            values = hold.heads[slot].reshape(2 * block, length)
            return contract_cols(values, hold.normed_one[...]).reshape(2, block, width)

        def keep_rows(shard, slot):
            for lane in range(2):
                sums_of.swap(part_of(lane), shard, lane).wait()
            sums_of.add(shard, qkv_rows(slot), True)

        order = lambda g: jnp.where(
            g < 2, jnp.where(g == 0, every[0], every[1]), jnp.where(g == 2, every[2], every[3])
        )

        dk_acc = hold.acc.at[pl.ds(0, length), pl.ds(0, HD)]
        dv_acc = hold.acc.at[pl.ds(0, length), pl.ds(128, HD)]

        def shard_back(g, _):
            shard = order(g)
            at = lambda i: 4 * shard + i

            def body(step, qkv_ref, do_ref, o_ref, lse_ref, d_ref):
                for when, now, event in events:
                    pl.when(jnp.logical_and(g == when, step == now))(event)
                sums = attend_back_head(
                    qkv_ref, do_ref, o_ref, lse_ref, d_ref, dk_acc, dv_acc
                )
                half, lane = step // 2, lax.rem(step, 2)
                hold.heads[jnp.where(half == 1, 0, 1 + lax.rem(g, 2)), lane] = d_ref[0]
                for k in range(2):
                    where = pl.multiple_of(640 + 128 * (2 * lane + k), 128)
                    padded = jnp.concatenate(
                        [as_row(sums[k]), jnp.zeros((1, 128 - HD), F32)], axis=1
                    )
                    vec[8 + 2 * shard + half, :, pl.ds(where, 128)] = padded

            flat = spec((1, HD, length), lambda i: (at(i), 0, 0))
            many = spec((1, 3, HD, length), lambda i: (at(i), 0, 0, 0))
            phase(
                4,
                body,
                [array.qkv, ref(pull), array.mixed, array.lse],
                [many, flat, flat, spec((1, 1, length), lambda i: (at(i), 0, 0))],
                [ref(d_qkv)],
                [many],
            )
            pl.when(g > 0)(lambda: keep_rows(order(g - 1), 1 + lax.rem(g + 1, 2)))
            sums = qkv_rows(0).astype(BF)
            for lane in range(2):
                part_of(lane)[...] = sums[lane]
            for lane in range(2):
                sums_of.swap(part_of(lane), shard, lane).start()
            return 0

        lax.fori_loop(0, 4, shard_back, 0)
        plane[OUT].finish(line[OUT])
        stream.begin(fc2, 0)
        keep_rows(jnp.int32(every[3]), 2)
        plane[QKV].forward()
        line[FC1].meet(0)
        back(
            fc2,
            array.act,
            2,
            unit,
            [
                (1, lambda: line[FC2].collect(1)),
                (2, plane[QKV].settle),
                (3, lambda: line[FC1].meet(1)),
            ],
        )
        line[FC1].leave(0)
        stream.begin(attn, 0, block)
        residual_of = parts_of(array.residual, hold.residual, sem.at[2])
        for cut in columns_of(length):
            values = residual_of(cut) + hold.acc[:, cut] + hold.vectors[:, 5:6]
            hold.normed_two[:, cut] = (values * live_now).astype(BF)
        store_rows(hold.normed_two, ref(block_rows), sem, share)
        for k in range(2):
            line[FC2].done(k)
        plane[QKV].finish(line[QKV])
        spread_block.start()
        line[OUT].meet(0)
        line[OUT].meet(1)
        picture_copy.wait()
        copies.stats_one.wait()
        back(
            attn,
            ref(d_qkv),
            4,
            block,
            [(2, lambda: line[FC1].leave(1)), (3, lambda: line[QKV].meet(0))],
        )
        line[OUT].leave(0)
        line[OUT].leave(1)
        for cut in columns_of(length):
            inverse = hold.stats_one[1:2, cut]
            grad = hold.acc[:, cut]
            units = hold.upstream[:, cut].astype(F32) - hold.stats_one[0:1, cut]
            units = units * inverse
            d_input = hold.low[:, cut].astype(F32) + norm_back(
                grad, units, inverse, hold.vectors[:, 0:1]
            )
            hold.normed_two[:, cut] = d_input.astype(BF)
            hold.vectors[:, 8:9] += total(grad * units)
            hold.vectors[:, 9:10] += total(grad)
        line[QKV].meet(1)
        line[QKV].leave(0)
        wide = hold.vectors[:, 8:16].T
        for k in range(8):
            vec[k] = wide[k : k + 1]
        vectors.plane()
        store_rows(hold.normed_two, ref(input_rows), sem, share)
        spread_input.start()
        line[QKV].leave(1)
        last = vectors.line()
        for each in (line[FC1], line[OUT], line[QKV]):
            for k in range(2):
                each.collect(k)
        last()
        spread_block.finish()
        spread_input.finish()
        for each in line[1:]:
            for k in range(2):
                each.done(k)
        for each in plane[1:]:
            each.drain()
        fc2.drain()

    result = p.call(script, 3, 8e10)
    sums = [(result(each.total), result(each.other)) for each in line]
    spreads = [
        (result(block_rows), result(spread_block.landed)),
        (result(input_rows), result(spread_input.landed)),
    ]
    return sums, spreads, result(vectors.total)[:, 0]


def parts_of(source, held, sem):
    width = held.shape[1]

    def bring(part):
        return fetch(source.at[part], held, sem)

    bring(0).wait()

    def columns(cut):
        if cut.start > 0 and cut.start % width == 0:
            bring(cut.start // width).wait()
        first = cut.start % width
        return held[:, first : first + cut.stop - cut.start]

    return columns


def store_rows(source, target, sem, share):
    copies = [
        fetch(source.at[pl.ds(k * share, share)], target.at[k], sem.at[k]) for k in range(4)
    ]
    for each in copies:
        each.wait()


def finish(sums, spreads, place_t, core, hidden):
    width = sums[FC2][0].shape[-1]
    share, length = spreads[0][0].shape[1:]

    def body(at, *refs):
        step = pl.program_id(0)
        same = lax.rem(step // 2 + at[1], 2) == 0
        ins, outs = refs[:12], refs[12:]
        for k in range(4):
            rows = jnp.where(same, ins[2 * k][0], ins[2 * k + 1][0]).astype(F32)
            outs[k][...] = rows.reshape(outs[k].shape)
        for k in range(2):
            rows = jnp.where(step == at[0], ins[8 + 2 * k][0], ins[9 + 2 * k][0])
            outs[4 + k][0] = rows.astype(F32)

    half = lambda array: pl.BlockSpec((1, *array.shape[1:]), lambda i, at: (lax.rem(i, 2), 0, 0))
    own = pl.BlockSpec((1, share, length), lambda i, at: (at[0], 0, 0))
    landed = pl.BlockSpec(
        (1, share, length), lambda i, at: (jnp.maximum((i ^ at[0]) - 1, 0), 0, 0)
    )
    units = [pair[0].shape[1] for pair in sums]
    rows = lambda unit: pl.BlockSpec((unit, width), lambda i, at: (i, 0))
    slot = pl.BlockSpec((1, share, length), lambda i, at: (i, 0, 0))
    shape = lambda *dims: jax.ShapeDtypeStruct(dims, F32)
    return pl.pallas_call(
        body,
        grid_spec=pltpu.PrefetchScalarGridSpec(
            num_scalar_prefetch=1,
            grid=(4,),
            in_specs=[half(array) for pair in sums for array in pair] + [own, landed] * 2,
            out_specs=[
                rows(units[FC2]),
                rows(units[FC1]),
                rows(units[OUT]),
                pl.BlockSpec((3, HD, width), lambda i, at: (0, i, 0)),
                slot,
                slot,
            ],
        ),
        out_shape=[
            shape(hidden, width),
            shape(hidden, width),
            shape(share, width),
            shape(3, share, width),
            shape(4, share, length),
            shape(4, share, length),
        ],
        compiler_params=pltpu.CompilerParams(vmem_limit_bytes=67_043_328),
        name="finish",
    )(
        jnp.stack([place_t, core]).astype(jnp.int32),
        *[array for pair in sums for array in pair],
        *spreads[0],
        *spreads[1],
    )


def whole_image(
    images,
    counts,
    ln1_gain,
    ln1_bias,
    qkv_weight,
    qv_bias,
    out_weight,
    out_bias,
    ln2_gain,
    ln2_bias,
    fc1_weight,
    fc1_bias,
    fc2_weight,
    fc2_bias,
    grad_out,
):
    slot_count, length, width = images.shape
    share = width // 4
    hidden = fc1_weight.shape[1]
    unit = -(-hidden // 64) * 16
    rows = 2 * unit
    place_t = lax.axis_index(TENSOR)
    core = lax.rem(lax.axis_index(DP), 2)
    block = 3 * HD

    qkv_rows = qkv_weight.reshape(3, width, 2, 2, HD).transpose(2, 3, 0, 4, 1)
    attn_own = jnp.concatenate(
        [qkv_rows.reshape(2, 2, block, width), out_weight.reshape(2, 2, HD, width)], axis=2
    )
    pad = 2 * rows - hidden
    fc1_own, fc2_own = (
        jnp.pad(each, ((0, pad), (0, 0))).reshape(2, 2, unit, width)
        for each in (fc1_weight.T, fc2_weight)
    )
    head_bias = qv_bias.reshape(2, 2, 2, HD).transpose(1, 2, 0, 3)
    head_bias = jnp.pad(turned(head_bias, 0, core).reshape(8, HD), ((0, 0), (0, 128 - HD)))
    hidden_bias = turned(jnp.pad(fc1_bias, (0, pad)).reshape(2, rows), 0, core)
    hidden_bias = jnp.pad(hidden_bias, ((0, 6), (0, 640 - rows)))
    bias = jnp.concatenate([head_bias, hidden_bias], axis=1).astype(F32)[:, None]
    vectors = jnp.stack(
        [ln1_gain, ln1_bias, out_bias, ln2_gain, ln2_bias, fc2_bias, fc2_bias, fc2_bias], axis=1
    )
    vectors = jnp.pad(vectors, ((0, 0), (0, 8))).astype(F32)
    live = (place_t < counts[0]).astype(jnp.int32)[None]

    picture, upstream, normed_one, stats_one, early, bias_far = prepare(
        images,
        grad_out,
        place_t[None].astype(jnp.int32),
        live,
        ln1_gain.astype(F32)[None],
        ln1_bias.astype(F32)[None],
        attn_own,
        bias,
    )
    attn_parts, fc1_parts, made, fc2_early = forward(
        attn_own, early, fc1_own, fc2_own, bias, bias_far, picture, normed_one, vectors
    )
    made.__dict__.update(
        upstream=upstream,
        picture=picture,
        normed_one=normed_one,
        stats_one=stats_one,
        vectors=vectors,
    )
    owns = Bag(attn=attn_own, fc1=fc1_own, fc2=fc2_own)
    sums, spreads, totals = backward(
        made, fc1_parts, attn_parts, owns, early, fc2_early, live
    )

    own_wide = lax.dynamic_slice_in_dim(totals[:6], place_t * share, share, 1)
    own_rows = turned(totals[8:10], 0, core)
    own_hidden = own_rows[:, :rows].reshape(-1)[:hidden]
    own_qv = own_rows[:, 640:].reshape(2, 2, 2, 128)[..., :HD].transpose(2, 0, 1, 3)
    own_qv = own_qv.reshape(2, share)

    fc2_result, fc1_result, out_result, qkv_result, block_result, input_result = finish(
        sums, spreads, place_t, core, hidden
    )
    return (
        block_result.transpose(0, 2, 1),
        input_result.transpose(0, 2, 1),
        own_wide[0],
        own_wide[1],
        qkv_result.transpose(0, 2, 1),
        own_qv,
        out_result,
        own_wide[2],
        own_wide[3],
        own_wide[4],
        fc1_result.T,
        own_hidden,
        fc2_result,
        own_wide[5],
    )


def solution(mesh):
    whole_fits = mesh.shape[TENSOR] == 4 and mesh.shape[DP] == 8
    return jax.shard_map(
        whole_image if whole_fits else local,
        mesh=mesh,
        in_specs=(
            P(DP, None, None),
            P(DP),
            P(),
            P(),
            P(None, None, TENSOR),
            P(None, TENSOR),
            P(TENSOR, None),
            P(),
            P(),
            P(),
            P(None, TENSOR),
            P(TENSOR),
            P(TENSOR, None),
            P(),
            P(DP, None, None),
        ),
        out_specs=(
            P(DP, None, TENSOR),
            P(DP, None, TENSOR),
            P(TENSOR),
            P(TENSOR),
            P(None, None, TENSOR),
            P(None, TENSOR),
            P(TENSOR, None),
            P(TENSOR),
            P(TENSOR),
            P(TENSOR),
            P(None, TENSOR),
            P(TENSOR),
            P(TENSOR, None),
            P(TENSOR),
        ),
        check_vma=False,
    )
```

```python
import math

import jax
import jax.numpy as jnp
from jax import lax
from jax.experimental import pallas as pl
from jax.experimental.pallas import tpu as pltpu
from jax.sharding import PartitionSpec as P

HD = 72


EPS = 1e-06


def own_columns(values, share_width):
    start = lax.axis_index(TENSOR) * share_width
    return lax.dynamic_slice_in_dim(values, start, share_width, values.ndim - 1)


def row_mean(values):
    return jnp.mean(values, axis=-1, keepdims=True)


def group_stats(first, second):
    return lax.psum((first, second), TENSOR)


def contract_rows(left, right):
    return lax.dot_general(
        left, right, (((0,), (0,)), ((), ())), preferred_element_type=jnp.float32
    )


def contract_cols(left, right):
    return lax.dot_general(
        left, right, (((1,), (1,)), ((), ())), preferred_element_type=jnp.float32
    )


def gelu_tanh(values):
    return jax.nn.gelu(values, approximate=True)


def local(
    images,
    counts,
    ln1_gain,
    ln1_bias,
    qkv_weight,
    qv_bias,
    out_weight,
    out_bias,
    ln2_gain,
    ln2_bias,
    fc1_weight,
    fc1_bias,
    fc2_weight,
    fc2_bias,
    grad_out,
):
    slot_count, length, full_width = images.shape
    share_width = full_width // lax.axis_size(TENSOR)
    local_width = qkv_weight.shape[2]
    local_heads = local_width // HD
    hidden_width = fc1_weight.shape[1]
    score_scale = 1.0 / math.sqrt(HD)
    gain_one = ln1_gain.astype(jnp.float32)
    shift_one = ln1_bias.astype(jnp.float32)
    gain_two = ln2_gain.astype(jnp.float32)
    shift_two = ln2_bias.astype(jnp.float32)
    bias_out = out_bias.astype(jnp.float32)
    bias_fc1 = fc1_bias.astype(jnp.float32)
    bias_fc2 = fc2_bias.astype(jnp.float32)
    bias_query = qv_bias[0].astype(jnp.float32)
    bias_value = qv_bias[1].astype(jnp.float32)
    live_count = counts[0]

    def to_heads(values):
        return values.reshape(length, local_heads, HD)

    def head_scores(query_heads, key_heads):
        return (
            jnp.einsum("qhd,khd->hqk", query_heads, key_heads, preferred_element_type=jnp.float32)
            * score_scale
        )

    def layer_step(slot_index, loop_state):
        block_acc, input_acc, grads = loop_state
        (
            grad_gain_one,
            grad_shift_one,
            grad_qkv,
            grad_qv,
            grad_out_w,
            grad_out_b,
            grad_gain_two,
            grad_shift_two,
            grad_fc1_w,
            grad_fc1_b,
            grad_fc2_w,
            grad_fc2_b,
        ) = grads
        live_flag = (slot_index < live_count).astype(jnp.float32)
        picture = lax.dynamic_index_in_dim(images, slot_index, 0, keepdims=False).astype(
            jnp.float32
        )
        upstream = (
            lax.dynamic_index_in_dim(grad_out, slot_index, 0, keepdims=False).astype(jnp.float32)
            * live_flag
        )
        upstream_low = upstream.astype(jnp.bfloat16)
        centered = picture - row_mean(picture)
        inv_one = lax.rsqrt(row_mean(centered * centered) + EPS)
        unit_one = centered * inv_one
        normed_one = (unit_one * gain_one + shift_one).astype(jnp.bfloat16)
        query_rows = (
            jnp.dot(normed_one, qkv_weight[0], preferred_element_type=jnp.float32) + bias_query
        ).astype(jnp.bfloat16)
        key_rows = jnp.dot(normed_one, qkv_weight[1], preferred_element_type=jnp.float32).astype(
            jnp.bfloat16
        )
        value_rows = (
            jnp.dot(normed_one, qkv_weight[2], preferred_element_type=jnp.float32) + bias_value
        ).astype(jnp.bfloat16)
        query_heads = to_heads(query_rows)
        key_heads = to_heads(key_rows)
        value_heads = to_heads(value_rows)
        scores = head_scores(query_heads, key_heads)
        row_top = jnp.max(scores, axis=-1, keepdims=True)
        logsum = row_top + jnp.log(jnp.sum(jnp.exp(scores - row_top), axis=-1, keepdims=True))
        probs_low = jnp.exp(scores - logsum).astype(jnp.bfloat16)
        mixed = jnp.einsum(
            "hqk,khd->qhd", probs_low, value_heads, preferred_element_type=jnp.float32
        )
        mixed = mixed.reshape(length, local_width).astype(jnp.bfloat16)
        partial_out = jnp.dot(mixed, out_weight, preferred_element_type=jnp.float32).astype(
            jnp.bfloat16
        )
        residual = (
            own_columns(picture, share_width)
            + lax.psum_scatter(partial_out, TENSOR, scatter_dimension=1, tiled=True).astype(
                jnp.float32
            )
            + own_columns(bias_out, share_width)
        )
        row_sum, row_square = group_stats(
            jnp.sum(residual, axis=-1), jnp.sum(residual * residual, axis=-1)
        )
        average = row_sum[:, None] / full_width
        inv_two = lax.rsqrt(row_square[:, None] / full_width - average * average + EPS)
        unit_two = (residual - average) * inv_two
        own_normed = (
            unit_two * own_columns(gain_two, share_width) + own_columns(shift_two, share_width)
        ).astype(jnp.bfloat16)
        normed_two = lax.all_gather(own_normed, TENSOR, axis=1, tiled=True)
        preact = jnp.dot(normed_two, fc1_weight, preferred_element_type=jnp.float32) + bias_fc1
        activated = gelu_tanh(preact).astype(jnp.bfloat16)
        partial_mlp = jnp.dot(activated, fc2_weight, preferred_element_type=jnp.float32).astype(
            jnp.bfloat16
        )
        block_rows = (
            residual
            + lax.psum_scatter(partial_mlp, TENSOR, scatter_dimension=1, tiled=True).astype(
                jnp.float32
            )
            + own_columns(bias_fc2, share_width)
        )
        block_rows = block_rows * live_flag
        grad_fc2_b = grad_fc2_b + own_columns(jnp.sum(upstream, axis=0), share_width)
        grad_fc2_w = grad_fc2_w + contract_rows(activated, upstream_low)
        d_act = contract_cols(upstream_low, fc2_weight)
        gelu_pull = jax.vjp(gelu_tanh, preact)[1]
        d_pre = gelu_pull(d_act)[0].astype(jnp.bfloat16)
        grad_fc1_b = grad_fc1_b + jnp.sum(d_pre.astype(jnp.float32), axis=0)
        grad_fc1_w = grad_fc1_w + contract_rows(normed_two, d_pre)
        back_mlp = contract_cols(d_pre, fc1_weight)
        d_norm_two = lax.psum_scatter(
            back_mlp.astype(jnp.bfloat16), TENSOR, scatter_dimension=1, tiled=True
        ).astype(jnp.float32)
        scaled_two = d_norm_two * own_columns(gain_two, share_width)
        sum_plain, sum_cross = group_stats(
            jnp.sum(scaled_two, axis=-1), jnp.sum(scaled_two * unit_two, axis=-1)
        )
        d_residual = own_columns(upstream, share_width) + inv_two * (
            scaled_two
            - sum_plain[:, None] / full_width
            - unit_two * (sum_cross[:, None] / full_width)
        )
        grad_gain_two = grad_gain_two + jnp.sum(d_norm_two * unit_two, axis=0)
        grad_shift_two = grad_shift_two + jnp.sum(d_norm_two, axis=0)
        grad_out_b = grad_out_b + jnp.sum(d_residual, axis=0)
        d_residual_low = lax.all_gather(
            d_residual.astype(jnp.bfloat16), TENSOR, axis=1, tiled=True
        )
        grad_out_w = grad_out_w + contract_rows(mixed, d_residual_low)
        d_mixed_heads = to_heads(contract_cols(d_residual_low, out_weight).astype(jnp.bfloat16))
        probs = jnp.exp(head_scores(query_heads, key_heads) - logsum)
        probs_again = probs.astype(jnp.bfloat16)
        d_value = jnp.einsum(
            "hqk,qhd->khd", probs_again, d_mixed_heads, preferred_element_type=jnp.float32
        )
        d_probs = jnp.einsum(
            "qhd,khd->hqk", d_mixed_heads, value_heads, preferred_element_type=jnp.float32
        )
        inner = jnp.sum(probs * d_probs, axis=-1, keepdims=True)
        d_scores = (probs * (d_probs - inner)).astype(jnp.bfloat16)
        d_query = (
            jnp.einsum("hqk,khd->qhd", d_scores, key_heads, preferred_element_type=jnp.float32)
            * score_scale
        )
        d_key = (
            jnp.einsum("hqk,qhd->khd", d_scores, query_heads, preferred_element_type=jnp.float32)
            * score_scale
        )
        d_stack = (
            jnp.stack([d_query, d_key, d_value], axis=1)
            .reshape(length, 3, local_width)
            .astype(jnp.bfloat16)
        )
        grad_qkv = grad_qkv + jnp.einsum(
            "ld,lje->jde", normed_one, d_stack, preferred_element_type=jnp.float32
        )
        bias_sums = jnp.sum(d_stack.astype(jnp.float32), axis=0)
        grad_qv = grad_qv + jnp.stack([bias_sums[0], bias_sums[2]])
        back_attn = jnp.einsum(
            "lje,jde->ld", d_stack, qkv_weight, preferred_element_type=jnp.float32
        )
        d_norm_one = lax.psum_scatter(
            back_attn.astype(jnp.bfloat16), TENSOR, scatter_dimension=1, tiled=True
        ).astype(jnp.float32)
        own_unit = own_columns(unit_one, share_width)
        scaled_one = d_norm_one * own_columns(gain_one, share_width)
        plain_one, cross_one = group_stats(
            jnp.sum(scaled_one, axis=-1), jnp.sum(scaled_one * own_unit, axis=-1)
        )
        d_input = d_residual + inv_one * (
            scaled_one
            - plain_one[:, None] / full_width
            - own_unit * (cross_one[:, None] / full_width)
        )
        grad_gain_one = grad_gain_one + jnp.sum(d_norm_one * own_unit, axis=0)
        grad_shift_one = grad_shift_one + jnp.sum(d_norm_one, axis=0)
        block_acc = lax.dynamic_update_index_in_dim(block_acc, block_rows, slot_index, 0)
        input_acc = lax.dynamic_update_index_in_dim(input_acc, d_input, slot_index, 0)
        new_grads = (
            grad_gain_one,
            grad_shift_one,
            grad_qkv,
            grad_qv,
            grad_out_w,
            grad_out_b,
            grad_gain_two,
            grad_shift_two,
            grad_fc1_w,
            grad_fc1_b,
            grad_fc2_w,
            grad_fc2_b,
        )
        return (block_acc, input_acc, new_grads)

    share_zeros = jnp.zeros((share_width,), jnp.float32)
    start_grads = (
        share_zeros,
        share_zeros,
        jnp.zeros((3, full_width, local_width), jnp.float32),
        jnp.zeros((2, local_width), jnp.float32),
        jnp.zeros((local_width, full_width), jnp.float32),
        share_zeros,
        share_zeros,
        share_zeros,
        jnp.zeros((full_width, hidden_width), jnp.float32),
        jnp.zeros((hidden_width,), jnp.float32),
        jnp.zeros((hidden_width, full_width), jnp.float32),
        share_zeros,
    )
    start_rows = jnp.zeros((slot_count, length, share_width), jnp.float32)
    block_acc, input_acc, grads = lax.fori_loop(
        0, slot_count, layer_step, (start_rows, start_rows, start_grads)
    )
    (
        grad_gain_one,
        grad_shift_one,
        grad_qkv,
        grad_qv,
        grad_out_w,
        grad_out_b,
        grad_gain_two,
        grad_shift_two,
        grad_fc1_w,
        grad_fc1_b,
        grad_fc2_w,
        grad_fc2_b,
    ) = grads
    summed = (
        lax.psum(grad_gain_one.astype(jnp.bfloat16), DP).astype(jnp.float32),
        lax.psum(grad_shift_one.astype(jnp.bfloat16), DP).astype(jnp.float32),
        lax.psum(grad_qkv.astype(jnp.bfloat16), DP).astype(jnp.float32),
        lax.psum(grad_qv.astype(jnp.bfloat16), DP).astype(jnp.float32),
        lax.psum(grad_out_w.astype(jnp.bfloat16), DP).astype(jnp.float32),
        lax.psum(grad_out_b.astype(jnp.bfloat16), DP).astype(jnp.float32),
        lax.psum(grad_gain_two.astype(jnp.bfloat16), DP).astype(jnp.float32),
        lax.psum(grad_shift_two.astype(jnp.bfloat16), DP).astype(jnp.float32),
        lax.psum(grad_fc1_w.astype(jnp.bfloat16), DP).astype(jnp.float32),
        lax.psum(grad_fc1_b.astype(jnp.bfloat16), DP).astype(jnp.float32),
        lax.psum(grad_fc2_w.astype(jnp.bfloat16), DP).astype(jnp.float32),
        lax.psum(grad_fc2_b.astype(jnp.bfloat16), DP).astype(jnp.float32),
    )
    return (
        block_acc,
        input_acc,
        summed[0],
        summed[1],
        summed[2],
        summed[3],
        summed[4],
        summed[5],
        summed[6],
        summed[7],
        summed[8],
        summed[9],
        summed[10],
        summed[11],
    )


LOG2E = math.log2(math.e)
LN2 = math.log(2.0)
GELU_A = math.sqrt(2.0 / math.pi)
GELU_B = 0.044715
BF = jnp.bfloat16
F32 = jnp.float32
QUERY_BLOCK = 256
BACK_BLOCK = 512
MESH = pl.DeviceIdType.MESH
TENSOR, DP = "tensor", "dp"
X, Y, XY, CORE, LINE = range(5)
TURN = {X: 1, Y: 2, XY: 3}
OTHER = {X: Y, Y: X}
SIDE = {X: 0, Y: 1}
LANES = (X, Y)
FC2, FC1, OUT, QKV = range(4)
INWARD, ACROSS, BACK, SWAP = range(4)


class Bag:
    def __init__(self, **things):
        self.__dict__.update(things)

    def each(self, action):
        return Bag(**{name: action(thing) for name, thing in self.__dict__.items()})
ANYWHERE = pl.BlockSpec(memory_space=pl.ANY)


def dot_nn(left, right):
    return lax.dot_general(left, right, (((1,), (0,)), ((), ())), preferred_element_type=F32)


def place(bit):
    if bit == CORE:
        return {DP: lax.axis_index(DP) ^ 1}
    return {TENSOR: lax.axis_index(TENSOR) ^ TURN[bit]}


def hop(source, target, sems, index, to):
    return pltpu.make_async_remote_copy(
        src_ref=source,
        dst_ref=target,
        send_sem=sems.at[0, index],
        recv_sem=sems.at[1, index],
        device_id=place(to) if isinstance(to, int) else to,
        device_id_type=MESH,
    )


def line_place():
    dp = lax.axis_index(DP)
    return dp // 2, {DP: lax.rem(dp + 2, 8)}, {DP: lax.rem(dp + 6, 8)}


class Program:
    def __init__(self, name, partners):
        self.name = name
        self.partners = partners
        self.arrays, self.specs, self.shapes, self.scratches = [], [], [], []

    def input(self, array, spec=ANYWHERE):
        self.arrays.append(array)
        self.specs.append(spec)
        return (0, len(self.arrays) - 1)

    def output(self, *shape, dtype=BF):
        self.shapes.append(jax.ShapeDtypeStruct(shape, dtype))
        return (1, len(self.shapes) - 1)

    def scratch(self, spec):
        self.scratches.append(spec)
        return (2, len(self.scratches) - 1)

    def tile(self, *shape, dtype=BF):
        return self.scratch(pltpu.VMEM(shape, dtype))

    def sems(self, *shape):
        return self.scratch(pltpu.SemaphoreType.DMA(shape))

    def call(self, script, collective_id, cost):
        count_in, count_out = len(self.arrays), len(self.shapes)

        def kernel(*refs):
            pools = (
                refs[:count_in],
                refs[count_in : count_in + count_out],
                refs[count_in + count_out :],
            )
            meet(self.partners)
            script(lambda handle: pools[handle[0]][handle[1]])

        results = pl.pallas_call(
            kernel,
            in_specs=self.specs,
            out_specs=[ANYWHERE] * count_out,
            out_shape=self.shapes,
            scratch_shapes=self.scratches,
            compiler_params=pltpu.CompilerParams(
                vmem_limit_bytes=67_043_328, collective_id=collective_id, has_side_effects=True
            ),
            cost_estimate=pl.CostEstimate(
                flops=int(cost), bytes_accessed=1 << 26, transcendentals=0
            ),
            name=self.name,
        )(*self.arrays)
        return lambda handle: results[handle[1]]


def meet(partners):
    barrier = pltpu.get_barrier_semaphore()
    signal = lambda at: pl.semaphore_signal(barrier, inc=1, device_id=at, device_id_type=MESH)
    for bit in partners:
        if bit == XY:
            signal({TENSOR: lax.axis_index(TENSOR) ^ 3})
        elif bit != LINE:
            signal(place(bit))
    singles = len([bit for bit in partners if bit != LINE])
    if LINE in partners:
        z, up, down = line_place()
        pl.when(z < 3)(lambda: signal(up))
        pl.when(z > 0)(lambda: signal(down))
        inner = jnp.logical_and(z > 0, z < 3)
        pl.when(inner)(lambda: pl.semaphore_wait(barrier, singles + 2))
        pl.when(jnp.logical_not(inner))(lambda: pl.semaphore_wait(barrier, singles + 1))
    else:
        pl.semaphore_wait(barrier, singles)


def phase(steps, body, ins, in_specs, outs, out_specs, events=()):
    def inner(at, *refs):
        step = at.index[0]
        for when, event in events:
            pl.when(step == when)(event)
        body(step, *refs)

    pltpu.emit_pipeline(
        inner, grid=(steps,), in_specs=in_specs, out_specs=out_specs, _explicit_indices=True
    )(*ins, *outs)


def fetch(source, target, sem):
    copy = pltpu.make_async_copy(source, target, sem)
    copy.start()
    return copy


def spec(shape, index):
    return pl.BlockSpec(shape, index)


class Gather:
    def __init__(self, program, own, shape, early=None):
        _, count, unit, width = shape
        self.own = own
        self.early = early
        self.near = program.output(2, count, unit, width)
        self.near_part = program.output(2, count, unit, width)
        self.far = program.output(count, unit, width)
        self.far_part = program.output(count, unit, width)
        self.sems = program.sems(2, 12)

    def bind(self, ref):
        self.refs = Bag(
            own=ref(self.own),
            near=ref(self.near),
            near_part=ref(self.near_part),
            far=ref(self.far),
            far_part=ref(self.far_part),
            sems=ref(self.sems),
            early=None if self.early is None else ref(self.early),
        )
        return self

    def piece(self, shard, part, lane):
        r = self.refs
        if shard == 0:
            return r.own.at[lax.rem(lax.axis_index(DP) + part, 2), lane]
        if shard == 3:
            return (r.far_part if part else r.far).at[lane]
        if self.early is not None and part == 0 and LANES[lane] == LANES[shard - 1]:
            return r.early.at[lane]
        return (r.near_part if part else r.near).at[shard - 1, lane]

    def _near(self, bit, lane):
        r = self.refs
        k = SIDE[bit]
        own = self.piece(0, 0, lane)
        return hop(own, r.near.at[k, lane], r.sems, 2 * lane + k, bit)

    def _far(self, lane):
        first = LANES[lane]
        source = self.piece(1 + SIDE[first], 0, lane)
        return hop(source, self.refs.far.at[lane], self.refs.sems, 4 + lane, OTHER[first])

    def _swap(self, shard, lane):
        target = self.piece(shard, 1, lane)
        index = 6 + 2 * (shard - 1) + lane
        return hop(self.piece(shard, 0, lane), target, self.refs.sems, index, CORE)

    def start(self):
        for first in (True, False):
            for lane, bit in enumerate(LANES):
                if first and self.early is None:
                    self._near(bit, lane).start()
                if not first:
                    self._near(OTHER[bit], lane).start()

    def forward(self):
        for lane, first in enumerate(LANES):
            if self.early is None:
                self._near(first, lane).wait_recv()
            self._far(lane).start()
            self._swap(1 + SIDE[first], lane).start()

    def near_here(self):
        for lane, first in enumerate(LANES):
            self._near(OTHER[first], lane).wait_recv()
            self._swap(1 + SIDE[OTHER[first]], lane).start()

    def near_whole(self):
        for lane in range(2):
            for shard in (1, 2):
                self._swap(shard, lane).wait_recv()

    def far_here(self):
        for lane in range(2):
            self._far(lane).wait_recv()
            self._swap(3, lane).start()

    def far_whole(self):
        for lane in range(2):
            self._swap(3, lane).wait_recv()

    def drain(self):
        for lane, first in enumerate(LANES):
            if self.early is None:
                self._near(first, lane).wait_send()
            self._near(OTHER[first], lane).wait_send()
            self._far(lane).wait_send()
            for shard in (1, 2, 3):
                self._swap(shard, lane).wait_send()


class Plane:
    def __init__(self, program, shape, share=None):
        _, count, unit, width = shape
        self.unit = unit
        if share is None:
            self.both = program.tile(2, count, 2, unit, width)
            self.got = program.tile(count, 2, unit, width)
            self.last = program.tile(count, unit, width)
        else:
            self.both, self.got, self.last = share.both, share.got, share.last
        self.sems = program.sems(2, 6)
        self.swap_sems = program.sems(2, 8)

    def bind(self, ref):
        self.refs = [ref(h) for h in (self.both, self.got, self.last, self.sems)]
        self.swaps = ref(self.swap_sems)
        return self

    def _part(self, which, *at):
        return self.refs[which].at[*at, pl.ds(0, self.unit)]

    @staticmethod
    def entry(shard, lane):
        odd, high = lax.rem(shard, 2), shard // 2
        return (odd, high) if LANES[lane] == X else (high, odd)

    def tile(self, shard, lane):
        gone, k = self.entry(shard, lane)
        return self._part(0, gone, lane, k)

    def swap(self, source, shard, lane):
        return hop(source, self.tile(shard, lane), self.swaps, 2 * shard + lane, CORE)

    def _first(self, lane, k):
        source = self._part(0, 1, lane, k)
        return hop(source, self._part(1, lane, k), self.refs[3], 2 * lane + k, LANES[lane])

    def _next(self, lane):
        source = self._part(0, 0, lane, 1)
        return hop(
            source, self._part(2, lane), self.refs[3], 4 + lane, OTHER[LANES[lane]]
        )

    def add(self, shard, sums, go):
        for lane in range(2):
            tile = self.tile(shard, lane)
            tile[...] = (sums[lane] + tile[...].astype(F32)).astype(BF)
        if go:
            for lane in range(2):
                gone, k = self.entry(shard, lane)
                pl.when(gone == 1)(lambda lane=lane, k=k: self._first(lane, k).start())

    def launch(self):
        for k in (1, 0):
            for lane in range(2):
                self._first(lane, k).start()

    def _add(self, lane, k):
        self._first(lane, k).wait_recv()
        base = self._part(0, 0, lane, k)
        base[...] = base[...] + self._part(1, lane, k)[...]

    def forward(self):
        for lane in (1, 0):
            self._add(lane, 1)
            self._next(lane).start()

    def settle(self):
        for lane in range(2):
            self._add(lane, 0)

    def finish(self, line):
        for lane in range(2):
            self._next(lane).wait_recv()
            line.take(lane, self._part(0, 0, lane, 0)[...] + self._part(2, lane)[...])

    def drain(self):
        for lane in range(2):
            self._next(lane).wait_send()
            for k in range(2):
                self._first(lane, k).wait_send()


class Line:
    def __init__(self, program, shape, share=None):
        count, unit, width = shape
        self.unit = unit
        self.total = program.output(*shape)
        self.other = program.output(*shape)
        if share is None:
            self.held = program.tile(*shape)
            self.outer = program.tile(*shape)
            self.middle = program.tile(*shape)
        else:
            self.held, self.outer, self.middle = share.held, share.outer, share.middle
        self.sems = program.sems(2, 4 * count)
        self.local = program.sems(count)
        self.count = count

    def bind(self, ref):
        self.refs = Bag(
            total=ref(self.total),
            other=ref(self.other),
            held=ref(self.held).at[:, pl.ds(0, self.unit)],
            outer=ref(self.outer).at[:, pl.ds(0, self.unit)],
            middle=ref(self.middle).at[:, pl.ds(0, self.unit)],
            sems=ref(self.sems),
            local=ref(self.local),
        )
        z, up, down = line_place()
        self.up, self.down = up, down
        self.is_outer = jnp.logical_or(z == 0, z == 3)
        self.is_inner = jnp.logical_not(self.is_outer)
        self.low = z < 2
        return self

    def _hop(self, kind, k, at):
        r = self.refs
        target = (r.outer, r.middle, r.outer, r.other)[kind]
        return hop(r.held.at[k], target.at[k], r.sems, kind * self.count + k, at)

    def _store(self, k):
        r = self.refs
        return pltpu.make_async_copy(r.held.at[k], r.total.at[k], r.local.at[k])

    def _send(self, kind, k):
        if kind == BACK:
            low, high = self.down, self.up
        else:
            low, high = self.up, self.down
        pl.when(self.low)(lambda: self._hop(kind, k, low).start())
        pl.when(jnp.logical_not(self.low))(lambda: self._hop(kind, k, high).start())

    def take(self, k, values):
        self.refs.held[k] = values
        pl.when(self.is_outer)(lambda: self._send(INWARD, k))

    def meet(self, k):
        r = self.refs

        @pl.when(self.is_inner)
        def _():
            self._hop(INWARD, k, self.up).wait_recv()
            r.held[k] += r.outer[k]
            self._send(ACROSS, k)

    def leave(self, k):
        r = self.refs

        @pl.when(self.is_inner)
        def _():
            self._hop(ACROSS, k, self.up).wait()
            r.held[k] += r.middle[k]
            self._send(BACK, k)
            self._hop(SWAP, k, CORE).start()
            self._store(k).start()

    def collect(self, k):
        r = self.refs

        @pl.when(self.is_outer)
        def _():
            self._hop(INWARD, k, self.up).wait_send()
            self._hop(BACK, k, self.up).wait_recv()
            r.held[k] = r.outer[k]
            self._hop(SWAP, k, CORE).start()
            self._store(k).start()

    def done(self, k):
        pl.when(self.is_inner)(lambda: self._hop(BACK, k, self.up).wait_send())
        self._store(k).wait()
        self._hop(SWAP, k, CORE).wait()


class Spread:
    def __init__(self, program, rows, shape):
        self.rows = rows
        self.landed = program.output(3, *shape[1:])
        self.sems = program.sems(2, 3)

    def bind(self, ref):
        self.refs = ref(self.rows), ref(self.landed), ref(self.sems)
        return self

    def _hop(self, r):
        rows, landed, sems = self.refs
        to = lax.axis_index(TENSOR) ^ r
        return hop(rows.at[to], landed.at[r - 1], sems, r - 1, {TENSOR: to})

    def start(self):
        for r in (3, 1, 2):
            self._hop(r).start()

    def finish(self):
        for r in (1, 2, 3):
            self._hop(r).wait()


class Vectors:
    def __init__(self, program, shape):
        self.total = program.output(*shape, dtype=F32)
        self.held = program.tile(*shape, dtype=F32)
        self.got = program.tile(6, *shape, dtype=F32)
        self.sems = program.sems(2, 6)
        self.local = program.sems(1)

    def bind(self, ref):
        self.refs = Bag(
            total=ref(self.total),
            held=ref(self.held),
            got=ref(self.got),
            sems=ref(self.sems),
            local=ref(self.local),
        )
        return self

    def _step(self, k, at):
        r = self.refs
        return hop(r.held, r.got.at[k], r.sems, k, at)

    def plane(self):
        held, got = self.refs.held, self.refs.got
        for k, (bit, turn) in enumerate(((CORE, 1), (X, 2), (Y, 4))):
            self._step(k, bit).start()
            self._step(k, bit).wait()
            held[0:8] += got[k, 0:8]
            for p in range(8):
                held[8 + p] += got[k, 8 + (p ^ turn)]

    def line(self):
        r = self.refs
        held, got = r.held, r.got
        z, up, down = line_place()
        is_outer = jnp.logical_or(z == 0, z == 3)
        low = z < 2

        def towards(k, first, second):
            pl.when(low)(lambda: self._step(k, first).start())
            pl.when(jnp.logical_not(low))(lambda: self._step(k, second).start())

        @pl.when(is_outer)
        def _():
            towards(3, up, down)
            self._step(3, up).wait_send()

        @pl.when(jnp.logical_not(is_outer))
        def _():
            self._step(3, up).wait_recv()
            held[...] += got[3]
            towards(4, up, down)
            self._step(4, up).wait()
            held[...] += got[4]
            towards(5, down, up)

        def last():
            @pl.when(is_outer)
            def _():
                self._step(5, up).wait_recv()
                held[...] = got[5]

            pl.when(jnp.logical_not(is_outer))(lambda: self._step(5, up).wait_send())
            fetch(held, r.total, r.local.at[0]).wait()

        return last


class Stream:
    def __init__(self, program, group, unit, width):
        self.group, self.unit = group, unit
        self.held = program.tile(2, group, 2, unit, width)
        self.sems = program.sems(2, group * 2)

    def bind(self, ref):
        self.refs = ref(self.held), ref(self.sems)
        return self

    def _copies(self, gather, index, slot, size):
        held, sems = self.refs
        return [
            pltpu.make_async_copy(
                gather.piece((index * self.group + g) // 2, (index * self.group + g) % 2, c).at[
                    pl.ds(0, size)
                ],
                held.at[slot, g, c, pl.ds(0, size)],
                sems.at[slot, 2 * g + c],
            )
            for g in range(self.group)
            for c in range(2)
        ]

    def begin(self, gather, index, size=None):
        for each in self._copies(gather, index, index % 2, size or self.unit):
            each.start()

    def here(self, gather, slot):
        for each in self._copies(gather, 0, slot, self.unit):
            each.wait()

    def bring(self, gather, step, first, last, size=None):
        size = size or self.unit
        for index in range(first + 1, last):
            pl.when(step == index - 1 - first)(
                lambda index=index: self.begin(gather, index, size)
            )
        slot = lax.rem(step + first, 2)
        for each in self._copies(gather, 0, slot, size):
            each.wait()
        held = self.refs[0]
        return held[slot, :, :, 0:size].reshape(-1, held.shape[-1])


def prepare_body(
    slot_ref, live_ref, im_ref, go_ref, gain_ref, shift_ref, own_ref, row_ref,
    x_ref, g_ref, n_ref, s_ref, early_ref, bias_ref, sems,
):
    step = pl.program_id(0)
    slot = slot_ref[0]
    hops = [lambda lane=lane: hop(own_ref.at[lax.rem(lax.axis_index(DP), 2), lane], early_ref.at[lane], sems, lane, LANES[lane]) for lane in range(2)]
    for r in range(1, 4):
        to = {TENSOR: lax.axis_index(TENSOR) ^ r}
        hops.append(lambda r=r, to=to: hop(row_ref, bias_ref.at[r - 1], sems, 1 + r, to))

    @pl.when(step == 0)
    def _():
        meet((X, Y, XY))
        for each in hops[2:] + hops[:2]:
            each().start()

    def pick(ref):
        values = ref[...].astype(F32)
        chosen = values[:, 0]
        for index in range(1, values.shape[1]):
            chosen = jnp.where(slot == index, values[:, index], chosen)
        return chosen

    picture = pick(im_ref)
    centered = picture - row_mean(picture)
    inverse = lax.rsqrt(row_mean(centered * centered) + EPS)
    normed = centered * inverse * gain_ref[...] + shift_ref[...]
    x_ref[...] = picture.T.astype(BF)
    g_ref[...] = (pick(go_ref) * live_ref[0].astype(F32)).T.astype(BF)
    n_ref[...] = normed.T.astype(BF)
    s_ref[0:1, :] = row_mean(picture).T
    s_ref[1:2, :] = inverse.T

    @pl.when(step == pl.num_programs(0) - 1)
    def _():
        for each in hops:
            each().wait()


def prepare(images, grad_out, slot, live, gain, shift, own, bias):
    slots, length, width = images.shape
    rows = 128
    scalar = pl.BlockSpec(memory_space=pltpu.SMEM)
    tokens = pl.BlockSpec((rows, slots, width), lambda i: (i, 0, 0))
    vector = pl.BlockSpec((1, width), lambda i: (0, 0))
    return pl.pallas_call(
        prepare_body,
        grid=(pl.cdiv(length, rows),),
        in_specs=[scalar, scalar, tokens, tokens, vector, vector, ANYWHERE, ANYWHERE],
        out_specs=[pl.BlockSpec((width, rows), lambda i: (0, i))] * 3
        + [pl.BlockSpec((2, rows), lambda i: (0, i)), ANYWHERE, ANYWHERE],
        out_shape=[jax.ShapeDtypeStruct((width, length), BF)] * 3
        + [
            jax.ShapeDtypeStruct((2, length), F32),
            jax.ShapeDtypeStruct(own.shape[1:], BF),
            jax.ShapeDtypeStruct((3, *bias.shape), F32),
        ],
        scratch_shapes=[pltpu.SemaphoreType.DMA((2, 5))],
        compiler_params=pltpu.CompilerParams(
            vmem_limit_bytes=67_043_328, collective_id=1, has_side_effects=True
        ),
        name="prepare",
    )(slot, live, images.transpose(1, 0, 2), grad_out.transpose(1, 0, 2), gain, shift, own, bias)


def as_column(row):
    return jnp.broadcast_to(row, (8, row.shape[1])).T[:, 0:1]


def as_row(column):
    return jnp.broadcast_to(column, (column.shape[0], 8)).T[0:1, :]


def attend_head(weight, normed, bias, qkv_ref, o_ref, lse_ref):
    length = normed.shape[1]
    rows = dot_nn(weight, normed)
    queries = ((rows[:HD] + bias[0]) * (LOG2E / math.sqrt(HD))).astype(BF)
    keys_t = rows[HD : 2 * HD].astype(BF)
    values = (rows[2 * HD :] + bias[1]).astype(BF)
    qkv_ref[0, 0] = queries
    qkv_ref[0, 1] = keys_t
    qkv_ref[0, 2] = values
    keys = keys_t.T
    for start in range(0, length, QUERY_BLOCK):
        block = slice(start, min(start + QUERY_BLOCK, length))
        scores = dot_nn(keys, queries[:, block])
        top = jnp.max(scores, axis=0, keepdims=True)
        weights = jnp.exp2(scores - top)
        total = jnp.sum(weights, axis=0, keepdims=True)
        mixed = dot_nn(values, weights.astype(BF))
        o_ref[0, :, block] = (mixed * (1.0 / total)).astype(BF)
        lse_ref[0, :, block] = top + jnp.log2(total)


def attend_back_head(qkv_ref, do_ref, o_ref, lse_ref, d_ref, dk_acc, dv_acc):
    keys_t = qkv_ref[0, 1]
    keys = keys_t.T
    values = qkv_ref[0, 2].T
    length = keys_t.shape[1]
    scale = 1.0 / math.sqrt(HD)
    for start in range(0, length, BACK_BLOCK):
        block = slice(start, min(start + BACK_BLOCK, length))
        queries_t = qkv_ref[0, 0, :, block]
        pull_t = do_ref[0, :, block]
        delta = jnp.sum(
            pull_t.astype(F32) * o_ref[0, :, block].astype(F32), axis=0, keepdims=True
        )
        probs = jnp.exp2(dot_nn(keys, queries_t) - lse_ref[0, :, block])
        probs_low = probs.astype(BF)
        d_probs = dot_nn(values, pull_t)
        d_scores = (probs * (d_probs - delta)).astype(BF)
        d_ref[0, 0, :, block] = (dot_nn(keys_t, d_scores) * scale).astype(BF)
        d_keys = dot_nn(d_scores, queries_t.T)
        d_values = dot_nn(probs_low, pull_t.T)
        if start == 0:
            dk_acc[...] = d_keys
            dv_acc[...] = d_values
        else:
            dk_acc[...] += d_keys
            dv_acc[...] += d_values
    d_ref[0, 1] = (dk_acc[...].T * LN2).astype(BF)
    d_ref[0, 2] = dv_acc[...].T.astype(BF)
    return [jnp.sum(d_ref[0, k].astype(F32), axis=1, keepdims=True) for k in (0, 2)]


def columns_of(length, block=128):
    return [slice(start, min(start + block, length)) for start in range(0, length, block)]


def norm_back(grad, unit_values, inverse, gain):
    scaled = grad * gain
    mean = lambda values: jnp.mean(values, axis=0, keepdims=True)
    return inverse * (scaled - mean(scaled) - unit_values * mean(scaled * unit_values))


def turned(values, axis, bit):
    return jnp.where(bit == 1, lax.rev(values, (axis,)), values)


def forward(attn_own, early, fc1_own, fc2_own, bias, bias_far, picture, normed_one, vectors):
    width, length = picture.shape
    chunk = attn_own.shape[2]
    unit = fc1_own.shape[2]
    rows = 2 * unit
    heads = 16
    p = Program("forward", (X, Y, CORE))
    own, soon, own_fc1 = p.input(attn_own), p.input(early), p.input(fc1_own)
    bias_in, x_in, n_in, v_in = p.input(bias), p.input(picture), p.input(normed_one), p.input(vectors)
    bias_far_in = p.input(bias_far)
    attn = Gather(p, own, attn_own.shape, soon)
    fc1 = Gather(p, own_fc1, fc1_own.shape)
    own_fc2, soon_fc2 = p.input(fc2_own), p.output(*fc2_own.shape[1:])
    soon_sems = p.sems(2, 2)
    stream = Stream(p, 1, unit, width)
    qkv, mixed = p.output(heads, 3, HD, length), p.output(heads, HD, length)
    lse = p.output(heads, 1, length, dtype=F32)
    residual, normed = p.output(3, width, 256, dtype=F32), p.output(width, length)
    stats, out_all = p.output(2, length, dtype=F32), p.output(heads, HD, width)
    act, slope = p.output(8, rows, length), p.output(8, rows, length)
    held = Bag(
        bias=p.tile(4, *bias.shape, dtype=F32),
        x=p.tile(width, length),
        n=p.tile(width, length),
        v=p.tile(*vectors.shape, dtype=F32),
        o=p.tile(heads, HD, length),
        w=p.tile(heads, HD, width),
        h=p.tile(3, width, 256, dtype=F32),
        n2=p.tile(width, length),
        s=p.tile(2, length, dtype=F32),
        rows=p.tile(2, 3 * HD, width),
    )
    sems, wsems, hsems = p.sems(8), p.sems(heads), p.sems(2)

    def script(ref):
        hold = held.each(ref)
        sem, wsem, hsem = ref(sems), ref(wsems), ref(hsems)
        attn.bind(ref)
        fc1.bind(ref)
        stream.bind(ref)
        attn.start()
        attn.forward()
        fc1.start()
        copies = [
            fetch(ref(n_in), hold.n, sem.at[0]),
            fetch(ref(bias_in), hold.bias.at[0], sem.at[1]),
            fetch(ref(bias_far_in), hold.bias.at[pl.ds(1, 3)], sem.at[2]),
            fetch(ref(x_in), hold.x, sem.at[5]),
            fetch(ref(v_in), hold.v, sem.at[6]),
        ]
        for each in copies[:3]:
            each.wait()

        def weights_in(head, slot):
            shard, half, lane = head // 4, (head // 2) % 2, head % 2
            return pltpu.make_async_copy(
                attn.piece(shard, half, lane).at[pl.ds(0, 3 * HD)], hold.rows.at[slot], hsem.at[slot]
            )

        def near_all():
            attn.near_here()
            attn.near_whole()

        def far_all():
            attn.far_here()
            attn.far_whole()

        def head(step, qkv_ref, o_ref, lse_ref):
            pl.when(step == 3)(near_all)
            pl.when(step == 11)(far_all)
            slot = lax.rem(step, 2)
            for each in range(1, heads):
                pl.when(step == each - 1)(
                    lambda each=each: weights_in(each, each % 2).start()
                )
            weights_in(0, slot).wait()
            shard, half, lane = step // 4, lax.rem(step // 2, 2), lax.rem(step, 2)
            at = 4 * half + 2 * lane
            shift = [as_column(hold.bias[shard, at + k, :, 0:HD]) for k in range(2)]
            attend_head(hold.rows[slot], hold.n[...], shift, qkv_ref, o_ref, lse_ref)
            hold.o[step] = o_ref[0]

        def bring_out(shard):
            return [
                pltpu.make_async_copy(
                    attn.piece(shard, half, lane).at[pl.ds(3 * HD, HD)],
                    hold.w.at[4 * shard + 2 * half + lane],
                    wsem.at[4 * shard + 2 * half + lane],
                )
                for half in range(2)
                for lane in range(2)
            ]

        weights_in(0, 0).start()
        phase(
            heads,
            head,
            [],
            [],
            [ref(qkv), ref(mixed), ref(lse)],
            [
                spec((1, 3, HD, length), lambda i: (i, 0, 0, 0)),
                spec((1, HD, length), lambda i: (i, 0, 0)),
                spec((1, 1, length), lambda i: (i, 0, 0)),
            ],
        )
        for shard in range(4):
            for each in bring_out(shard):
                each.start()
        fc1.forward()
        core = lax.rem(lax.axis_index(DP), 2)
        ahead = lambda lane: hop(
            ref(own_fc2).at[core, lane], ref(soon_fc2).at[lane], ref(soon_sems), lane, LANES[lane]
        )
        for lane in range(2):
            ahead(lane).start()
        for each in copies[3:]:
            each.wait()
        for shard in range(4):
            for each in bring_out(shard):
                each.wait()
        stream.begin(fc1, 0)
        store_w = fetch(hold.w, ref(out_all), sem.at[4])
        weight = hold.w[...].reshape(width, width)
        for block in columns_of(length, 256):
            mix = hold.o[:, :, block].reshape(width, -1)
            values = hold.x[:, block].astype(F32) + contract_rows(weight, mix)
            values = values + hold.v[:, 2:3]
            average = jnp.mean(values, axis=0, keepdims=True)
            centered = values - average
            inverse = lax.rsqrt(jnp.mean(centered * centered, axis=0, keepdims=True) + EPS)
            hold.h[block.start // 256, :, 0 : block.stop - block.start] = values
            hold.n2[:, block] = (
                centered * inverse * hold.v[:, 3:4] + hold.v[:, 4:5]
            ).astype(BF)
            hold.s[0:1, block] = average
            hold.s[1:2, block] = inverse
        stores = [store_w] + [
            fetch(source, ref(target), sem.at[k])
            for k, (source, target) in enumerate(((hold.h, residual), (hold.n2, normed), (hold.s, stats)))
        ]

        def hidden(step, act_ref, slope_ref):
            weight = stream.bring(fc1, step, 0, 8)
            shard, half = step // 2, lax.rem(step, 2)
            shift = as_column(hold.bias[shard, half, :, 128 : 128 + rows])
            preact = dot_nn(weight, hold.n2[...]) + shift
            square = preact * preact
            curve = jnp.tanh(preact * (GELU_A + (GELU_A * GELU_B) * square))
            rise = 0.5 * (1.0 + curve)
            act_ref[0] = (preact * rise).astype(BF)
            inner = GELU_A + (3.0 * GELU_A * GELU_B) * square
            slope_ref[0] = (rise + (0.5 * preact) * (1.0 - curve * curve) * inner).astype(BF)

        block = spec((1, rows, length), lambda i: (i, 0, 0))

        def fc1_near():
            fc1.near_here()
            fc1.near_whole()

        def fc1_far():
            fc1.far_here()
            fc1.far_whole()

        phase(
            8, hidden, [], [], [ref(act), ref(slope)], [block, block],
            [(1, fc1_near), (5, fc1_far)],
        )
        for each in stores:
            each.wait()
        attn.drain()
        fc1.drain()
        for lane in range(2):
            ahead(lane).wait()

    result = p.call(script, 2, 3e10)
    return (
        gathered(attn).each(result),
        gathered(fc1).each(result),
        Bag(
            qkv=qkv,
            mixed=mixed,
            lse=lse,
            residual=residual,
            normed_two=normed,
            stats_two=stats,
            out_all=out_all,
            act=act,
            slope=slope,
        ).each(result),
        result(soon_fc2),
    )


def gathered(source):
    return Bag(
        near=source.near, near_part=source.near_part, far=source.far, far_part=source.far_part
    )


class Ready:
    def __init__(self, program, own, parts, early=None):
        self.handles = parts.each(program.input)
        self.handles.own = program.input(own)
        self.handles.early = None if early is None else program.input(early)
        self.early = early

    def bind(self, ref):
        self.refs = self.handles.each(lambda h: None if h is None else ref(h))
        return self

    piece = Gather.piece


def backward(arrays, fc1_parts, attn_parts, owns, early, fc2_early, live):
    width, length = arrays.picture.shape
    share = width // 4
    unit = owns.fc2.shape[2]
    rows = 2 * unit
    block = 3 * HD
    p = Program("backward", (X, Y, XY, CORE, LINE))
    into = arrays.each(p.input)
    live_in = p.input(live, pl.BlockSpec(memory_space=pltpu.SMEM))
    fc1 = Ready(p, owns.fc1, fc1_parts)
    attn = Ready(p, owns.attn, attn_parts, early)
    fc2 = Gather(p, p.input(owns.fc2), owns.fc2.shape, p.input(fc2_early))
    stream = Stream(p, 2, unit, width)

    fc_shape, out_shape, qkv_shape = ((4, 2, u, width) for u in (unit, HD, block))
    shapes = (fc_shape, fc_shape, out_shape, qkv_shape)
    plane = [Plane(p, shape) for shape in shapes[:QKV]]
    plane.append(Plane(p, shapes[QKV], plane[FC2]))
    line = [Line(p, shape[1:]) for shape in shapes[:QKV]]
    line.append(Line(p, shapes[QKV][1:], line[FC2]))
    d_pre = p.output(8, rows, length)
    pull = p.output(16, HD, length)
    d_qkv = p.output(16, 3, HD, length)
    block_rows, input_rows = p.output(4, share, length), p.output(4, share, length)
    spread_block = Spread(p, block_rows, (4, share, length))
    spread_input = Spread(p, input_rows, (4, share, length))
    vectors = Vectors(p, (16, 1, width))
    held = Bag(
        upstream=p.tile(width, length),
        normed_two=p.tile(width, length),
        normed_one=p.tile(width, length),
        low=p.tile(width, length),
        residual=p.tile(width, 256, dtype=F32),
        acc=p.tile(width, length, dtype=F32),
        vectors=p.tile(*arrays.vectors.shape, dtype=F32),
        stats_two=p.tile(2, length, dtype=F32),
        stats_one=p.tile(2, length, dtype=F32),
        rows=p.tile(2, rows, length),
        heads=p.tile(3, 2, 3, HD, length),
        part=p.tile(2, 2, unit, width),
    )
    tile_sems = p.sems(2)
    sems = p.sems(12)

    def script(ref):
        hold = held.each(ref)
        sem = ref(sems)
        for each in (fc1, attn, fc2, stream, spread_block, spread_input, vectors):
            each.bind(ref)
        for group in (plane, line):
            for each in group:
                each.bind(ref)
        vec = vectors.refs.held
        array = into.each(ref)
        live_now = ref(live_in)[0].astype(F32)

        copies = Bag(
            upstream=fetch(array.upstream, hold.upstream, sem.at[0]),
            normed_two=fetch(array.normed_two, hold.normed_two, sem.at[1]),
            vectors=fetch(array.vectors, hold.vectors, sem.at[3]),
            stats_two=fetch(array.stats_two, hold.stats_two, sem.at[4]),
            normed_one=fetch(array.normed_one, hold.normed_one, sem.at[5]),
            stats_one=fetch(array.stats_one, hold.stats_one, sem.at[6]),
        )
        fc2.start()
        fc2.forward()
        stream.begin(fc2, 0)
        vec[...] = jnp.zeros(vec.shape, F32)
        copies.upstream.wait()
        copies.normed_two.wait()

        tile_sem = ref(tile_sems)

        def rows_in(source, index, slot):
            if len(source.shape) == 3 and source.shape[0] == 8:
                target = hold.rows.at[slot]
                source = source.at[index]
            else:
                target = hold.heads.at[slot, :, 0]
                source = source.at[pl.ds(2 * index, 2)]
            return pltpu.make_async_copy(source, target, tile_sem.at[slot])

        def rows_of(source, slot, count):
            if len(source.shape) == 3 and source.shape[0] == 8:
                return hold.rows[slot]
            return hold.heads[slot, :, 0].reshape(count, length)

        def gradient(source, other, name, shards, go=True):
            _, _, size, _ = shapes[name]
            count = 2 * size
            total = len(shards)

            def pick(i):
                if total == 1:
                    return shards[0]
                if total == 2:
                    return jnp.where(i == 0, shards[0], shards[1])
                return jnp.where(
                    i < 2,
                    jnp.where(i == 0, shards[0], shards[1]),
                    jnp.where(i == 2, shards[2], shards[3]),
                )

            part_of = lambda slot, lane: hold.part.at[slot, lane, pl.ds(0, size)]
            sums_of = plane[name]
            piece = lambda k: jnp.where(
                k < total, 2 * pick(k) + 1, 2 * pick(jnp.maximum(k - total, 0))
            )
            rows_in(source, 2 * shards[0] + 1, 0).start()

            def product(k):
                slot = lax.rem(k, 2)

                @pl.when(k + 1 < 2 * total)
                def _():
                    rows_in(source, piece(k + 1), 1 - slot).start()

                rows_in(source, 0, slot).wait()
                return contract_cols(rows_of(source, slot, count), other[...])

            def give(i, _):
                slot = lax.rem(i, 2)
                shard = pick(i)

                @pl.when(i >= 2)
                def _():
                    for lane in range(2):
                        before = pick(jnp.maximum(i - 2, 0))
                        sums_of.swap(part_of(slot, lane), before, lane).wait_send()

                sums = product(i).astype(BF).reshape(2, size, width)
                for lane in range(2):
                    part_of(slot, lane)[...] = sums[lane]
                for lane in range(2):
                    sums_of.swap(part_of(slot, lane), shard, lane).start()
                return 0

            def keep(i, _):
                shard = pick(i)
                for lane in range(2):
                    sums_of.swap(part_of(0, lane), shard, lane).wait_recv()
                sums_of.add(shard, product(total + i).reshape(2, size, width), go)
                return 0

            lax.fori_loop(0, total, give, 0)
            lax.fori_loop(0, total, keep, 0)
            for i in range(max(total - 2, 0), total):
                for lane in range(2):
                    sums_of.swap(
                        part_of(i % 2, lane), jnp.int32(shards[i]), lane
                    ).wait_send()

        every = (3, 1, 2, 0)
        gradient(array.act, hold.upstream, FC2, every, False)

        def hidden(step, slope_ref, d_ref):
            slot = lax.rem(step, 2)
            stream.here(fc2, slot)
            pl.when(step == 1)(lambda: stream.begin(fc2, 2))
            for half in range(2):
                weight = stream.refs[0][slot, half].reshape(rows, width)
                values = dot_nn(weight, hold.upstream[...])
                values = (values * slope_ref[half].astype(F32)).astype(BF)
                d_ref[half] = values
                sums = jnp.sum(values.astype(F32), axis=1, keepdims=True)
                vec[8 + 2 * step + half, :, 0:rows] = as_row(sums)

            @pl.when(step == 0)
            def _():
                fc2.near_here()
                fc2.near_whole()
                stream.begin(fc2, 1)

            @pl.when(step == 2)
            def _():
                fc2.far_here()
                fc2.far_whole()
                stream.begin(fc2, 3)

        plane[FC2].launch()
        pair = spec((2, rows, length), lambda i: (i, 0, 0))
        phase(4, hidden, [array.slope], [pair], [ref(d_pre)], [pair])

        def back(weights, values, lead, size, events=()):
            def body(step, d_ref):
                weight = stream.bring(weights, step, 0, 4, size)
                values = d_ref[...].reshape(4 * size, length)
                hold.acc[...] += contract_rows(weight, values)

            hold.acc[...] = jnp.zeros(hold.acc.shape, F32)
            tail = values.shape[1:]
            zeros = (0,) * len(tail)
            phase(4, body, [values], [spec((lead, *tail), lambda i: (i, *zeros))], [], [], events)

        stream.begin(fc1, 0)
        back(fc1, ref(d_pre), 2, unit)
        for each in (copies.vectors, copies.stats_two):
            each.wait()
        total = lambda values: jnp.sum(values, axis=1, keepdims=True)
        residual_of = parts_of(array.residual, hold.residual, sem.at[2])
        for cut in columns_of(length):
            inverse = hold.stats_two[1:2, cut]
            grad = hold.acc[:, cut]
            units = (residual_of(cut) - hold.stats_two[0:1, cut]) * inverse
            up = hold.upstream[:, cut].astype(F32)
            d_residual = up + norm_back(grad, units, inverse, hold.vectors[:, 3:4])
            hold.low[:, cut] = d_residual.astype(BF)
            hold.vectors[:, 10:11] += total(d_residual)
            hold.vectors[:, 11:12] += total(grad * units)
            hold.vectors[:, 12:13] += total(grad)
            hold.vectors[:, 13:14] += total(up)

        plane[FC2].forward()
        plane[FC2].settle()
        picture_copy = fetch(array.picture, hold.upstream, sem.at[7])

        def pull_body(step, w_ref, o_ref):
            weight = w_ref[...].reshape(4 * HD, width)
            o_ref[...] = dot_nn(weight, hold.low[...]).reshape(4, HD, length).astype(BF)

        quarter = lambda *tail: spec((4, *tail), lambda i: (i, *(0 for _ in tail)))
        phase(
            4, pull_body, [array.out_all], [quarter(HD, width)], [ref(pull)], [quarter(HD, length)]
        )
        gradient(ref(d_pre), hold.normed_two, FC1, every)
        plane[FC2].finish(line[FC2])
        plane[FC2].drain()
        gradient(array.mixed, hold.low, OUT, every)
        copies.normed_one.wait()

        def settle(name):
            plane[name].forward()
            plane[name].settle()

        events = [
            (1, 0, lambda: line[FC2].meet(0)),
            (2, 0, lambda: line[FC2].meet(1)),
            (2, 0, lambda: line[FC2].leave(0)),
            (1, 2, lambda: settle(FC1)),
            (2, 2, lambda: settle(OUT)),
            (3, 0, lambda: plane[FC1].finish(line[FC1])),
            (3, 0, lambda: line[FC2].leave(1)),
            (3, 1, lambda: line[FC2].collect(0)),
        ]
        part_of = lambda lane: hold.part.at[0, lane, pl.ds(0, block)]
        sums_of = plane[QKV]

        def qkv_rows(slot):
            values = hold.heads[slot].reshape(2 * block, length)
            return contract_cols(values, hold.normed_one[...]).reshape(2, block, width)

        def keep_rows(shard, slot):
            for lane in range(2):
                sums_of.swap(part_of(lane), shard, lane).wait()
            sums_of.add(shard, qkv_rows(slot), True)

        order = lambda g: jnp.where(
            g < 2, jnp.where(g == 0, every[0], every[1]), jnp.where(g == 2, every[2], every[3])
        )

        dk_acc = hold.acc.at[pl.ds(0, length), pl.ds(0, HD)]
        dv_acc = hold.acc.at[pl.ds(0, length), pl.ds(128, HD)]

        def shard_back(g, _):
            shard = order(g)
            at = lambda i: 4 * shard + i

            def body(step, qkv_ref, do_ref, o_ref, lse_ref, d_ref):
                for when, now, event in events:
                    pl.when(jnp.logical_and(g == when, step == now))(event)
                sums = attend_back_head(
                    qkv_ref, do_ref, o_ref, lse_ref, d_ref, dk_acc, dv_acc
                )
                half, lane = step // 2, lax.rem(step, 2)
                hold.heads[jnp.where(half == 1, 0, 1 + lax.rem(g, 2)), lane] = d_ref[0]
                for k in range(2):
                    where = pl.multiple_of(640 + 128 * (2 * lane + k), 128)
                    padded = jnp.concatenate(
                        [as_row(sums[k]), jnp.zeros((1, 128 - HD), F32)], axis=1
                    )
                    vec[8 + 2 * shard + half, :, pl.ds(where, 128)] = padded

            flat = spec((1, HD, length), lambda i: (at(i), 0, 0))
            many = spec((1, 3, HD, length), lambda i: (at(i), 0, 0, 0))
            phase(
                4,
                body,
                [array.qkv, ref(pull), array.mixed, array.lse],
                [many, flat, flat, spec((1, 1, length), lambda i: (at(i), 0, 0))],
                [ref(d_qkv)],
                [many],
            )
            pl.when(g > 0)(lambda: keep_rows(order(g - 1), 1 + lax.rem(g + 1, 2)))
            sums = qkv_rows(0).astype(BF)
            for lane in range(2):
                part_of(lane)[...] = sums[lane]
            for lane in range(2):
                sums_of.swap(part_of(lane), shard, lane).start()
            return 0

        lax.fori_loop(0, 4, shard_back, 0)
        plane[OUT].finish(line[OUT])
        stream.begin(fc2, 0)
        keep_rows(jnp.int32(every[3]), 2)
        plane[QKV].forward()
        line[FC1].meet(0)
        back(
            fc2,
            array.act,
            2,
            unit,
            [
                (1, lambda: line[FC2].collect(1)),
                (2, plane[QKV].settle),
                (3, lambda: line[FC1].meet(1)),
            ],
        )
        line[FC1].leave(0)
        stream.begin(attn, 0, block)
        residual_of = parts_of(array.residual, hold.residual, sem.at[2])
        for cut in columns_of(length):
            values = residual_of(cut) + hold.acc[:, cut] + hold.vectors[:, 5:6]
            hold.normed_two[:, cut] = (values * live_now).astype(BF)
        store_rows(hold.normed_two, ref(block_rows), sem, share)
        for k in range(2):
            line[FC2].done(k)
        plane[QKV].finish(line[QKV])
        spread_block.start()
        line[OUT].meet(0)
        line[OUT].meet(1)
        picture_copy.wait()
        copies.stats_one.wait()
        back(
            attn,
            ref(d_qkv),
            4,
            block,
            [(2, lambda: line[FC1].leave(1)), (3, lambda: line[QKV].meet(0))],
        )
        line[OUT].leave(0)
        line[OUT].leave(1)
        for cut in columns_of(length):
            inverse = hold.stats_one[1:2, cut]
            grad = hold.acc[:, cut]
            units = hold.upstream[:, cut].astype(F32) - hold.stats_one[0:1, cut]
            units = units * inverse
            d_input = hold.low[:, cut].astype(F32) + norm_back(
                grad, units, inverse, hold.vectors[:, 0:1]
            )
            hold.normed_two[:, cut] = d_input.astype(BF)
            hold.vectors[:, 8:9] += total(grad * units)
            hold.vectors[:, 9:10] += total(grad)
        line[QKV].meet(1)
        line[QKV].leave(0)
        wide = hold.vectors[:, 8:16].T
        for k in range(8):
            vec[k] = wide[k : k + 1]
        stores = start_rows(hold.normed_two, ref(input_rows), sem, share)
        vectors.plane()
        for each in stores:
            each.wait()
        spread_input.start()
        line[QKV].leave(1)
        last = vectors.line()
        for each in (line[FC1], line[OUT], line[QKV]):
            for k in range(2):
                each.collect(k)
        last()
        spread_block.finish()
        spread_input.finish()
        for each in line[1:]:
            for k in range(2):
                each.done(k)
        for each in plane[1:]:
            each.drain()
        fc2.drain()

    result = p.call(script, 3, 8e10)
    sums = [(result(each.total), result(each.other)) for each in line]
    spreads = [
        (result(block_rows), result(spread_block.landed)),
        (result(input_rows), result(spread_input.landed)),
    ]
    return sums, spreads, result(vectors.total)[:, 0]


def parts_of(source, held, sem):
    width = held.shape[1]

    def bring(part):
        return fetch(source.at[part], held, sem)

    bring(0).wait()

    def columns(cut):
        if cut.start > 0 and cut.start % width == 0:
            bring(cut.start // width).wait()
        first = cut.start % width
        return held[:, first : first + cut.stop - cut.start]

    return columns


def start_rows(source, target, sem, share):
    return [fetch(source.at[pl.ds(k * share, share)], target.at[k], sem.at[k]) for k in range(4)]


def store_rows(source, target, sem, share):
    for each in start_rows(source, target, sem, share):
        each.wait()


def finish(sums, spreads, place_t, core, hidden):
    width = sums[FC2][0].shape[-1]
    share, length = spreads[0][0].shape[1:]

    def body(at, *refs):
        step = pl.program_id(0)
        same = lax.rem(step // 2 + at[1], 2) == 0
        ins, outs = refs[:12], refs[12:]
        for k in range(4):
            rows = jnp.where(same, ins[2 * k][0], ins[2 * k + 1][0]).astype(F32)
            outs[k][...] = rows.reshape(outs[k].shape)
        for k in range(2):
            rows = jnp.where(step == at[0], ins[8 + 2 * k][0], ins[9 + 2 * k][0])
            outs[4 + k][0] = rows.astype(F32)

    half = lambda array: pl.BlockSpec((1, *array.shape[1:]), lambda i, at: (lax.rem(i, 2), 0, 0))
    own = pl.BlockSpec((1, share, length), lambda i, at: (at[0], 0, 0))
    landed = pl.BlockSpec(
        (1, share, length), lambda i, at: (jnp.maximum((i ^ at[0]) - 1, 0), 0, 0)
    )
    units = [pair[0].shape[1] for pair in sums]
    rows = lambda unit: pl.BlockSpec((unit, width), lambda i, at: (i, 0))
    slot = pl.BlockSpec((1, share, length), lambda i, at: (i, 0, 0))
    shape = lambda *dims: jax.ShapeDtypeStruct(dims, F32)
    return pl.pallas_call(
        body,
        grid_spec=pltpu.PrefetchScalarGridSpec(
            num_scalar_prefetch=1,
            grid=(4,),
            in_specs=[half(array) for pair in sums for array in pair] + [own, landed] * 2,
            out_specs=[
                rows(units[FC2]),
                rows(units[FC1]),
                rows(units[OUT]),
                pl.BlockSpec((3, HD, width), lambda i, at: (0, i, 0)),
                slot,
                slot,
            ],
        ),
        out_shape=[
            shape(hidden, width),
            shape(hidden, width),
            shape(share, width),
            shape(3, share, width),
            shape(4, share, length),
            shape(4, share, length),
        ],
        compiler_params=pltpu.CompilerParams(vmem_limit_bytes=67_043_328),
        name="finish",
    )(
        jnp.stack([place_t, core]).astype(jnp.int32),
        *[array for pair in sums for array in pair],
        *spreads[0],
        *spreads[1],
    )


def whole_image(
    images,
    counts,
    ln1_gain,
    ln1_bias,
    qkv_weight,
    qv_bias,
    out_weight,
    out_bias,
    ln2_gain,
    ln2_bias,
    fc1_weight,
    fc1_bias,
    fc2_weight,
    fc2_bias,
    grad_out,
):
    slot_count, length, width = images.shape
    share = width // 4
    hidden = fc1_weight.shape[1]
    unit = -(-hidden // 64) * 16
    rows = 2 * unit
    place_t = lax.axis_index(TENSOR)
    core = lax.rem(lax.axis_index(DP), 2)
    block = 3 * HD

    qkv_rows = qkv_weight.reshape(3, width, 2, 2, HD).transpose(2, 3, 0, 4, 1)
    attn_own = jnp.concatenate(
        [qkv_rows.reshape(2, 2, block, width), out_weight.reshape(2, 2, HD, width)], axis=2
    )
    pad = 2 * rows - hidden
    fc1_own, fc2_own = (
        jnp.pad(each, ((0, pad), (0, 0))).reshape(2, 2, unit, width)
        for each in (fc1_weight.T, fc2_weight)
    )
    head_bias = qv_bias.reshape(2, 2, 2, HD).transpose(1, 2, 0, 3)
    head_bias = jnp.pad(turned(head_bias, 0, core).reshape(8, HD), ((0, 0), (0, 128 - HD)))
    hidden_bias = turned(jnp.pad(fc1_bias, (0, pad)).reshape(2, rows), 0, core)
    hidden_bias = jnp.pad(hidden_bias, ((0, 6), (0, 640 - rows)))
    bias = jnp.concatenate([head_bias, hidden_bias], axis=1).astype(F32)[:, None]
    vectors = jnp.stack(
        [ln1_gain, ln1_bias, out_bias, ln2_gain, ln2_bias, fc2_bias, fc2_bias, fc2_bias], axis=1
    )
    vectors = jnp.pad(vectors, ((0, 0), (0, 8))).astype(F32)
    live = (place_t < counts[0]).astype(jnp.int32)[None]

    picture, upstream, normed_one, stats_one, early, bias_far = prepare(
        images,
        grad_out,
        place_t[None].astype(jnp.int32),
        live,
        ln1_gain.astype(F32)[None],
        ln1_bias.astype(F32)[None],
        attn_own,
        bias,
    )
    attn_parts, fc1_parts, made, fc2_early = forward(
        attn_own, early, fc1_own, fc2_own, bias, bias_far, picture, normed_one, vectors
    )
    made.__dict__.update(
        upstream=upstream,
        picture=picture,
        normed_one=normed_one,
        stats_one=stats_one,
        vectors=vectors,
    )
    owns = Bag(attn=attn_own, fc1=fc1_own, fc2=fc2_own)
    sums, spreads, totals = backward(
        made, fc1_parts, attn_parts, owns, early, fc2_early, live
    )

    own_wide = lax.dynamic_slice_in_dim(totals[:6], place_t * share, share, 1)
    own_rows = turned(totals[8:10], 0, core)
    own_hidden = own_rows[:, :rows].reshape(-1)[:hidden]
    own_qv = own_rows[:, 640:].reshape(2, 2, 2, 128)[..., :HD].transpose(2, 0, 1, 3)
    own_qv = own_qv.reshape(2, share)

    fc2_result, fc1_result, out_result, qkv_result, block_result, input_result = finish(
        sums, spreads, place_t, core, hidden
    )
    return (
        block_result.transpose(0, 2, 1),
        input_result.transpose(0, 2, 1),
        own_wide[0],
        own_wide[1],
        qkv_result.transpose(0, 2, 1),
        own_qv,
        out_result,
        own_wide[2],
        own_wide[3],
        own_wide[4],
        fc1_result.T,
        own_hidden,
        fc2_result,
        own_wide[5],
    )


def solution(mesh):
    whole_fits = mesh.shape[TENSOR] == 4 and mesh.shape[DP] == 8
    return jax.shard_map(
        whole_image if whole_fits else local,
        mesh=mesh,
        in_specs=(
            P(DP, None, None),
            P(DP),
            P(),
            P(),
            P(None, None, TENSOR),
            P(None, TENSOR),
            P(TENSOR, None),
            P(),
            P(),
            P(),
            P(None, TENSOR),
            P(TENSOR),
            P(TENSOR, None),
            P(),
            P(DP, None, None),
        ),
        out_specs=(
            P(DP, None, TENSOR),
            P(DP, None, TENSOR),
            P(TENSOR),
            P(TENSOR),
            P(None, None, TENSOR),
            P(None, TENSOR),
            P(TENSOR, None),
            P(TENSOR),
            P(TENSOR),
            P(TENSOR),
            P(None, TENSOR),
            P(TENSOR),
            P(TENSOR, None),
            P(TENSOR),
        ),
        check_vma=False,
    )
```
